32 devices in a mesh: dp: 4 (over z), ctx: 8 (over y, x, core).
Axes of the slice: x: 2, y: 2, z: 4, core: 2. Of those that a mesh axis runs over, the one named last changes fastest.
Arguments:
- hidden_in: bfloat16 [4, 1024, 2048], P('dp', 'ctx'), may hold values from -6 to 6
- w_in_t: bfloat16 [14336, 2048], P(None, ('dp', 'ctx')), may hold values from -4 to 4
- in_bias: bfloat16 [7, 2048], P(None, ('dp', 'ctx')), may hold values from -3 to 3
- ln_gain: bfloat16 [1, 2048], P(None, ('dp', 'ctx')), may hold values from 0.5 to 1.5
- ln_shift: bfloat16 [1, 2048], P(None, ('dp', 'ctx')), may hold values from -2 to 2
- w_out_t: bfloat16 [2048, 10240], P(('dp', 'ctx')), may hold values from -4 to 4
- out_bias: bfloat16 [2048], P(('dp', 'ctx')), may hold values from -3 to 3
- segment_ids: int32 [4, 1024], P('dp'), may hold values from 0 to 3, never falling along the last dimension, each value on 1 to 768 neighbouring positions
- out_grad: bfloat16 [4, 1024, 2048], P('dp', 'ctx'), may hold values from -6 to 6
Outputs:
- layer_out: bfloat16 [4, 1024, 2048], P('dp', 'ctx')
- input_grad: float32 [4, 1024, 2048], P('dp', 'ctx')
- grad_w_in: float32 [14336, 2048], P(None, ('dp', 'ctx'))
- grad_in_bias: float32 [7, 2048], P(None, ('dp', 'ctx'))
- grad_gain: float32 [1, 2048], P(None, ('dp', 'ctx'))
- grad_shift: float32 [1, 2048], P(None, ('dp', 'ctx'))
- grad_w_out: float32 [2048, 10240], P(('dp', 'ctx'))
- grad_out_bias: float32 [2048], P(('dp', 'ctx'))
The draws below stay inside these ranges and needn't reach their ends.
Inputs may be any that keep to these rules, and one draw needn't show every extreme that they name: `segment_ids`: within each sequence the numbers never fall; every document has 1 to 768 tokens and one has exactly 768.
All inputs are finite; a program needn't handle non-finite values.
Results may differ from the reference program's by a relative error of at most 0.033.
Values may be sent and summed in bfloat16 or wider, within the bound.
A program may use at most 704 MiB of HBM per device.

```python
import math
import jax
import jax.numpy as jnp
import numpy as np
from jax import lax

D = 2048
H = 32
HD = 64
ROT = 32
FF = 8192
KEY_BLOCK = 512
SEQ = 1024
SEQS = 4
MOST = 768
DOCS = 4
UNITE = 7


def draw_w_in_t(key, part):
    scale_in = D ** (-0.5)
    key_base = jax.random.fold_in(key, 0)
    base = jax.random.truncated_normal(key_base, -6.0, 6.0, (3 * D + FF, D), jnp.float32) * scale_in
    return base.astype(jnp.bfloat16)


def draw_w_out_t(key, part):
    scale_out = (D + FF) ** (-0.5)
    column = jnp.arange(D + FF)
    factor = jnp.where(column < D, 16.0, 1.5)[None, :] * scale_out
    base = jax.random.truncated_normal(key, -6.0, 6.0, (D, D + FF), jnp.float32)
    return (base * factor).astype(jnp.bfloat16)


def strengthened(array, key, source, target, blocks, factor):
    owner, partner = [(jnp.arange(array.shape[dim]) // (array.shape[dim] // blocks)).reshape([-1 if axis == dim else 1 for axis in range(array.ndim)]) for dim in (source, target)]
    chosen = jax.random.permutation(key, blocks)[partner]
    strong = (owner == chosen) | (owner == (partner + blocks // 2) % blocks)
    return jnp.where(strong, factor * array, array)


def block_levels(rng, shape, cuts, low, top_value):
    gain, own = 1.0, jax.random.fold_in(rng, 6)
    for axis_at, blocks in cuts:
        heights = jnp.exp(jax.random.uniform(jax.random.fold_in(own, axis_at), (blocks,), jnp.float32, low / len(cuts), top_value / len(cuts)))
        gain = gain * jnp.repeat(heights, shape[axis_at] // blocks).reshape([-1 if axis == axis_at else 1 for axis in range(len(shape))])
    return gain


def length_profile(number_of, total, limit, slope):
    loads = [(1 << 20) // math.isqrt(standing ** slope) + 1 for standing in range(2, number_of + 1)]
    rest, given = total - limit - (number_of - 1), [1] * (number_of - 1)
    while rest > 0:
        free = [i for i in range(number_of - 1) if given[i] < limit]
        whole, budget = sum([loads[i] for i in free]), rest
        for i in free:
            addition = min(limit - given[i], max(1, budget * loads[i] // whole), rest)
            given[i] = given[i] + addition
            rest = rest - addition
    return np.array([limit] + given)


def uneven(stream_key, count, total, most, lean):
    if count == 2:
        one = jax.random.randint(stream_key, (), max(1, total - most), min(most, total - 1) + 1)
        return jnp.stack([one, total - one])
    lengths = jnp.asarray(length_profile(count, total, most, lean), jnp.int32)
    twos = (count - 1) // 2
    donor, sink = lengths[1:1 + 2 * twos:2], lengths[2:2 + 2 * twos:2]
    slack = jnp.minimum(donor - 1, most - sink)
    passed = jax.random.randint(jax.random.fold_in(stream_key, 1), (twos,), 0, 1 << 20) % (slack + 1)
    lengths = lengths.at[1:1 + 2 * twos:2].set(donor - passed).at[2:2 + 2 * twos:2].set(sink + passed)
    return lengths[jax.random.permutation(jax.random.fold_in(stream_key, 2), count)]


def bell_draw(stream_key, shape, spread, limit, shards=(), kind=jnp.bfloat16):
    values = spread * jax.random.normal(stream_key, shape, jnp.float32)
    if shards:
        values = values * block_levels(stream_key, shape, shards, -0.22, 0.18)
    return jnp.clip(values, -limit, limit).astype(kind)


def gaussian_with(rng, shape, deviation, most, shards, heavy, kind=jnp.bfloat16):
    result = deviation * jax.random.normal(rng, shape, jnp.float32)
    if shards:
        result = result * block_levels(rng, shape, shards, -0.22, 0.18)
    return jnp.clip(strengthened(result, jax.random.fold_in(rng, 3), *heavy), -most, most).astype(kind)


def setup_inputs(seed: int = 0) -> dict:
    key_list = jax.random.split(jax.random.key(seed), 10)
    hidden_in = bell_draw(key_list[0], (SEQS, SEQ, D), 1.0, 6.0, ((0, 4), (1, 8)))
    w_in_t = draw_w_in_t(jax.random.fold_in(key_list[9], 71), 0)
    in_bias = bell_draw(key_list[2], (UNITE, D), 0.5, 3.0, ((1, 32),))
    ln_gain = jnp.clip(1.0 + 0.1 * jax.random.normal(key_list[3], (1, D), jnp.float32), 0.5, 1.5).astype(jnp.bfloat16)
    ln_shift = bell_draw(key_list[4], (1, D), 0.3, 2.0, ((1, 32),))
    w_out_t = draw_w_out_t(jax.random.fold_in(key_list[9], 71), 0)
    out_bias = bell_draw(key_list[6], (D,), 0.5, 3.0, ((0, 32),))
    segment_ids = jax.vmap(lambda own: jnp.searchsorted(jnp.cumsum(uneven(own, DOCS, SEQ, MOST, 0)), jnp.arange(SEQ), side="right"))(jax.random.split(key_list[7], SEQS)).reshape((SEQS, SEQ)).astype(jnp.int32)
    out_grad = gaussian_with(key_list[8], (SEQS, SEQ, D), 1.0, 6.0, ((0, 4), (1, 8)), (1, 2, 8, 2.0))
    return {"hidden_in": hidden_in, "w_in_t": w_in_t, "in_bias": in_bias, "ln_gain": ln_gain, "ln_shift": ln_shift, "w_out_t": w_out_t, "out_bias": out_bias, "segment_ids": segment_ids, "out_grad": out_grad}


@jax.custom_vjp
def low(v):
    return lax.optimization_barrier(v.astype(jnp.bfloat16)).astype(jnp.float32)

@jax.custom_vjp
def low_back(v):
    return v

def low_keep(v):
    return (low(v), None)

def low_pass(kept, grad):
    return (grad,)

def back_keep(v):
    return (v, None)

def back_low(kept, grad):
    return (low(grad),)
low.defvjp(low_keep, low_pass)
low_back.defvjp(back_keep, back_low)
epsilon = 1e-05
highest = lax.Precision.HIGHEST

def rotation_tables(positions):
    half_dims = ROT // 2
    frequency = 10000.0 ** (-2.0 * jnp.arange(half_dims, dtype=jnp.float32) / ROT)
    angles = positions[:, None] * frequency[None, :]
    return (jnp.cos(angles)[:, None, :], jnp.sin(angles)[:, None, :])

def rotate(heads_in, cosine_table, sine_table):
    half_dims = ROT // 2
    first_half = heads_in[..., :half_dims]
    second_half = heads_in[..., half_dims:ROT]
    return jnp.concatenate([first_half * cosine_table - second_half * sine_table, second_half * cosine_table + first_half * sine_table, heads_in[..., ROT:]], -1)

def attend_block(query_rows, query_seg, query_index, key_heads, value_heads, seg_row, key_index):
    scores = jnp.einsum('qhd,khd->hqk', query_rows, key_heads, precision=highest) * HD ** (-0.5)
    scores = low_back(scores)
    allowed = (query_seg[:, None] == seg_row[None, :]) & (query_index[:, None] >= key_index[None, :])
    scores = jnp.where(allowed[None], scores, -1e+30)
    largest = lax.optimization_barrier(jnp.max(scores, -1, keepdims=True))
    weights = jnp.where(allowed[None], jnp.exp(scores - largest), 0.0)
    weights = weights / lax.optimization_barrier(jnp.sum(weights, -1, keepdims=True))
    return jnp.einsum('hqk,khd->qhd', low(weights), value_heads, precision=highest)

def sequence_layer(params, inputs, seg_row):
    weight_in, bias_in, gain_row, shift_row, weight_out, bias_out = params
    index_all = jnp.arange(SEQ, dtype=jnp.int32)
    earlier = jnp.concatenate([seg_row[:1], seg_row[:-1]])
    begins = jnp.where((index_all == 0) | (seg_row != earlier), index_all, 0)
    positions = (index_all - lax.cummax(begins, axis=0)).astype(jnp.float32)
    cosine_table, sine_table = rotation_tables(positions)
    average = lax.optimization_barrier(jnp.mean(inputs, -1, keepdims=True))
    centred = inputs - average
    inv_std = lax.rsqrt(lax.optimization_barrier(jnp.mean(centred * centred, -1, keepdims=True)) + epsilon)
    normed = low(centred * inv_std * gain_row + shift_row)
    projected = jnp.dot(normed, weight_in.T, precision=highest, preferred_element_type=jnp.float32)
    projected = low_back(projected + bias_in.reshape(1, -1))
    queries = low(rotate(projected[:, :D].reshape(SEQ, H, HD), cosine_table, sine_table))
    key_heads = low(rotate(projected[:, D:2 * D].reshape(SEQ, H, HD), cosine_table, sine_table))
    value_heads = low(projected[:, 2 * D:3 * D].reshape(SEQ, H, HD))
    hidden = low(jax.nn.gelu(projected[:, 3 * D:], approximate=True))
    blocks = SEQ // KEY_BLOCK
    attend = jax.checkpoint(attend_block)

    def one_block(pieces):
        return attend(pieces[0], pieces[1], pieces[2], key_heads, value_heads, seg_row, index_all)
    attended = lax.map(one_block, (queries.reshape(blocks, KEY_BLOCK, H, HD), seg_row.reshape(blocks, KEY_BLOCK), index_all.reshape(blocks, KEY_BLOCK)))
    attention = low(low_back(attended.reshape(SEQ, D)))
    joined = jnp.concatenate([attention, hidden], 1)
    branch = jnp.dot(joined, weight_out.T, precision=highest, preferred_element_type=jnp.float32)
    return inputs + branch + bias_out[None, :]

def reference(hidden_in, w_in_t, in_bias, ln_gain, ln_shift, w_out_t, out_bias, segment_ids, out_grad):
    params = tuple((parameter.astype(jnp.float32) for parameter in (w_in_t, in_bias, ln_gain, ln_shift, w_out_t, out_bias)))
    inputs = hidden_in.astype(jnp.float32)

    def forward(params, inputs):

        def one_sequence(running, slices):
            return (running, sequence_layer(params, slices[0], slices[1]))
        return lax.scan(one_sequence, jnp.zeros((), jnp.float32), (inputs, segment_ids))[1]
    outputs, pullback = jax.vjp(forward, params, inputs)
    gradients, d_input = pullback(out_grad.astype(jnp.float32))
    return (outputs.astype(jnp.bfloat16), d_input, gradients[0], gradients[1], gradients[2], gradients[3], gradients[4], gradients[5])
```

```python
import math

import jax
import jax.numpy as jnp
from jax import lax
from jax.sharding import PartitionSpec as P

H = 32
HD = 64
ROT = 32
KEY_BLOCK = 512


epsilon = 1e-05
negative = -1e30


def rotation_tables(positions):
    half_dims = ROT // 2
    frequency = 10000.0 ** (-2.0 * jnp.arange(half_dims, dtype=jnp.float32) / ROT)
    angles = positions[:, None] * frequency[None, :]
    return (jnp.cos(angles)[:, None, :], jnp.sin(angles)[:, None, :])


def rotate(heads_in, cosine_table, sine_table, direction):
    half_dims = ROT // 2
    first_half = heads_in[..., :half_dims]
    second_half = heads_in[..., half_dims:ROT]
    return jnp.concatenate(
        [
            first_half * cosine_table - direction * second_half * sine_table,
            second_half * cosine_table + direction * first_half * sine_table,
            heads_in[..., ROT:],
        ],
        -1,
    )


def masked_scores(queries, key_rows, key_seg, key_index, query_seg, query_index):
    scaling = queries.shape[2] ** (-0.5)
    scores = (
        jnp.einsum("thd,khd->htk", queries, key_rows, preferred_element_type=jnp.float32) * scaling
    )
    allowed = (query_seg[:, None] == key_seg[None, :]) & (
        query_index[:, None] >= key_index[None, :]
    )
    return (jnp.where(allowed[None], scores, negative), allowed)


def score_grads(
    query_part,
    dout_part,
    lse_part,
    dot_part,
    query_seg,
    query_index,
    key_rows,
    value_rows,
    key_seg,
    key_index,
):
    scores, allowed = masked_scores(
        query_part, key_rows, key_seg, key_index, query_seg, query_index
    )
    weights = jnp.where(allowed[None], jnp.exp(scores - lse_part[..., None]), 0.0)
    d_weights = jnp.einsum(
        "thd,khd->htk", dout_part, value_rows, preferred_element_type=jnp.float32
    )
    d_scores = (weights * (d_weights - dot_part[..., None])).astype(jnp.bfloat16)
    return (weights.astype(jnp.bfloat16), d_scores)


def key_grads(
    key_rows,
    value_rows,
    key_seg,
    key_index,
    query_src,
    dout_src,
    lse_src,
    dot_src,
    seg_src,
    index_src,
    query_block,
):
    key_count = key_rows.shape[0]
    scaling = HD ** (-0.5)
    block_count = query_src.shape[0] // query_block

    def query_step(running, block_no):
        weights_low, d_scores = score_grads(
            query_src,
            dout_src,
            lse_src,
            dot_src,
            seg_src,
            index_src,
            key_rows,
            value_rows,
            key_seg,
            key_index,
        )
        d_key = (
            running[0]
            + jnp.einsum("htk,thd->khd", d_scores, query_src, preferred_element_type=jnp.float32)
            * scaling
        )
        d_value = running[1] + jnp.einsum(
            "htk,thd->khd", weights_low, dout_src, preferred_element_type=jnp.float32
        )
        return ((d_key, d_value), None)

    zero_heads = jnp.zeros((key_count, H, HD), jnp.float32)
    (d_key, d_value), _ = lax.scan(query_step, (zero_heads, zero_heads), jnp.arange(block_count))
    return (d_key.reshape(key_count, H * HD), d_value.reshape(key_count, H * HD))


def on_device_gathered(
    hidden_in, w_in_t, in_bias, ln_gain, ln_shift, w_out_t, out_bias, segment_ids, out_grad
):
    inputs = hidden_in[0].astype(jnp.float32)
    tok_rows, model_width = inputs.shape
    seg_row = segment_ids[0]
    seq_len = seg_row.shape[0]
    offset = lax.axis_index("ctx") * tok_rows
    index_all = jnp.arange(seq_len, dtype=jnp.int32)
    earlier = jnp.concatenate([seg_row[:1], seg_row[:-1]])
    begins = jnp.where((index_all == 0) | (seg_row != earlier), index_all, 0)
    positions = (index_all - lax.cummax(begins, axis=0)).astype(jnp.float32)
    local_pos = lax.dynamic_slice_in_dim(positions, offset, tok_rows)
    query_seg = lax.dynamic_slice_in_dim(seg_row, offset, tok_rows)
    query_index = offset + jnp.arange(tok_rows, dtype=jnp.int32)
    cosine_table, sine_table = rotation_tables(local_pos)
    scaling = HD ** (-0.5)
    average = jnp.mean(inputs, -1, keepdims=True)
    centred = inputs - average
    inv_std = lax.rsqrt(jnp.mean(centred * centred, -1, keepdims=True) + epsilon)
    normed_hat = centred * inv_std
    joint_width = w_in_t.shape[0]
    bias_rows = in_bias.shape[0]
    weight_piece = lax.all_gather(w_in_t, ("dp", "ctx"), axis=1, tiled=True)
    bias_piece = lax.all_gather(in_bias, ("dp", "ctx"), axis=1, tiled=True)
    gain_piece = lax.all_gather(ln_gain, ("dp", "ctx"), axis=1, tiled=True)
    shift_piece = lax.all_gather(ln_shift, ("dp", "ctx"), axis=1, tiled=True)
    normed_piece = (
        normed_hat * gain_piece.astype(jnp.float32) + shift_piece.astype(jnp.float32)
    ).astype(jnp.bfloat16)
    summed = lax.dot_general(
        normed_piece, weight_piece, (((1,), (1,)), ((), ())), preferred_element_type=jnp.float32
    )
    gain_all = gain_piece.astype(jnp.float32)
    bias_all = bias_piece.astype(jnp.float32)
    projected, normed, gain_all, bias_all = (summed, normed_piece, gain_all, bias_all)
    projected = projected + bias_all.reshape(1, joint_width)
    queries = rotate(
        projected[:, :model_width].reshape(tok_rows, H, HD), cosine_table, sine_table, 1.0
    ).astype(jnp.bfloat16)
    keys_new = (
        rotate(
            projected[:, model_width : 2 * model_width].reshape(tok_rows, H, HD),
            cosine_table,
            sine_table,
            1.0,
        )
        .astype(jnp.bfloat16)
        .reshape(tok_rows, model_width)
    )
    values_new = projected[:, 2 * model_width : 3 * model_width].astype(jnp.bfloat16)
    pre_gelu = projected[:, 3 * model_width :]
    keys_all, values_all = (
        lax.all_gather(keys_new, "ctx", axis=0, tiled=True),
        lax.all_gather(values_new, "ctx", axis=0, tiled=True),
    )
    block_count = seq_len // KEY_BLOCK

    def key_slice(first_key, key_count):
        key_rows = lax.dynamic_slice_in_dim(keys_all, first_key, key_count, 0).reshape(
            key_count, H, HD
        )
        value_rows = lax.dynamic_slice_in_dim(values_all, first_key, key_count, 0).reshape(
            key_count, H, HD
        )
        key_seg = lax.dynamic_slice_in_dim(seg_row, first_key, key_count)
        key_index = first_key + jnp.arange(key_count, dtype=jnp.int32)
        return (key_rows, value_rows, key_seg, key_index)

    def stats_step(running, block_no):
        running_max, running_sum = running
        key_rows, value_rows, key_seg, key_index = key_slice(block_no * KEY_BLOCK, KEY_BLOCK)
        scores, allowed = masked_scores(
            queries, key_rows, key_seg, key_index, query_seg, query_index
        )
        new_max = jnp.maximum(running_max, jnp.max(scores, -1))
        weights = jnp.where(allowed[None], jnp.exp(scores - new_max[..., None]), 0.0)
        running_sum = running_sum * jnp.exp(running_max - new_max) + jnp.sum(weights, -1)
        return ((new_max, running_sum), None)

    stats_init = (
        jnp.full((H, tok_rows), negative, jnp.float32),
        jnp.zeros((H, tok_rows), jnp.float32),
    )
    (final_max, final_sum), _ = lax.scan(stats_step, stats_init, jnp.arange(block_count))
    log_total = final_max + jnp.log(final_sum)

    def value_step(attended, block_no):
        key_rows, value_rows, key_seg, key_index = key_slice(block_no * KEY_BLOCK, KEY_BLOCK)
        scores, allowed = masked_scores(
            queries, key_rows, key_seg, key_index, query_seg, query_index
        )
        weights = jnp.where(allowed[None], jnp.exp(scores - log_total[..., None]), 0.0).astype(
            jnp.bfloat16
        )
        attended = attended + jnp.einsum(
            "htk,khd->thd", weights, value_rows, preferred_element_type=jnp.float32
        )
        return (attended, None)

    attended, _ = lax.scan(
        value_step, jnp.zeros((tok_rows, H, HD), jnp.float32), jnp.arange(block_count)
    )
    hidden = jax.nn.gelu(pre_gelu, approximate=True).astype(jnp.bfloat16)
    joined = jnp.concatenate(
        [attended.reshape(tok_rows, model_width).astype(jnp.bfloat16), hidden], 1
    )
    weight_piece, bias_piece = lax.all_gather(
        (w_out_t, out_bias), ("dp", "ctx"), axis=0, tiled=True
    )
    branch = (
        lax.dot_general(
            joined, weight_piece, (((1,), (1,)), ((), ())), preferred_element_type=jnp.float32
        )
        + bias_piece.astype(jnp.float32)[None, :]
    )
    result = (inputs + branch).astype(jnp.bfloat16)
    cotangent = out_grad[0]
    grad_part = cotangent
    d_joined = jnp.dot(
        grad_part,
        lax.all_gather(w_out_t, ("dp", "ctx"), axis=0, tiled=True),
        preferred_element_type=jnp.float32,
    )
    d_attn = d_joined[:, :model_width].astype(jnp.bfloat16).reshape(tok_rows, H, HD)

    def gelu_tanh(pre_values):
        return jax.nn.gelu(pre_values, approximate=True)

    _, gelu_pull = jax.vjp(gelu_tanh, pre_gelu)
    d_pre = gelu_pull(d_joined[:, model_width:])[0]
    row_dots = jnp.einsum("thd,thd->ht", d_attn.astype(jnp.float32), attended)

    def query_grad_step(d_query, block_no):
        key_rows, value_rows, key_seg, key_index = key_slice(block_no * KEY_BLOCK, KEY_BLOCK)
        _, d_scores = score_grads(
            queries,
            d_attn,
            log_total,
            row_dots,
            query_seg,
            query_index,
            key_rows,
            value_rows,
            key_seg,
            key_index,
        )
        d_query = (
            d_query
            + jnp.einsum("htk,khd->thd", d_scores, key_rows, preferred_element_type=jnp.float32)
            * scaling
        )
        return (d_query, None)

    d_query, _ = lax.scan(
        query_grad_step, jnp.zeros((tok_rows, H, HD), jnp.float32), jnp.arange(block_count)
    )
    count = lax.axis_size("ctx") * tok_rows
    sub_rows = math.gcd(count, KEY_BLOCK)

    def sub_step(carry_none, block_no):
        key_rows, value_rows, key_seg, key_index = key_slice(block_no * sub_rows, sub_rows)
        d_key, d_value = key_grads(
            key_rows,
            value_rows,
            key_seg,
            key_index,
            queries,
            d_attn,
            log_total,
            row_dots,
            query_seg,
            query_index,
            tok_rows,
        )
        return (carry_none, jnp.concatenate([d_key, d_value], 1))

    _, stacked = lax.scan(sub_step, jnp.zeros((), jnp.float32), jnp.arange(count // sub_rows))
    d_kv = lax.psum_scatter(
        stacked.reshape(count, 2 * model_width).astype(jnp.bfloat16),
        "ctx",
        scatter_dimension=0,
        tiled=True,
    ).astype(jnp.float32)
    d_key_local, d_value_local = (d_kv[:, :model_width], d_kv[:, model_width:])
    d_query_pre = rotate(d_query, cosine_table, sine_table, -1.0).reshape(tok_rows, model_width)
    d_key_pre = rotate(
        d_key_local.reshape(tok_rows, H, HD), cosine_table, sine_table, -1.0
    ).reshape(tok_rows, model_width)
    d_joint = jnp.concatenate([d_query_pre, d_key_pre, d_value_local, d_pre], 1).astype(
        jnp.bfloat16
    )
    d_normed = jnp.dot(
        d_joint,
        lax.all_gather(w_in_t, ("dp", "ctx"), axis=1, tiled=True),
        preferred_element_type=jnp.float32,
    )
    grad_part = cotangent
    in_term = lax.dot_general(
        normed, d_joint, (((0,), (0,)), ((), ())), preferred_element_type=jnp.float32
    )
    out_term = lax.dot_general(
        grad_part, joined, (((0,), (0,)), ((), ())), preferred_element_type=jnp.float32
    )
    grad_rows = lax.psum_scatter(
        jnp.concatenate([in_term, out_term], 1), ("dp", "ctx"), scatter_dimension=0, tiled=True
    )
    grad_w_in = grad_rows[:, :joint_width].T
    grad_w_out = grad_rows[:, joint_width:]
    grad_bias_in = jnp.sum(d_joint.astype(jnp.float32), 0).reshape(bias_rows, model_width)
    grad_gain_row = jnp.sum(d_normed * normed_hat, 0, keepdims=True)
    grad_shift_row = jnp.sum(d_normed, 0, keepdims=True)
    grad_bias_out = jnp.sum(cotangent.astype(jnp.float32), 0, keepdims=True)
    grad_in_bias, grad_gain, grad_shift, grad_out_row = (
        lax.psum_scatter(grad_bias_in, ("dp", "ctx"), scatter_dimension=1, tiled=True),
        lax.psum_scatter(grad_gain_row, ("dp", "ctx"), scatter_dimension=1, tiled=True),
        lax.psum_scatter(grad_shift_row, ("dp", "ctx"), scatter_dimension=1, tiled=True),
        lax.psum_scatter(grad_bias_out, ("dp", "ctx"), scatter_dimension=1, tiled=True),
    )
    d_hat = d_normed * gain_all
    d_input = inv_std * (
        d_hat
        - jnp.mean(d_hat, -1, keepdims=True)
        - normed_hat * jnp.mean(d_hat * normed_hat, -1, keepdims=True)
    ) + cotangent.astype(jnp.float32)
    return (
        result[None],
        d_input[None],
        grad_w_in,
        grad_in_bias,
        grad_gain,
        grad_shift,
        grad_w_out,
        grad_out_row[0],
    )


AXES = ("dp", "ctx")


def layer_norm_stats(inputs):
    average = jnp.mean(inputs, -1, keepdims=True)
    centred = inputs - average
    inv_std = lax.rsqrt(jnp.mean(centred * centred, -1, keepdims=True) + epsilon)
    return centred * inv_std, inv_std


def exchange(blocks):
    return lax.all_to_all(blocks, AXES, split_axis=0, concat_axis=0, tiled=True)


def to_blocks(rows, parts, count, width):
    depth = rows.shape[0]
    return rows.reshape(depth, parts, count, width).transpose(2, 0, 1, 3).reshape(count, depth, parts * width)


def from_blocks(blocks, parts, width):
    count, depth, _ = blocks.shape
    return blocks.reshape(count, depth, parts, width).transpose(1, 2, 0, 3).reshape(depth, parts * count * width)


def attention(queries, keys, values, d_out, seg_all):
    seq_len = seg_all.shape[1]
    scaling = HD ** (-0.5)
    index = jnp.arange(seq_len)
    allowed = (seg_all[:, :, None] == seg_all[:, None, :]) & (index[:, None] >= index[None, :])[None]
    scores = jnp.einsum("bqd,bkd->bqk", queries, keys, preferred_element_type=jnp.float32) * scaling
    scores = jnp.where(allowed, scores, negative)
    largest = jnp.max(scores, -1, keepdims=True)
    weights = jnp.where(allowed, jnp.exp(scores - largest), 0.0)
    weights = weights / jnp.sum(weights, -1, keepdims=True)
    weights_low = weights.astype(jnp.bfloat16)
    attended = jnp.einsum("bqk,bkd->bqd", weights_low, values, preferred_element_type=jnp.float32)
    row_dots = jnp.sum(d_out.astype(jnp.float32) * attended, -1, keepdims=True)
    d_weights = jnp.einsum("bqd,bkd->bqk", d_out, values, preferred_element_type=jnp.float32)
    d_scores = (weights * (d_weights - row_dots)).astype(jnp.bfloat16)
    d_query = jnp.einsum("bqk,bkd->bqd", d_scores, keys, preferred_element_type=jnp.float32) * scaling
    d_key = jnp.einsum("bqk,bqd->bkd", d_scores, queries, preferred_element_type=jnp.float32) * scaling
    d_value = jnp.einsum("bqk,bqd->bkd", weights_low, d_out, preferred_element_type=jnp.float32)
    return attended, d_query, d_key, d_value


def rotate_rows(rows, cosine, sine, direction):
    half = ROT // 2
    first, second = rows[:, :half], rows[:, half:ROT]
    return jnp.concatenate(
        [first * cosine - direction * second * sine, second * cosine + direction * first * sine, rows[:, ROT:]], 1
    )


def on_device(
    hidden_in, w_in_t, in_bias, ln_gain, ln_shift, w_out_t, out_bias, segment_ids, out_grad
):
    devices = lax.axis_size("dp") * lax.axis_size("ctx")
    me = lax.axis_index("dp") * lax.axis_size("ctx") + lax.axis_index("ctx")
    tok_rows, model_width = hidden_in.shape[1:]
    seq_len = segment_ids.shape[1]
    tokens = devices * tok_rows
    seqs = tokens // seq_len
    own = model_width // devices
    in_parts = in_bias.shape[0]
    out_parts = w_out_t.shape[1] // model_width
    w_in = exchange(to_blocks(w_in_t.T, in_parts, devices, own)).reshape(model_width, in_parts * own)
    x_all = lax.all_gather(hidden_in[0], AXES, axis=0, tiled=True)
    vectors = lax.all_gather(jnp.concatenate([ln_gain, ln_shift], 0), AXES, axis=1, tiled=True).astype(jnp.float32)
    seg_all = lax.all_gather(segment_ids, "dp", axis=0, tiled=True)
    w_out = exchange(to_blocks(w_out_t, out_parts, devices, own)).reshape(model_width, out_parts * own)
    g_all = lax.all_gather(out_grad[0], AXES, axis=0, tiled=True)

    index_all = jnp.arange(seq_len, dtype=jnp.int32)[None]
    earlier = jnp.concatenate([seg_all[:, :1], seg_all[:, :-1]], 1)
    begins = jnp.where((index_all == 0) | (seg_all != earlier), index_all, 0)
    positions = (index_all - lax.cummax(begins, axis=1)).astype(jnp.float32).reshape(tokens)
    half = ROT // 2
    frequency = 10000.0 ** (-2.0 * jnp.arange(half, dtype=jnp.float32) / ROT)
    angles = positions[:, None] * frequency[None, :]
    cosine, sine = jnp.cos(angles), jnp.sin(angles)

    hat_all, _ = layer_norm_stats(x_all.astype(jnp.float32))
    normed = (hat_all * vectors[:1] + vectors[1:]).astype(jnp.bfloat16)
    joint = jnp.dot(normed, w_in, preferred_element_type=jnp.float32)
    joint = joint + in_bias.astype(jnp.float32).reshape(1, in_parts * own)
    shape = (seqs, seq_len, HD)
    queries = rotate_rows(joint[:, :own], cosine, sine, 1.0).astype(jnp.bfloat16)
    keys = rotate_rows(joint[:, own : 2 * own], cosine, sine, 1.0).astype(jnp.bfloat16)
    values = joint[:, 2 * own : 3 * own].astype(jnp.bfloat16)
    pre_gelu = joint[:, 3 * own :]

    d_joined = jnp.dot(g_all, w_out, preferred_element_type=jnp.float32)
    d_attn = d_joined[:, :own].astype(jnp.bfloat16)
    hidden, gelu_pull = jax.vjp(lambda t: jax.nn.gelu(t, approximate=True), pre_gelu)
    d_pre = gelu_pull(d_joined[:, own:])[0]

    attended, d_query, d_key, d_value = attention(
        queries.reshape(shape), keys.reshape(shape), values.reshape(shape), d_attn.reshape(shape), seg_all
    )
    joined = jnp.concatenate([attended.reshape(tokens, own).astype(jnp.bfloat16), hidden.astype(jnp.bfloat16)], 1)

    branch = lax.dot_general(joined, w_out, (((1,), (1,)), ((), ())), preferred_element_type=jnp.float32)
    column = jnp.arange(model_width) // own
    bias_row = jnp.where(column == me, jnp.tile(out_bias.astype(jnp.float32), devices), 0.0)
    branch = (branch + bias_row[None]).astype(jnp.bfloat16)
    branch_own = lax.psum_scatter(branch, AXES, scatter_dimension=0, tiled=True)
    inputs = hidden_in[0].astype(jnp.float32)
    result = (inputs + branch_own.astype(jnp.float32)).astype(jnp.bfloat16)

    d_joint = jnp.concatenate(
        [
            rotate_rows(d_query.reshape(tokens, own), cosine, sine, -1.0),
            rotate_rows(d_key.reshape(tokens, own), cosine, sine, -1.0),
            d_value.reshape(tokens, own),
            d_pre,
        ],
        1,
    )
    d_joint = d_joint.astype(jnp.bfloat16)
    d_normed_part = lax.dot_general(
        d_joint, w_in, (((1,), (1,)), ((), ())), preferred_element_type=jnp.float32
    ).astype(jnp.bfloat16)
    d_normed = lax.psum_scatter(d_normed_part, AXES, scatter_dimension=0, tiled=True).astype(jnp.float32)

    grad_out_local = lax.dot_general(
        g_all, joined, (((0,), (0,)), ((), ())), preferred_element_type=jnp.float32
    ).astype(jnp.bfloat16)
    grad_w_out = from_blocks(
        exchange(grad_out_local.reshape(devices, own, out_parts * own)), out_parts, own
    ).astype(jnp.float32)
    grad_in_local = lax.dot_general(
        normed, d_joint, (((0,), (0,)), ((), ())), preferred_element_type=jnp.float32
    ).astype(jnp.bfloat16)
    grad_w_in = from_blocks(
        exchange(grad_in_local.reshape(devices, own, in_parts * own)), in_parts, own
    ).astype(jnp.float32).T
    grad_in_bias = jnp.sum(d_joint.astype(jnp.float32), 0).reshape(in_parts, own)
    g_columns = lax.dynamic_slice_in_dim(g_all, me * own, own, 1)
    grad_out_bias = jnp.sum(g_columns.astype(jnp.float32), 0)

    hat, inv_std = layer_norm_stats(inputs)
    pair = jnp.stack([jnp.sum(d_normed * hat, 0), jnp.sum(d_normed, 0)])
    pair = lax.psum_scatter(pair, AXES, scatter_dimension=1, tiled=True)
    d_hat = d_normed * vectors[:1]
    d_input = inv_std * (
        d_hat - jnp.mean(d_hat, -1, keepdims=True) - hat * jnp.mean(d_hat * hat, -1, keepdims=True)
    ) + out_grad[0].astype(jnp.float32)
    return (
        result[None],
        d_input[None],
        grad_w_in,
        grad_in_bias,
        pair[:1],
        pair[1:],
        grad_w_out,
        grad_out_bias,
    )


def solution(mesh):
    in_specs = (
        P("dp", "ctx", None),
        P(None, ("dp", "ctx")),
        P(None, ("dp", "ctx")),
        P(None, ("dp", "ctx")),
        P(None, ("dp", "ctx")),
        P(("dp", "ctx"), None),
        P(("dp", "ctx")),
        P("dp", None),
        P("dp", "ctx", None),
    )
    out_specs = (
        P("dp", "ctx", None),
        P("dp", "ctx", None),
        P(None, ("dp", "ctx")),
        P(None, ("dp", "ctx")),
        P(None, ("dp", "ctx")),
        P(None, ("dp", "ctx")),
        P(("dp", "ctx"), None),
        P(("dp", "ctx")),
    )
    devices = mesh.shape["dp"] * mesh.shape["ctx"]
    body = on_device if devices == H else on_device_gathered
    return jax.shard_map(
        body, mesh=mesh, in_specs=in_specs, out_specs=out_specs, check_vma=False
    )
```

```python
import functools
import math

import jax
import jax.numpy as jnp
from jax import lax
from jax.experimental import pallas as pl
from jax.experimental.pallas import tpu as pltpu
from jax.sharding import PartitionSpec as P

H = 32
HD = 64
ROT = 32
KEY_BLOCK = 512


epsilon = 1e-05
negative = -1e30


def rotation_tables(positions):
    half_dims = ROT // 2
    frequency = 10000.0 ** (-2.0 * jnp.arange(half_dims, dtype=jnp.float32) / ROT)
    angles = positions[:, None] * frequency[None, :]
    return (jnp.cos(angles)[:, None, :], jnp.sin(angles)[:, None, :])


def rotate(heads_in, cosine_table, sine_table, direction):
    half_dims = ROT // 2
    first_half = heads_in[..., :half_dims]
    second_half = heads_in[..., half_dims:ROT]
    return jnp.concatenate(
        [
            first_half * cosine_table - direction * second_half * sine_table,
            second_half * cosine_table + direction * first_half * sine_table,
            heads_in[..., ROT:],
        ],
        -1,
    )


def masked_scores(queries, key_rows, key_seg, key_index, query_seg, query_index):
    scaling = queries.shape[2] ** (-0.5)
    scores = (
        jnp.einsum("thd,khd->htk", queries, key_rows, preferred_element_type=jnp.float32) * scaling
    )
    allowed = (query_seg[:, None] == key_seg[None, :]) & (
        query_index[:, None] >= key_index[None, :]
    )
    return (jnp.where(allowed[None], scores, negative), allowed)


def score_grads(
    query_part,
    dout_part,
    lse_part,
    dot_part,
    query_seg,
    query_index,
    key_rows,
    value_rows,
    key_seg,
    key_index,
):
    scores, allowed = masked_scores(
        query_part, key_rows, key_seg, key_index, query_seg, query_index
    )
    weights = jnp.where(allowed[None], jnp.exp(scores - lse_part[..., None]), 0.0)
    d_weights = jnp.einsum(
        "thd,khd->htk", dout_part, value_rows, preferred_element_type=jnp.float32
    )
    d_scores = (weights * (d_weights - dot_part[..., None])).astype(jnp.bfloat16)
    return (weights.astype(jnp.bfloat16), d_scores)


def key_grads(
    key_rows,
    value_rows,
    key_seg,
    key_index,
    query_src,
    dout_src,
    lse_src,
    dot_src,
    seg_src,
    index_src,
    query_block,
):
    key_count = key_rows.shape[0]
    scaling = HD ** (-0.5)
    block_count = query_src.shape[0] // query_block

    def query_step(running, block_no):
        weights_low, d_scores = score_grads(
            query_src,
            dout_src,
            lse_src,
            dot_src,
            seg_src,
            index_src,
            key_rows,
            value_rows,
            key_seg,
            key_index,
        )
        d_key = (
            running[0]
            + jnp.einsum("htk,thd->khd", d_scores, query_src, preferred_element_type=jnp.float32)
            * scaling
        )
        d_value = running[1] + jnp.einsum(
            "htk,thd->khd", weights_low, dout_src, preferred_element_type=jnp.float32
        )
        return ((d_key, d_value), None)

    zero_heads = jnp.zeros((key_count, H, HD), jnp.float32)
    (d_key, d_value), _ = lax.scan(query_step, (zero_heads, zero_heads), jnp.arange(block_count))
    return (d_key.reshape(key_count, H * HD), d_value.reshape(key_count, H * HD))


def on_device_gathered(
    hidden_in, w_in_t, in_bias, ln_gain, ln_shift, w_out_t, out_bias, segment_ids, out_grad
):
    inputs = hidden_in[0].astype(jnp.float32)
    tok_rows, model_width = inputs.shape
    seg_row = segment_ids[0]
    seq_len = seg_row.shape[0]
    offset = lax.axis_index("ctx") * tok_rows
    index_all = jnp.arange(seq_len, dtype=jnp.int32)
    earlier = jnp.concatenate([seg_row[:1], seg_row[:-1]])
    begins = jnp.where((index_all == 0) | (seg_row != earlier), index_all, 0)
    positions = (index_all - lax.cummax(begins, axis=0)).astype(jnp.float32)
    local_pos = lax.dynamic_slice_in_dim(positions, offset, tok_rows)
    query_seg = lax.dynamic_slice_in_dim(seg_row, offset, tok_rows)
    query_index = offset + jnp.arange(tok_rows, dtype=jnp.int32)
    cosine_table, sine_table = rotation_tables(local_pos)
    scaling = HD ** (-0.5)
    average = jnp.mean(inputs, -1, keepdims=True)
    centred = inputs - average
    inv_std = lax.rsqrt(jnp.mean(centred * centred, -1, keepdims=True) + epsilon)
    normed_hat = centred * inv_std
    joint_width = w_in_t.shape[0]
    bias_rows = in_bias.shape[0]
    weight_piece = lax.all_gather(w_in_t, ("dp", "ctx"), axis=1, tiled=True)
    bias_piece = lax.all_gather(in_bias, ("dp", "ctx"), axis=1, tiled=True)
    gain_piece = lax.all_gather(ln_gain, ("dp", "ctx"), axis=1, tiled=True)
    shift_piece = lax.all_gather(ln_shift, ("dp", "ctx"), axis=1, tiled=True)
    normed_piece = (
        normed_hat * gain_piece.astype(jnp.float32) + shift_piece.astype(jnp.float32)
    ).astype(jnp.bfloat16)
    summed = lax.dot_general(
        normed_piece, weight_piece, (((1,), (1,)), ((), ())), preferred_element_type=jnp.float32
    )
    gain_all = gain_piece.astype(jnp.float32)
    bias_all = bias_piece.astype(jnp.float32)
    projected, normed, gain_all, bias_all = (summed, normed_piece, gain_all, bias_all)
    projected = projected + bias_all.reshape(1, joint_width)
    queries = rotate(
        projected[:, :model_width].reshape(tok_rows, H, HD), cosine_table, sine_table, 1.0
    ).astype(jnp.bfloat16)
    keys_new = (
        rotate(
            projected[:, model_width : 2 * model_width].reshape(tok_rows, H, HD),
            cosine_table,
            sine_table,
            1.0,
        )
        .astype(jnp.bfloat16)
        .reshape(tok_rows, model_width)
    )
    values_new = projected[:, 2 * model_width : 3 * model_width].astype(jnp.bfloat16)
    pre_gelu = projected[:, 3 * model_width :]
    keys_all, values_all = (
        lax.all_gather(keys_new, "ctx", axis=0, tiled=True),
        lax.all_gather(values_new, "ctx", axis=0, tiled=True),
    )
    block_count = seq_len // KEY_BLOCK

    def key_slice(first_key, key_count):
        key_rows = lax.dynamic_slice_in_dim(keys_all, first_key, key_count, 0).reshape(
            key_count, H, HD
        )
        value_rows = lax.dynamic_slice_in_dim(values_all, first_key, key_count, 0).reshape(
            key_count, H, HD
        )
        key_seg = lax.dynamic_slice_in_dim(seg_row, first_key, key_count)
        key_index = first_key + jnp.arange(key_count, dtype=jnp.int32)
        return (key_rows, value_rows, key_seg, key_index)

    def stats_step(running, block_no):
        running_max, running_sum = running
        key_rows, value_rows, key_seg, key_index = key_slice(block_no * KEY_BLOCK, KEY_BLOCK)
        scores, allowed = masked_scores(
            queries, key_rows, key_seg, key_index, query_seg, query_index
        )
        new_max = jnp.maximum(running_max, jnp.max(scores, -1))
        weights = jnp.where(allowed[None], jnp.exp(scores - new_max[..., None]), 0.0)
        running_sum = running_sum * jnp.exp(running_max - new_max) + jnp.sum(weights, -1)
        return ((new_max, running_sum), None)

    stats_init = (
        jnp.full((H, tok_rows), negative, jnp.float32),
        jnp.zeros((H, tok_rows), jnp.float32),
    )
    (final_max, final_sum), _ = lax.scan(stats_step, stats_init, jnp.arange(block_count))
    log_total = final_max + jnp.log(final_sum)

    def value_step(attended, block_no):
        key_rows, value_rows, key_seg, key_index = key_slice(block_no * KEY_BLOCK, KEY_BLOCK)
        scores, allowed = masked_scores(
            queries, key_rows, key_seg, key_index, query_seg, query_index
        )
        weights = jnp.where(allowed[None], jnp.exp(scores - log_total[..., None]), 0.0).astype(
            jnp.bfloat16
        )
        attended = attended + jnp.einsum(
            "htk,khd->thd", weights, value_rows, preferred_element_type=jnp.float32
        )
        return (attended, None)

    attended, _ = lax.scan(
        value_step, jnp.zeros((tok_rows, H, HD), jnp.float32), jnp.arange(block_count)
    )
    hidden = jax.nn.gelu(pre_gelu, approximate=True).astype(jnp.bfloat16)
    joined = jnp.concatenate(
        [attended.reshape(tok_rows, model_width).astype(jnp.bfloat16), hidden], 1
    )
    weight_piece, bias_piece = lax.all_gather(
        (w_out_t, out_bias), ("dp", "ctx"), axis=0, tiled=True
    )
    branch = (
        lax.dot_general(
            joined, weight_piece, (((1,), (1,)), ((), ())), preferred_element_type=jnp.float32
        )
        + bias_piece.astype(jnp.float32)[None, :]
    )
    result = (inputs + branch).astype(jnp.bfloat16)
    cotangent = out_grad[0]
    grad_part = cotangent
    d_joined = jnp.dot(
        grad_part,
        lax.all_gather(w_out_t, ("dp", "ctx"), axis=0, tiled=True),
        preferred_element_type=jnp.float32,
    )
    d_attn = d_joined[:, :model_width].astype(jnp.bfloat16).reshape(tok_rows, H, HD)

    def gelu_tanh(pre_values):
        return jax.nn.gelu(pre_values, approximate=True)

    _, gelu_pull = jax.vjp(gelu_tanh, pre_gelu)
    d_pre = gelu_pull(d_joined[:, model_width:])[0]
    row_dots = jnp.einsum("thd,thd->ht", d_attn.astype(jnp.float32), attended)

    def query_grad_step(d_query, block_no):
        key_rows, value_rows, key_seg, key_index = key_slice(block_no * KEY_BLOCK, KEY_BLOCK)
        _, d_scores = score_grads(
            queries,
            d_attn,
            log_total,
            row_dots,
            query_seg,
            query_index,
            key_rows,
            value_rows,
            key_seg,
            key_index,
        )
        d_query = (
            d_query
            + jnp.einsum("htk,khd->thd", d_scores, key_rows, preferred_element_type=jnp.float32)
            * scaling
        )
        return (d_query, None)

    d_query, _ = lax.scan(
        query_grad_step, jnp.zeros((tok_rows, H, HD), jnp.float32), jnp.arange(block_count)
    )
    count = lax.axis_size("ctx") * tok_rows
    sub_rows = math.gcd(count, KEY_BLOCK)

    def sub_step(carry_none, block_no):
        key_rows, value_rows, key_seg, key_index = key_slice(block_no * sub_rows, sub_rows)
        d_key, d_value = key_grads(
            key_rows,
            value_rows,
            key_seg,
            key_index,
            queries,
            d_attn,
            log_total,
            row_dots,
            query_seg,
            query_index,
            tok_rows,
        )
        return (carry_none, jnp.concatenate([d_key, d_value], 1))

    _, stacked = lax.scan(sub_step, jnp.zeros((), jnp.float32), jnp.arange(count // sub_rows))
    d_kv = lax.psum_scatter(
        stacked.reshape(count, 2 * model_width).astype(jnp.bfloat16),
        "ctx",
        scatter_dimension=0,
        tiled=True,
    ).astype(jnp.float32)
    d_key_local, d_value_local = (d_kv[:, :model_width], d_kv[:, model_width:])
    d_query_pre = rotate(d_query, cosine_table, sine_table, -1.0).reshape(tok_rows, model_width)
    d_key_pre = rotate(
        d_key_local.reshape(tok_rows, H, HD), cosine_table, sine_table, -1.0
    ).reshape(tok_rows, model_width)
    d_joint = jnp.concatenate([d_query_pre, d_key_pre, d_value_local, d_pre], 1).astype(
        jnp.bfloat16
    )
    d_normed = jnp.dot(
        d_joint,
        lax.all_gather(w_in_t, ("dp", "ctx"), axis=1, tiled=True),
        preferred_element_type=jnp.float32,
    )
    grad_part = cotangent
    in_term = lax.dot_general(
        normed, d_joint, (((0,), (0,)), ((), ())), preferred_element_type=jnp.float32
    )
    out_term = lax.dot_general(
        grad_part, joined, (((0,), (0,)), ((), ())), preferred_element_type=jnp.float32
    )
    grad_rows = lax.psum_scatter(
        jnp.concatenate([in_term, out_term], 1), ("dp", "ctx"), scatter_dimension=0, tiled=True
    )
    grad_w_in = grad_rows[:, :joint_width].T
    grad_w_out = grad_rows[:, joint_width:]
    grad_bias_in = jnp.sum(d_joint.astype(jnp.float32), 0).reshape(bias_rows, model_width)
    grad_gain_row = jnp.sum(d_normed * normed_hat, 0, keepdims=True)
    grad_shift_row = jnp.sum(d_normed, 0, keepdims=True)
    grad_bias_out = jnp.sum(cotangent.astype(jnp.float32), 0, keepdims=True)
    grad_in_bias, grad_gain, grad_shift, grad_out_row = (
        lax.psum_scatter(grad_bias_in, ("dp", "ctx"), scatter_dimension=1, tiled=True),
        lax.psum_scatter(grad_gain_row, ("dp", "ctx"), scatter_dimension=1, tiled=True),
        lax.psum_scatter(grad_shift_row, ("dp", "ctx"), scatter_dimension=1, tiled=True),
        lax.psum_scatter(grad_bias_out, ("dp", "ctx"), scatter_dimension=1, tiled=True),
    )
    d_hat = d_normed * gain_all
    d_input = inv_std * (
        d_hat
        - jnp.mean(d_hat, -1, keepdims=True)
        - normed_hat * jnp.mean(d_hat * normed_hat, -1, keepdims=True)
    ) + cotangent.astype(jnp.float32)
    return (
        result[None],
        d_input[None],
        grad_w_in,
        grad_in_bias,
        grad_gain,
        grad_shift,
        grad_w_out,
        grad_out_row[0],
    )


AXES = ("dp", "ctx")
MESH = pl.DeviceIdType.MESH
class Place:
    def __init__(self, depth):
        self.depth = depth
        self.z = lax.axis_index("dp")
        self.c = lax.axis_index("ctx")
        y, x, self.core = self.c // 4, (self.c // 2) % 2, self.c % 2
        self.first_stride = jnp.where(self.core == 0, 2, 4)
        self.last_stride = jnp.where(self.core == 0, 4, 2)
        self.f = jnp.where(self.core == 0, x, y)
        self.l = jnp.where(self.core == 0, y, x)

    def ctx(self, f, l, core):
        return f * self.first_stride + l * self.last_stride + core

    def shard(self, z, f, l, core):
        return z * 8 + self.ctx(f, l, core)

    def first(self):
        return {"dp": self.z, "ctx": self.ctx(1 - self.f, self.l, self.core)}

    def last(self):
        return {"dp": self.z, "ctx": self.ctx(self.f, 1 - self.l, self.core)}

    def sibling(self):
        return {"dp": self.z, "ctx": self.ctx(self.f, self.l, 1 - self.core)}

    def above(self):
        return {"dp": self.z + 1, "ctx": self.c}

    def below(self):
        return {"dp": self.z - 1, "ctx": self.c}

    def greet(self):
        barrier = pltpu.get_barrier_semaphore()
        for device in (self.first(), self.last(), self.sibling()):
            pl.semaphore_signal(barrier, inc=1, device_id=device, device_id_type=MESH)

        @pl.when(self.z > 0)
        def _():
            pl.semaphore_signal(barrier, inc=1, device_id=self.below(), device_id_type=MESH)

        @pl.when(self.z < self.depth - 1)
        def _():
            pl.semaphore_signal(barrier, inc=1, device_id=self.above(), device_id_type=MESH)

        ends = jnp.where(self.z > 0, 1, 0) + jnp.where(self.z < self.depth - 1, 1, 0)
        pl.semaphore_wait(barrier, 3 + ends)


def push(source, target, send, receive, device):
    return pltpu.make_async_remote_copy(
        src_ref=source, dst_ref=target, send_sem=send, recv_sem=receive, device_id=device, device_id_type=MESH
    )


def gather_kernel(depth, rows, own_ref, all_ref, local, sends, arrivals):
    me = Place(depth)
    last = depth - 1

    def block(shard):
        return all_ref.at[pl.ds(pl.multiple_of(shard * rows, rows), rows)]

    def send(source, shard, slot, device):
        push(source, block(shard), sends.at[slot], arrivals.at[shard], device).start()

    def drained(slot):
        push(own_ref, block(0), sends.at[slot], arrivals.at[0], me.sibling()).wait_send()

    def arrived(shard):
        push(own_ref, block(shard), sends.at[0], arrivals.at[shard], me.sibling()).wait_recv()

    me.greet()
    mine = me.shard(me.z, me.f, me.l, me.core)
    keep = pltpu.make_async_copy(own_ref, block(mine), local)
    send(own_ref, mine, 0, me.first())

    def spread(source, shard, base):
        @pl.when(me.z < last)
        def _():
            send(source, shard, base, me.above())

        @pl.when(me.z > 0)
        def _():
            send(source, shard, base + 1, me.below())

        send(source, shard, base + 2, me.last())
        send(source, shard, base + 3, me.sibling())

    spread(own_ref, mine, 1)
    keep.start()
    other = me.shard(me.z, 1 - me.f, me.l, me.core)
    arrived(other)
    spread(block(other), other, 5)

    def level(step):
        near = []
        for z in range(depth):
            order = sorted([q for q in range(depth) if q != z], key=lambda q: (abs(q - z), q))
            near.append(order)
        value = jnp.int32(0)
        for z in range(depth):
            value = jnp.where(me.z == z, near[z][step], value)
        return value

    def relay(shard, from_z, base):
        arrived(shard)

        @pl.when((from_z < me.z) & (me.z < last))
        def _():
            send(block(shard), shard, base, me.above())

        @pl.when((from_z > me.z) & (me.z > 0))
        def _():
            send(block(shard), shard, base, me.below())

        send(block(shard), shard, base + 1, me.last())
        send(block(shard), shard, base + 2, me.sibling())

    def cross(z, f, slot):
        shard = me.shard(z, f, 1 - me.l, me.core)
        arrived(shard)
        send(block(shard), shard, slot, me.sibling())

    base = 9
    cross(me.z, me.f, base)
    base += 1
    pending = (me.z, 1 - me.f)
    for step in range(last):
        z = level(step)
        for f in (me.f, 1 - me.f):
            relay(me.shard(z, f, me.l, me.core), z, base)
            base += 3
            cross(*pending, base)
            base += 1
            pending = (z, f)
    cross(*pending, base)
    base += 1
    for z in range(depth):
        for f in range(2):
            for l in range(2):
                arrived(me.shard(z, f, l, 1 - me.core))
    keep.wait()
    drained(0)
    for start in (1, 5):

        @pl.when(me.z < last)
        def _():
            drained(start)

        @pl.when(me.z > 0)
        def _():
            drained(start + 1)

        drained(start + 2)
        drained(start + 3)
    slot = 9
    drained(slot)
    slot += 1
    for step in range(last):
        z = level(step)
        for _ in range(2):

            @pl.when(((z < me.z) & (me.z < last)) | ((z > me.z) & (me.z > 0)))
            def _():
                drained(slot)

            drained(slot + 1)
            drained(slot + 2)
            drained(slot + 3)
            slot += 4
    drained(slot)


def gather_all(own, depth, collective_id):
    rows, width = own.shape
    devices = depth * 8
    slots = 9 + 1 + 8 * (depth - 1) + 1
    return pl.pallas_call(
        functools.partial(gather_kernel, depth, rows),
        out_shape=jax.ShapeDtypeStruct((devices * rows, width), own.dtype),
        in_specs=[pl.BlockSpec(memory_space=pl.ANY)],
        out_specs=pl.BlockSpec(memory_space=pl.ANY),
        scratch_shapes=[
            pltpu.SemaphoreType.DMA(()),
            pltpu.SemaphoreType.DMA((slots,)),
            pltpu.SemaphoreType.DMA((devices,)),
        ],
        compiler_params=pltpu.CompilerParams(collective_id=collective_id, has_side_effects=True),
    )(own)


def add_into(target, source, rows, step):
    @pl.loop(0, rows // step)
    def _(i):
        part = pl.ds(pl.multiple_of(i * step, step), step)
        target[part, :] = (target[part, :].astype(jnp.float32) + source[part, :].astype(jnp.float32)).astype(
            target.dtype
        )


def scatter_kernel(depth, rows, part_ref, out_ref, sums, from_sib, from_last, from_below, from_above, from_first,
                   loads, send_sib, send_last, send_line, send_first, got_sib, got_last, got_below, got_above, got_first):
    me = Place(depth)
    last = depth - 1
    step = min(rows, 16)

    def source(z, f, l, core):
        return part_ref.at[pl.ds(pl.multiple_of(me.shard(z, f, l, core) * rows, rows), rows)]

    def at(z, f, l):
        return z * 4 + f * 2 + l

    def order(i):
        value = jnp.int32(0)
        for z in range(depth):
            far = [q for q in range(depth - 1, z, -1)] + [q for q in range(z)] if 2 * z < depth else [q for q in range(z)] + [q for q in range(depth - 1, z, -1)]
            value = jnp.where(me.z == z, (far + [z])[i], value)
        return value

    me.greet()
    pairs = [(f, l) for l in (1 - me.l, me.l) for f in (1 - me.f, me.f)]
    for i in range(depth):
        z = order(i)
        for f in (1 - me.f, me.f):
            for l in (1 - me.l, me.l):
                push(source(z, f, l, 1 - me.core), from_sib.at[at(z, l, f)], send_sib.at[at(z, f, l)], got_sib.at[at(z, l, f)], me.sibling()).start()
        for f, l in pairs:
            pltpu.make_async_copy(source(z, f, l, me.core), sums.at[at(z, f, l)], loads.at[at(z, f, l)]).start()

    def chip(i):
        z = order(i)
        for n, (f, l) in enumerate(pairs):
            k = at(z, f, l)
            pltpu.make_async_copy(source(z, f, l, me.core), sums.at[k], loads.at[k]).wait()
            push(source(z, f, l, me.core), from_sib.at[k], send_sib.at[k], got_sib.at[k], me.sibling()).wait_recv()
            add_into(sums.at[k], from_sib.at[k], rows, step)
            if n in (1, 2):
                f0 = pairs[n - 1][0]
                push(sums.at[at(z, f0, 1 - me.l)], from_last.at[z * 2 + f0], send_last.at[z * 2 + f0], got_last.at[z * 2 + f0], me.last()).start()

    def up(z, f):
        return push(sums.at[at(z, f, me.l)], from_below.at[z * 2 + f], send_line.at[z * 2 + f], got_below.at[z * 2 + f], me.above())

    def down(z, f):
        return push(sums.at[at(z, f, me.l)], from_above.at[z * 2 + f], send_line.at[z * 2 + f], got_above.at[z * 2 + f], me.below())

    def plane(i):
        z = order(i)
        for f in (1 - me.f, me.f):
            k = at(z, f, me.l)
            push(sums.at[k], from_last.at[z * 2 + f], send_last.at[z * 2 + f], got_last.at[z * 2 + f], me.last()).wait_recv()
            add_into(sums.at[k], from_last.at[z * 2 + f], rows, step)
        for f in (1 - me.f, me.f):
            k = at(z, f, me.l)
            if i < last:

                @pl.when((z > me.z) & (me.z > 0))
                def _():
                    up(z, f).wait_recv()
                    add_into(sums.at[k], from_below.at[z * 2 + f], rows, step)

                @pl.when((z < me.z) & (me.z < last))
                def _():
                    down(z, f).wait_recv()
                    add_into(sums.at[k], from_above.at[z * 2 + f], rows, step)

                @pl.when(z > me.z)
                def _():
                    up(z, f).start()

                @pl.when(z < me.z)
                def _():
                    down(z, f).start()
            else:

                @pl.when(me.z > 0)
                def _():
                    up(z, f).wait_recv()
                    add_into(sums.at[k], from_below.at[z * 2 + f], rows, step)

                @pl.when(me.z < last)
                def _():
                    down(z, f).wait_recv()
                    add_into(sums.at[k], from_above.at[z * 2 + f], rows, step)

    chip(0)
    for i in range(1, depth):
        chip(i)
        plane(i - 1)
    plane(last)
    give = push(sums.at[at(me.z, 1 - me.f, me.l)], from_first, send_first, got_first, me.first())
    give.start()
    give.wait_recv()
    mine = sums.at[at(me.z, me.f, me.l)]

    @pl.loop(0, rows // step)
    def _(i):
        part = pl.ds(pl.multiple_of(i * step, step), step)
        out_ref[part, :] = (mine[part, :].astype(jnp.float32) + from_first[part, :].astype(jnp.float32)).astype(out_ref.dtype)

    give.wait_send()
    for i in range(depth):
        z = order(i)
        for f, l in pairs:
            k = at(z, f, l)
            push(source(z, f, l, 1 - me.core), from_sib.at[k], send_sib.at[k], got_sib.at[k], me.sibling()).wait_send()
        for f in (1 - me.f, me.f):
            push(sums.at[at(z, f, 1 - me.l)], from_last.at[z * 2 + f], send_last.at[z * 2 + f], got_last.at[z * 2 + f], me.last()).wait_send()
            if i < last:
                up(z, f).wait_send()


def scatter_sum(part, depth, collective_id, out_dtype):
    tokens, width = part.shape
    devices = depth * 8
    rows = tokens // devices
    shard = (rows, width)
    dma = pltpu.SemaphoreType.DMA
    return pl.pallas_call(
        functools.partial(scatter_kernel, depth, rows),
        out_shape=jax.ShapeDtypeStruct(shard, out_dtype),
        in_specs=[pl.BlockSpec(memory_space=pl.ANY)],
        out_specs=pl.BlockSpec(memory_space=pltpu.VMEM),
        scratch_shapes=[
            pltpu.VMEM((depth * 4, *shard), part.dtype),
            pltpu.VMEM((depth * 4, *shard), part.dtype),
            pltpu.VMEM((depth * 2, *shard), part.dtype),
            pltpu.VMEM((depth * 2, *shard), part.dtype),
            pltpu.VMEM((depth * 2, *shard), part.dtype),
            pltpu.VMEM(shard, part.dtype),
            dma((depth * 4,)), dma((depth * 4,)), dma((depth * 2,)), dma((depth * 2,)), dma(()),
            dma((depth * 4,)), dma((depth * 2,)), dma((depth * 2,)), dma((depth * 2,)), dma(()),
        ],
        compiler_params=pltpu.CompilerParams(collective_id=collective_id, has_side_effects=True, vmem_limit_bytes=60 << 20),
    )(part)


def layer_norm_stats(inputs):
    average = jnp.mean(inputs, -1, keepdims=True)
    centred = inputs - average
    inv_std = lax.rsqrt(jnp.mean(centred * centred, -1, keepdims=True) + epsilon)
    return centred * inv_std, inv_std


def exchange(blocks):
    return lax.all_to_all(blocks, AXES, split_axis=0, concat_axis=0, tiled=True)


def to_blocks(rows, parts, count, width):
    depth = rows.shape[0]
    return rows.reshape(depth, parts, count, width).transpose(2, 0, 1, 3).reshape(count, depth, parts * width)


def from_blocks(blocks, parts, width):
    count, depth, _ = blocks.shape
    return blocks.reshape(count, depth, parts, width).transpose(1, 2, 0, 3).reshape(depth, parts * count * width)


def attention(queries, keys, values, d_out, seg_all):
    seq_len = seg_all.shape[1]
    scaling = HD ** (-0.5)
    index = jnp.arange(seq_len)
    allowed = (seg_all[:, :, None] == seg_all[:, None, :]) & (index[:, None] >= index[None, :])[None]
    scores = jnp.einsum("bqd,bkd->bqk", queries, keys, preferred_element_type=jnp.float32) * scaling
    scores = jnp.where(allowed, scores, negative)
    largest = jnp.max(scores, -1, keepdims=True)
    weights = jnp.where(allowed, jnp.exp(scores - largest), 0.0)
    weights = weights / jnp.sum(weights, -1, keepdims=True)
    weights_low = weights.astype(jnp.bfloat16)
    attended = jnp.einsum("bqk,bkd->bqd", weights_low, values, preferred_element_type=jnp.float32)
    row_dots = jnp.sum(d_out.astype(jnp.float32) * attended, -1, keepdims=True)
    d_weights = jnp.einsum("bqd,bkd->bqk", d_out, values, preferred_element_type=jnp.float32)
    d_scores = (weights * (d_weights - row_dots)).astype(jnp.bfloat16)
    d_query = jnp.einsum("bqk,bkd->bqd", d_scores, keys, preferred_element_type=jnp.float32) * scaling
    d_key = jnp.einsum("bqk,bqd->bkd", d_scores, queries, preferred_element_type=jnp.float32) * scaling
    d_value = jnp.einsum("bqk,bqd->bkd", weights_low, d_out, preferred_element_type=jnp.float32)
    return attended, d_query, d_key, d_value


def rotate_rows(rows, cosine, sine, direction):
    half = ROT // 2
    first, second = rows[:, :half], rows[:, half:ROT]
    return jnp.concatenate(
        [first * cosine - direction * second * sine, second * cosine + direction * first * sine, rows[:, ROT:]], 1
    )


def on_device(
    hidden_in, w_in_t, in_bias, ln_gain, ln_shift, w_out_t, out_bias, segment_ids, out_grad
):
    depth = lax.axis_size("dp")
    devices = depth * lax.axis_size("ctx")
    ctx = lax.axis_index("ctx")
    me = lax.axis_index("dp") * lax.axis_size("ctx") + ctx
    tok_rows, model_width = hidden_in.shape[1:]
    seq_len = segment_ids.shape[1]
    tokens = devices * tok_rows
    seqs = tokens // seq_len
    own = model_width // devices
    in_parts = in_bias.shape[0]
    in_width = in_parts * own
    out_parts = w_out_t.shape[1] // model_width
    out_width = out_parts * own
    own_seg = lax.dynamic_slice_in_dim(segment_ids[0], ctx * tok_rows, tok_rows)
    extra = jnp.concatenate(
        [ln_gain.T, ln_shift.T, own_seg.astype(jnp.bfloat16).reshape(own, tok_rows // own)], 1
    )
    extra = jnp.broadcast_to(extra[None], (devices, *extra.shape))
    in_blocks = jnp.concatenate([to_blocks(w_in_t.T, in_parts, devices, own), extra], 2)
    in_got = exchange(in_blocks)
    w_in = in_got[:, :, :in_width].reshape(model_width, in_width)
    gain = in_got[:, :, in_width].reshape(1, model_width).astype(jnp.float32)
    shift = in_got[:, :, in_width + 1].reshape(1, model_width).astype(jnp.float32)
    seg_all = in_got[:, :, in_width + 2 :].astype(jnp.int32).reshape(seqs, seq_len)
    w_out = exchange(to_blocks(w_out_t, out_parts, devices, own)).reshape(model_width, out_width)
    x_all = gather_all(hidden_in[0], depth, 0)
    g_all = lax.all_gather(out_grad[0], AXES, axis=0, tiled=True)

    index_all = jnp.arange(seq_len, dtype=jnp.int32)[None]
    earlier = jnp.concatenate([seg_all[:, :1], seg_all[:, :-1]], 1)
    begins = jnp.where((index_all == 0) | (seg_all != earlier), index_all, 0)
    positions = (index_all - lax.cummax(begins, axis=1)).astype(jnp.float32).reshape(tokens)
    half = ROT // 2
    frequency = 10000.0 ** (-2.0 * jnp.arange(half, dtype=jnp.float32) / ROT)
    angles = positions[:, None] * frequency[None, :]
    cosine, sine = jnp.cos(angles), jnp.sin(angles)

    hat_all, _ = layer_norm_stats(x_all.astype(jnp.float32))
    normed = (hat_all * gain + shift).astype(jnp.bfloat16)
    joint = jnp.dot(normed, w_in, preferred_element_type=jnp.float32)
    joint = joint + in_bias.astype(jnp.float32).reshape(1, in_width)
    shape = (seqs, seq_len, HD)
    queries = rotate_rows(joint[:, :own], cosine, sine, 1.0).astype(jnp.bfloat16)
    keys = rotate_rows(joint[:, own : 2 * own], cosine, sine, 1.0).astype(jnp.bfloat16)
    values = joint[:, 2 * own : 3 * own].astype(jnp.bfloat16)
    pre_gelu = joint[:, 3 * own :]

    d_joined = jnp.dot(g_all, w_out, preferred_element_type=jnp.float32)
    d_attn = d_joined[:, :own].astype(jnp.bfloat16)
    hidden, gelu_pull = jax.vjp(lambda t: jax.nn.gelu(t, approximate=True), pre_gelu)
    d_pre = gelu_pull(d_joined[:, own:])[0]

    attended, d_query, d_key, d_value = attention(
        queries.reshape(shape), keys.reshape(shape), values.reshape(shape), d_attn.reshape(shape), seg_all
    )
    joined = jnp.concatenate([attended.reshape(tokens, own).astype(jnp.bfloat16), hidden.astype(jnp.bfloat16)], 1)

    branch = lax.dot_general(joined, w_out, (((1,), (1,)), ((), ())), preferred_element_type=jnp.float32)
    column = jnp.arange(model_width) // own
    bias_row = jnp.where(column == me, jnp.tile(out_bias.astype(jnp.float32), devices), 0.0)
    branch = (branch + bias_row[None]).astype(jnp.bfloat16)
    branch_own = lax.psum_scatter(branch, AXES, scatter_dimension=0, tiled=True)
    inputs = hidden_in[0].astype(jnp.float32)
    result = (inputs + branch_own.astype(jnp.float32)).astype(jnp.bfloat16)

    d_joint = jnp.concatenate(
        [
            rotate_rows(d_query.reshape(tokens, own), cosine, sine, -1.0),
            rotate_rows(d_key.reshape(tokens, own), cosine, sine, -1.0),
            d_value.reshape(tokens, own),
            d_pre,
        ],
        1,
    )
    d_joint = d_joint.astype(jnp.bfloat16)
    d_normed_part = lax.dot_general(
        d_joint, w_in, (((1,), (1,)), ((), ())), preferred_element_type=jnp.float32
    ).astype(jnp.bfloat16)

    grad_out_local = lax.dot_general(
        g_all, joined, (((0,), (0,)), ((), ())), preferred_element_type=jnp.float32
    ).astype(jnp.bfloat16)
    grad_w_out = from_blocks(exchange(grad_out_local.reshape(devices, own, out_width)), out_parts, own).astype(
        jnp.float32
    )
    grad_in_local = lax.dot_general(
        normed, d_joint, (((0,), (0,)), ((), ())), preferred_element_type=jnp.float32
    )
    joint_sums = jnp.sum(d_joint.astype(jnp.float32), 0)
    grad_in_bias = joint_sums.reshape(in_parts, own)
    weight_in = w_in.astype(jnp.float32)
    shift_part = jnp.sum(weight_in * joint_sums[None], 1)
    gain_part = (jnp.sum(weight_in * grad_in_local, 1) - shift[0] * shift_part) / gain[0]
    back = jnp.concatenate(
        [grad_in_local.astype(jnp.bfloat16), gain_part[:, None].astype(jnp.bfloat16), shift_part[:, None].astype(jnp.bfloat16)], 1
    )
    back = exchange(back.reshape(devices, own, in_width + 2))
    grad_w_in = from_blocks(back[:, :, :in_width], in_parts, own).astype(jnp.float32).T
    grad_gain, grad_shift = [
        jnp.sum(back[:, :, in_width + i].astype(jnp.float32), 0, keepdims=True) for i in range(2)
    ]
    g_columns = lax.dynamic_slice_in_dim(g_all, me * own, own, 1)
    grad_out_bias = jnp.sum(g_columns.astype(jnp.float32), 0)

    d_normed = scatter_sum(d_normed_part, depth, 1, jnp.float32)
    hat, inv_std = layer_norm_stats(inputs)
    d_hat = d_normed * gain
    d_input = inv_std * (
        d_hat - jnp.mean(d_hat, -1, keepdims=True) - hat * jnp.mean(d_hat * hat, -1, keepdims=True)
    ) + out_grad[0].astype(jnp.float32)
    return (
        result[None],
        d_input[None],
        grad_w_in,
        grad_in_bias,
        grad_gain,
        grad_shift,
        grad_w_out,
        grad_out_bias,
    )


def solution(mesh):
    in_specs = (
        P("dp", "ctx", None),
        P(None, ("dp", "ctx")),
        P(None, ("dp", "ctx")),
        P(None, ("dp", "ctx")),
        P(None, ("dp", "ctx")),
        P(("dp", "ctx"), None),
        P(("dp", "ctx")),
        P("dp", None),
        P("dp", "ctx", None),
    )
    out_specs = (
        P("dp", "ctx", None),
        P("dp", "ctx", None),
        P(None, ("dp", "ctx")),
        P(None, ("dp", "ctx")),
        P(None, ("dp", "ctx")),
        P(None, ("dp", "ctx")),
        P(("dp", "ctx"), None),
        P(("dp", "ctx")),
    )
    tensor_parallel = mesh.shape["ctx"] == 8 and mesh.shape["dp"] * 8 == H
    body = on_device if tensor_parallel else on_device_gathered
    return jax.shard_map(
        body, mesh=mesh, in_specs=in_specs, out_specs=out_specs, check_vma=False
    )
```

```python
import functools
import math

import jax
import jax.numpy as jnp
from jax import lax
from jax.experimental import pallas as pl
from jax.experimental.pallas import tpu as pltpu
from jax.sharding import PartitionSpec as P

H = 32
HD = 64
ROT = 32
KEY_BLOCK = 512


epsilon = 1e-05
negative = -1e30


def rotation_tables(positions):
    half_dims = ROT // 2
    frequency = 10000.0 ** (-2.0 * jnp.arange(half_dims, dtype=jnp.float32) / ROT)
    angles = positions[:, None] * frequency[None, :]
    return (jnp.cos(angles)[:, None, :], jnp.sin(angles)[:, None, :])


def rotate(heads_in, cosine_table, sine_table, direction):
    half_dims = ROT // 2
    first_half = heads_in[..., :half_dims]
    second_half = heads_in[..., half_dims:ROT]
    return jnp.concatenate(
        [
            first_half * cosine_table - direction * second_half * sine_table,
            second_half * cosine_table + direction * first_half * sine_table,
            heads_in[..., ROT:],
        ],
        -1,
    )


def masked_scores(queries, key_rows, key_seg, key_index, query_seg, query_index):
    scaling = queries.shape[2] ** (-0.5)
    scores = (
        jnp.einsum("thd,khd->htk", queries, key_rows, preferred_element_type=jnp.float32) * scaling
    )
    allowed = (query_seg[:, None] == key_seg[None, :]) & (
        query_index[:, None] >= key_index[None, :]
    )
    return (jnp.where(allowed[None], scores, negative), allowed)


def score_grads(
    query_part,
    dout_part,
    lse_part,
    dot_part,
    query_seg,
    query_index,
    key_rows,
    value_rows,
    key_seg,
    key_index,
):
    scores, allowed = masked_scores(
        query_part, key_rows, key_seg, key_index, query_seg, query_index
    )
    weights = jnp.where(allowed[None], jnp.exp(scores - lse_part[..., None]), 0.0)
    d_weights = jnp.einsum(
        "thd,khd->htk", dout_part, value_rows, preferred_element_type=jnp.float32
    )
    d_scores = (weights * (d_weights - dot_part[..., None])).astype(jnp.bfloat16)
    return (weights.astype(jnp.bfloat16), d_scores)


def key_grads(
    key_rows,
    value_rows,
    key_seg,
    key_index,
    query_src,
    dout_src,
    lse_src,
    dot_src,
    seg_src,
    index_src,
    query_block,
):
    key_count = key_rows.shape[0]
    scaling = HD ** (-0.5)
    block_count = query_src.shape[0] // query_block

    def query_step(running, block_no):
        weights_low, d_scores = score_grads(
            query_src,
            dout_src,
            lse_src,
            dot_src,
            seg_src,
            index_src,
            key_rows,
            value_rows,
            key_seg,
            key_index,
        )
        d_key = (
            running[0]
            + jnp.einsum("htk,thd->khd", d_scores, query_src, preferred_element_type=jnp.float32)
            * scaling
        )
        d_value = running[1] + jnp.einsum(
            "htk,thd->khd", weights_low, dout_src, preferred_element_type=jnp.float32
        )
        return ((d_key, d_value), None)

    zero_heads = jnp.zeros((key_count, H, HD), jnp.float32)
    (d_key, d_value), _ = lax.scan(query_step, (zero_heads, zero_heads), jnp.arange(block_count))
    return (d_key.reshape(key_count, H * HD), d_value.reshape(key_count, H * HD))


def on_device_gathered(
    hidden_in, w_in_t, in_bias, ln_gain, ln_shift, w_out_t, out_bias, segment_ids, out_grad
):
    inputs = hidden_in[0].astype(jnp.float32)
    tok_rows, model_width = inputs.shape
    seg_row = segment_ids[0]
    seq_len = seg_row.shape[0]
    offset = lax.axis_index("ctx") * tok_rows
    index_all = jnp.arange(seq_len, dtype=jnp.int32)
    earlier = jnp.concatenate([seg_row[:1], seg_row[:-1]])
    begins = jnp.where((index_all == 0) | (seg_row != earlier), index_all, 0)
    positions = (index_all - lax.cummax(begins, axis=0)).astype(jnp.float32)
    local_pos = lax.dynamic_slice_in_dim(positions, offset, tok_rows)
    query_seg = lax.dynamic_slice_in_dim(seg_row, offset, tok_rows)
    query_index = offset + jnp.arange(tok_rows, dtype=jnp.int32)
    cosine_table, sine_table = rotation_tables(local_pos)
    scaling = HD ** (-0.5)
    average = jnp.mean(inputs, -1, keepdims=True)
    centred = inputs - average
    inv_std = lax.rsqrt(jnp.mean(centred * centred, -1, keepdims=True) + epsilon)
    normed_hat = centred * inv_std
    joint_width = w_in_t.shape[0]
    bias_rows = in_bias.shape[0]
    weight_piece = lax.all_gather(w_in_t, ("dp", "ctx"), axis=1, tiled=True)
    bias_piece = lax.all_gather(in_bias, ("dp", "ctx"), axis=1, tiled=True)
    gain_piece = lax.all_gather(ln_gain, ("dp", "ctx"), axis=1, tiled=True)
    shift_piece = lax.all_gather(ln_shift, ("dp", "ctx"), axis=1, tiled=True)
    normed_piece = (
        normed_hat * gain_piece.astype(jnp.float32) + shift_piece.astype(jnp.float32)
    ).astype(jnp.bfloat16)
    summed = lax.dot_general(
        normed_piece, weight_piece, (((1,), (1,)), ((), ())), preferred_element_type=jnp.float32
    )
    gain_all = gain_piece.astype(jnp.float32)
    bias_all = bias_piece.astype(jnp.float32)
    projected, normed, gain_all, bias_all = (summed, normed_piece, gain_all, bias_all)
    projected = projected + bias_all.reshape(1, joint_width)
    queries = rotate(
        projected[:, :model_width].reshape(tok_rows, H, HD), cosine_table, sine_table, 1.0
    ).astype(jnp.bfloat16)
    keys_new = (
        rotate(
            projected[:, model_width : 2 * model_width].reshape(tok_rows, H, HD),
            cosine_table,
            sine_table,
            1.0,
        )
        .astype(jnp.bfloat16)
        .reshape(tok_rows, model_width)
    )
    values_new = projected[:, 2 * model_width : 3 * model_width].astype(jnp.bfloat16)
    pre_gelu = projected[:, 3 * model_width :]
    keys_all, values_all = (
        lax.all_gather(keys_new, "ctx", axis=0, tiled=True),
        lax.all_gather(values_new, "ctx", axis=0, tiled=True),
    )
    block_count = seq_len // KEY_BLOCK

    def key_slice(first_key, key_count):
        key_rows = lax.dynamic_slice_in_dim(keys_all, first_key, key_count, 0).reshape(
            key_count, H, HD
        )
        value_rows = lax.dynamic_slice_in_dim(values_all, first_key, key_count, 0).reshape(
            key_count, H, HD
        )
        key_seg = lax.dynamic_slice_in_dim(seg_row, first_key, key_count)
        key_index = first_key + jnp.arange(key_count, dtype=jnp.int32)
        return (key_rows, value_rows, key_seg, key_index)

    def stats_step(running, block_no):
        running_max, running_sum = running
        key_rows, value_rows, key_seg, key_index = key_slice(block_no * KEY_BLOCK, KEY_BLOCK)
        scores, allowed = masked_scores(
            queries, key_rows, key_seg, key_index, query_seg, query_index
        )
        new_max = jnp.maximum(running_max, jnp.max(scores, -1))
        weights = jnp.where(allowed[None], jnp.exp(scores - new_max[..., None]), 0.0)
        running_sum = running_sum * jnp.exp(running_max - new_max) + jnp.sum(weights, -1)
        return ((new_max, running_sum), None)

    stats_init = (
        jnp.full((H, tok_rows), negative, jnp.float32),
        jnp.zeros((H, tok_rows), jnp.float32),
    )
    (final_max, final_sum), _ = lax.scan(stats_step, stats_init, jnp.arange(block_count))
    log_total = final_max + jnp.log(final_sum)

    def value_step(attended, block_no):
        key_rows, value_rows, key_seg, key_index = key_slice(block_no * KEY_BLOCK, KEY_BLOCK)
        scores, allowed = masked_scores(
            queries, key_rows, key_seg, key_index, query_seg, query_index
        )
        weights = jnp.where(allowed[None], jnp.exp(scores - log_total[..., None]), 0.0).astype(
            jnp.bfloat16
        )
        attended = attended + jnp.einsum(
            "htk,khd->thd", weights, value_rows, preferred_element_type=jnp.float32
        )
        return (attended, None)

    attended, _ = lax.scan(
        value_step, jnp.zeros((tok_rows, H, HD), jnp.float32), jnp.arange(block_count)
    )
    hidden = jax.nn.gelu(pre_gelu, approximate=True).astype(jnp.bfloat16)
    joined = jnp.concatenate(
        [attended.reshape(tok_rows, model_width).astype(jnp.bfloat16), hidden], 1
    )
    weight_piece, bias_piece = lax.all_gather(
        (w_out_t, out_bias), ("dp", "ctx"), axis=0, tiled=True
    )
    branch = (
        lax.dot_general(
            joined, weight_piece, (((1,), (1,)), ((), ())), preferred_element_type=jnp.float32
        )
        + bias_piece.astype(jnp.float32)[None, :]
    )
    result = (inputs + branch).astype(jnp.bfloat16)
    cotangent = out_grad[0]
    grad_part = cotangent
    d_joined = jnp.dot(
        grad_part,
        lax.all_gather(w_out_t, ("dp", "ctx"), axis=0, tiled=True),
        preferred_element_type=jnp.float32,
    )
    d_attn = d_joined[:, :model_width].astype(jnp.bfloat16).reshape(tok_rows, H, HD)

    def gelu_tanh(pre_values):
        return jax.nn.gelu(pre_values, approximate=True)

    _, gelu_pull = jax.vjp(gelu_tanh, pre_gelu)
    d_pre = gelu_pull(d_joined[:, model_width:])[0]
    row_dots = jnp.einsum("thd,thd->ht", d_attn.astype(jnp.float32), attended)

    def query_grad_step(d_query, block_no):
        key_rows, value_rows, key_seg, key_index = key_slice(block_no * KEY_BLOCK, KEY_BLOCK)
        _, d_scores = score_grads(
            queries,
            d_attn,
            log_total,
            row_dots,
            query_seg,
            query_index,
            key_rows,
            value_rows,
            key_seg,
            key_index,
        )
        d_query = (
            d_query
            + jnp.einsum("htk,khd->thd", d_scores, key_rows, preferred_element_type=jnp.float32)
            * scaling
        )
        return (d_query, None)

    d_query, _ = lax.scan(
        query_grad_step, jnp.zeros((tok_rows, H, HD), jnp.float32), jnp.arange(block_count)
    )
    count = lax.axis_size("ctx") * tok_rows
    sub_rows = math.gcd(count, KEY_BLOCK)

    def sub_step(carry_none, block_no):
        key_rows, value_rows, key_seg, key_index = key_slice(block_no * sub_rows, sub_rows)
        d_key, d_value = key_grads(
            key_rows,
            value_rows,
            key_seg,
            key_index,
            queries,
            d_attn,
            log_total,
            row_dots,
            query_seg,
            query_index,
            tok_rows,
        )
        return (carry_none, jnp.concatenate([d_key, d_value], 1))

    _, stacked = lax.scan(sub_step, jnp.zeros((), jnp.float32), jnp.arange(count // sub_rows))
    d_kv = lax.psum_scatter(
        stacked.reshape(count, 2 * model_width).astype(jnp.bfloat16),
        "ctx",
        scatter_dimension=0,
        tiled=True,
    ).astype(jnp.float32)
    d_key_local, d_value_local = (d_kv[:, :model_width], d_kv[:, model_width:])
    d_query_pre = rotate(d_query, cosine_table, sine_table, -1.0).reshape(tok_rows, model_width)
    d_key_pre = rotate(
        d_key_local.reshape(tok_rows, H, HD), cosine_table, sine_table, -1.0
    ).reshape(tok_rows, model_width)
    d_joint = jnp.concatenate([d_query_pre, d_key_pre, d_value_local, d_pre], 1).astype(
        jnp.bfloat16
    )
    d_normed = jnp.dot(
        d_joint,
        lax.all_gather(w_in_t, ("dp", "ctx"), axis=1, tiled=True),
        preferred_element_type=jnp.float32,
    )
    grad_part = cotangent
    in_term = lax.dot_general(
        normed, d_joint, (((0,), (0,)), ((), ())), preferred_element_type=jnp.float32
    )
    out_term = lax.dot_general(
        grad_part, joined, (((0,), (0,)), ((), ())), preferred_element_type=jnp.float32
    )
    grad_rows = lax.psum_scatter(
        jnp.concatenate([in_term, out_term], 1), ("dp", "ctx"), scatter_dimension=0, tiled=True
    )
    grad_w_in = grad_rows[:, :joint_width].T
    grad_w_out = grad_rows[:, joint_width:]
    grad_bias_in = jnp.sum(d_joint.astype(jnp.float32), 0).reshape(bias_rows, model_width)
    grad_gain_row = jnp.sum(d_normed * normed_hat, 0, keepdims=True)
    grad_shift_row = jnp.sum(d_normed, 0, keepdims=True)
    grad_bias_out = jnp.sum(cotangent.astype(jnp.float32), 0, keepdims=True)
    grad_in_bias, grad_gain, grad_shift, grad_out_row = (
        lax.psum_scatter(grad_bias_in, ("dp", "ctx"), scatter_dimension=1, tiled=True),
        lax.psum_scatter(grad_gain_row, ("dp", "ctx"), scatter_dimension=1, tiled=True),
        lax.psum_scatter(grad_shift_row, ("dp", "ctx"), scatter_dimension=1, tiled=True),
        lax.psum_scatter(grad_bias_out, ("dp", "ctx"), scatter_dimension=1, tiled=True),
    )
    d_hat = d_normed * gain_all
    d_input = inv_std * (
        d_hat
        - jnp.mean(d_hat, -1, keepdims=True)
        - normed_hat * jnp.mean(d_hat * normed_hat, -1, keepdims=True)
    ) + cotangent.astype(jnp.float32)
    return (
        result[None],
        d_input[None],
        grad_w_in,
        grad_in_bias,
        grad_gain,
        grad_shift,
        grad_w_out,
        grad_out_row[0],
    )


AXES = ("dp", "ctx")
MESH = pl.DeviceIdType.MESH
class Place:
    def __init__(self, depth):
        self.depth = depth
        self.top = depth - 1
        self.z = lax.axis_index("dp")
        self.c = lax.axis_index("ctx")
        y, x, self.core = self.c // 4, (self.c // 2) % 2, self.c % 2
        self.first_stride = jnp.where(self.core == 0, 2, 4)
        self.last_stride = jnp.where(self.core == 0, 4, 2)
        self.f = jnp.where(self.core == 0, x, y)
        self.l = jnp.where(self.core == 0, y, x)

    def ctx(self, f, l, core):
        return f * self.first_stride + l * self.last_stride + core

    def shard(self, z, f, l, core=None):
        return z * 8 + self.ctx(f, l, self.core if core is None else core)

    def first(self):
        return {"dp": self.z, "ctx": self.ctx(1 - self.f, self.l, self.core)}

    def last(self):
        return {"dp": self.z, "ctx": self.ctx(self.f, 1 - self.l, self.core)}

    def sibling(self):
        return {"dp": self.z, "ctx": self.ctx(self.f, self.l, 1 - self.core)}

    def above(self):
        return {"dp": self.z + 1, "ctx": self.c}

    def below(self):
        return {"dp": self.z - 1, "ctx": self.c}

    def greet(self):
        barrier = pltpu.get_barrier_semaphore()
        for device in (self.first(), self.last(), self.sibling()):
            pl.semaphore_signal(barrier, inc=1, device_id=device, device_id_type=MESH)

        @pl.when(self.z > 0)
        def _():
            pl.semaphore_signal(barrier, inc=1, device_id=self.below(), device_id_type=MESH)

        @pl.when(self.z < self.top)
        def _():
            pl.semaphore_signal(barrier, inc=1, device_id=self.above(), device_id_type=MESH)

        ends = jnp.where(self.z > 0, 1, 0) + jnp.where(self.z < self.top, 1, 0)
        pl.semaphore_wait(barrier, 3 + ends)

    def choose(self, rule):
        value = jnp.int32(0)
        for z in range(self.depth):
            value = jnp.where(self.z == z, rule(z), value)
        return value

    def near(self, step):
        return self.choose(lambda z: sorted([q for q in range(self.depth) if q != z], key=lambda q: (abs(q - z), q))[step])

    def far(self, step):
        def rule(z):
            ups, downs = list(range(self.top, z, -1)), list(range(z))
            return ((ups + downs if 2 * z < self.depth else downs + ups) + [z])[step]

        return self.choose(rule)


def push(source, target, send, receive, device):
    return pltpu.make_async_remote_copy(
        src_ref=source, dst_ref=target, send_sem=send, recv_sem=receive, device_id=device, device_id_type=MESH
    )


class Gather:
    def __init__(self, depth, rows, own_ref, all_ref, local, sends, arrivals):
        self.me, self.rows = Place(depth), rows
        self.own_ref, self.all_ref, self.sends, self.arrivals = own_ref, all_ref, sends, arrivals
        me = self.me
        self.keep = pltpu.make_async_copy(own_ref, self.block(me.shard(me.z, me.f, me.l)), local)
        self.used, self.drains = 0, []
        zs = [me.z] + [me.near(step) for step in range(depth - 1)]
        self.steps = [self.begin]
        crossings = [(z, f) for z in zs for f in (me.f, 1 - me.f)]
        relays = []
        for z in zs:
            if z is not me.z:
                relays.append(functools.partial(self.along_line, z))
            relays.append(functools.partial(self.along_first, z))
        for n, relay in enumerate(relays):
            self.steps += [relay, functools.partial(self.cross, *crossings[n])]
        self.steps.append(functools.partial(self.cross, *crossings[-1]))

    def block(self, shard):
        return self.all_ref.at[pl.ds(pl.multiple_of(shard * self.rows, self.rows), self.rows)]

    def send(self, source, shard, device, when=None):
        slot = self.used
        self.used += 1

        def start():
            push(source, self.block(shard), self.sends.at[slot], self.arrivals.at[shard], device).start()

        def drain():
            push(self.own_ref, self.block(0), self.sends.at[slot], self.arrivals.at[0], self.me.sibling()).wait_send()

        if when is None:
            start()
            self.drains.append(drain)
        else:
            pl.when(when())(start)
            self.drains.append(lambda: pl.when(when())(drain))

    def arrived(self, shard):
        push(self.own_ref, self.block(shard), self.sends.at[0], self.arrivals.at[shard], self.me.sibling()).wait_recv()

    def begin(self):
        me = self.me
        shard = me.shard(me.z, me.f, me.l)
        self.send(self.own_ref, shard, me.above(), lambda: me.z < me.top)
        self.send(self.own_ref, shard, me.below(), lambda: me.z > 0)
        self.send(self.own_ref, shard, me.first())
        self.send(self.own_ref, shard, me.last())
        self.send(self.own_ref, shard, me.sibling())
        self.keep.start()

    def along_line(self, z):
        me = self.me
        shard = me.shard(z, me.f, me.l)
        self.arrived(shard)
        self.send(self.block(shard), shard, me.above(), lambda: (z < me.z) & (me.z < me.top))
        self.send(self.block(shard), shard, me.below(), lambda: (z > me.z) & (me.z > 0))
        self.send(self.block(shard), shard, me.first())
        self.send(self.block(shard), shard, me.last())
        self.send(self.block(shard), shard, me.sibling())

    def along_first(self, z):
        me = self.me
        shard = me.shard(z, 1 - me.f, me.l)
        self.arrived(shard)
        self.send(self.block(shard), shard, me.last())
        self.send(self.block(shard), shard, me.sibling())

    def cross(self, z, f):
        me = self.me
        shard = me.shard(z, f, 1 - me.l)
        self.arrived(shard)
        self.send(self.block(shard), shard, me.sibling())

    def finish(self):
        me = self.me
        for z in range(me.depth):
            for f in range(2):
                for l in range(2):
                    self.arrived(me.shard(z, f, l, 1 - me.core))
        self.keep.wait()
        for drain in self.drains:
            drain()

    @staticmethod
    def scratch(depth):
        return [
            pltpu.SemaphoreType.DMA(()),
            pltpu.SemaphoreType.DMA((5 + 5 * (depth - 1) + 2 * depth + 2 * depth,)),
            pltpu.SemaphoreType.DMA((depth * 8,)),
        ]


def gather_kernel(depth, rows, own_ref, all_ref, *scratch):
    gather = Gather(depth, rows, own_ref, all_ref, *scratch)
    gather.me.greet()
    for step in gather.steps:
        step()
    gather.finish()


def gather_all(own, depth, collective_id):
    rows, width = own.shape
    return pl.pallas_call(
        functools.partial(gather_kernel, depth, rows),
        out_shape=jax.ShapeDtypeStruct((depth * 8 * rows, width), own.dtype),
        in_specs=[pl.BlockSpec(memory_space=pl.ANY)],
        out_specs=pl.BlockSpec(memory_space=pl.ANY),
        scratch_shapes=Gather.scratch(depth),
        compiler_params=pltpu.CompilerParams(collective_id=collective_id, has_side_effects=True),
    )(own)


class Scatter:
    def __init__(self, depth, rows, part_ref, out_ref, sums, from_sib, from_last, from_first, from_below, from_above,
                 loads, send_sib, send_last, send_first, send_line, got_sib, got_last, got_first, got_below, got_above):
        self.me, self.rows, self.step = Place(depth), rows, min(rows, 16)
        self.part_ref, self.out_ref, self.sums, self.loads = part_ref, out_ref, sums, loads
        self.sib, self.last, self.first = (from_sib, send_sib, got_sib), (from_last, send_last, got_last), (from_first, send_first, got_first)
        self.up, self.down = (from_below, send_line, got_below), (from_above, send_line, got_above)
        me = self.me
        self.zs = [me.far(i) for i in range(depth)]
        chip = [functools.partial(self.chip, z) for z in self.zs]
        plane = [functools.partial(self.plane, z) for z in self.zs]
        line = [functools.partial(self.line, z) for z in self.zs[:-1]] + [self.final]
        self.steps = [self.begin, chip[0]]
        for i in range(1, depth + 2):
            if i < depth:
                self.steps.append(chip[i])
            if i <= depth:
                self.steps.append(plane[i - 1])
            if i >= 2:
                self.steps.append(line[i - 2])

    def source(self, z, f, l, core):
        me = self.me
        return self.part_ref.at[pl.ds(pl.multiple_of(me.shard(z, f, l, core) * self.rows, self.rows), self.rows)]

    def at(self, z, f, l):
        return z * 4 + f * 2 + l

    def add(self, target, source):
        @pl.loop(0, self.rows // self.step)
        def _(i):
            part = pl.ds(pl.multiple_of(i * self.step, self.step), self.step)
            target[part, :] = (target[part, :].astype(jnp.float32) + source[part, :].astype(jnp.float32)).astype(target.dtype)

    def copy(self, stage, source, slot, device, send_slot=None):
        landing, send, got = stage
        return push(source, landing.at[slot], send.at[slot if send_slot is None else send_slot], got.at[slot], device)

    def to_sibling(self, z, f, l):
        return self.copy(self.sib, self.source(z, f, l, 1 - self.me.core), self.at(z, l, f), self.me.sibling())

    def to_last(self, z, f):
        me = self.me
        return self.copy(self.last, self.sums.at[self.at(z, f, 1 - me.l)], z * 2 + f, me.last())

    def to_first(self, z):
        me = self.me
        return self.copy(self.first, self.sums.at[self.at(z, 1 - me.f, me.l)], z, me.first())

    def mine(self, z):
        return self.sums.at[self.at(z, self.me.f, self.me.l)]

    def load(self, z, f, l):
        k = self.at(z, f, l)
        return pltpu.make_async_copy(self.source(z, f, l, self.me.core), self.sums.at[k], self.loads.at[k])

    def pairs(self):
        me = self.me
        return [(f, l) for l in (1 - me.l, me.l) for f in (1 - me.f, me.f)]

    def begin(self):
        me = self.me
        for z in self.zs:
            for f in (1 - me.f, me.f):
                for l in (1 - me.l, me.l):
                    self.to_sibling(z, f, l).start()
            for f, l in self.pairs():
                self.load(z, f, l).start()

    def chip(self, z):
        me = self.me
        for n, (f, l) in enumerate(self.pairs()):
            k = self.at(z, f, l)
            self.load(z, f, l).wait()
            self.copy(self.sib, self.sums.at[k], k, me.sibling()).wait_recv()
            self.add(self.sums.at[k], self.sib[0].at[k])
            if n in (1, 2):
                self.to_last(z, self.pairs()[n - 1][0]).start()

    def plane(self, z):
        me = self.me
        for f in (1 - me.f, me.f):
            k = self.at(z, f, me.l)
            self.to_last(z, f).wait_recv()
            self.add(self.sums.at[k], self.last[0].at[z * 2 + f])
        self.to_first(z).start()

    def line(self, z):
        me = self.me
        self.to_first(z).wait_recv()
        self.add(self.mine(z), self.first[0].at[z])
        upward, downward = self.copy(self.up, self.mine(z), z, me.above()), self.copy(self.down, self.mine(z), z, me.below())

        @pl.when((z > me.z) & (me.z > 0))
        def _():
            upward.wait_recv()
            self.add(self.mine(z), self.up[0].at[z])

        @pl.when((z < me.z) & (me.z < me.top))
        def _():
            downward.wait_recv()
            self.add(self.mine(z), self.down[0].at[z])

        @pl.when(z > me.z)
        def _():
            upward.start()

        @pl.when(z < me.z)
        def _():
            downward.start()

    def final(self):
        me = self.me
        z = me.z
        self.to_first(z).wait_recv()
        self.add(self.mine(z), self.first[0].at[z])

        @pl.when(z > 0)
        def _():
            self.copy(self.up, self.mine(z), z, me.above()).wait_recv()
            self.add(self.mine(z), self.up[0].at[z])

        @pl.when(z < me.top)
        def _():
            self.copy(self.down, self.mine(z), z, me.below()).wait_recv()
            self.add(self.mine(z), self.down[0].at[z])

        self.out_ref[...] = self.mine(z)[...].astype(self.out_ref.dtype)

    def finish(self):
        me = self.me
        for i, z in enumerate(self.zs):
            for f, l in self.pairs():
                self.to_sibling(z, f, l).wait_send()
            for f in (1 - me.f, me.f):
                self.to_last(z, f).wait_send()
            self.to_first(z).wait_send()
            if i < me.top:
                self.copy(self.up, self.mine(z), z, me.above()).wait_send()

    @staticmethod
    def scratch(depth, shard, dtype):
        dma = pltpu.SemaphoreType.DMA
        counts = [depth * 4, depth * 4, depth * 2, depth, depth, depth]
        sems = [depth * 4, depth * 4, depth * 2, depth, depth, depth * 4, depth * 2, depth, depth, depth]
        return [pltpu.VMEM((count, *shard), dtype) for count in counts] + [dma((count,)) for count in sems]


def scatter_kernel(depth, rows, part_ref, out_ref, *scratch):
    scatter = Scatter(depth, rows, part_ref, out_ref, *scratch)
    scatter.me.greet()
    for step in scatter.steps:
        step()
    scatter.finish()


def scatter_sum(part, depth, collective_id, out_dtype):
    tokens, width = part.shape
    rows = tokens // (depth * 8)
    return pl.pallas_call(
        functools.partial(scatter_kernel, depth, rows),
        out_shape=jax.ShapeDtypeStruct((rows, width), out_dtype),
        in_specs=[pl.BlockSpec(memory_space=pl.ANY)],
        out_specs=pl.BlockSpec(memory_space=pltpu.VMEM),
        scratch_shapes=Scatter.scratch(depth, (rows, width), part.dtype),
        compiler_params=pltpu.CompilerParams(collective_id=collective_id, has_side_effects=True, vmem_limit_bytes=48 << 20),
    )(part)


LANES = 128
NT = (((1,), (1,)), ((), ()))
TN = (((0,), (0,)), ((), ()))


def low_half(shape):
    return lax.broadcasted_iota(jnp.int32, shape, 1) < LANES // 2


def swap_halves(block):
    return pltpu.roll(block, LANES // 2, 1)


def split_kernel(parts, width, *refs):
    scale_ref, extra_ref, out_ref = refs[len(parts) :]
    depth = out_ref.shape[1]
    low = low_half((depth, LANES))

    @pl.loop(0, width // LANES)
    def _(m):
        base = 0
        for count, rows_ref in zip(parts, refs):
            for pair in range((count + 1) // 2):

                def piece(part):
                    lanes = pl.ds(pl.multiple_of(part * width + m * LANES, LANES), LANES)
                    values = rows_ref[:, lanes].astype(jnp.float32)
                    return values * scale_ref[...] if base == 0 else values

                first = piece(2 * pair)
                if 2 * pair + 1 < count:
                    second = piece(2 * pair + 1)
                    even = jnp.where(low, first, swap_halves(second))
                    odd = jnp.where(low, swap_halves(first), second)
                else:
                    rest = extra_ref[...] if base == 0 else jnp.zeros_like(first)
                    even = jnp.where(low, first, rest)
                    odd = jnp.where(low, swap_halves(first), rest)
                lanes = slice((base + pair) * LANES, (base + pair + 1) * LANES)
                out_ref[2 * m, :, lanes] = even.astype(out_ref.dtype)
                out_ref[2 * m + 1, :, lanes] = odd.astype(out_ref.dtype)
            base += (count + 1) // 2


def split_blocks(arrays, parts, scale, extra):
    depth = arrays[0].shape[0]
    width = arrays[0].shape[1] // parts[0]
    padded = sum((count + 1) // 2 for count in parts) * LANES
    return pl.pallas_call(
        functools.partial(split_kernel, parts, width),
        out_shape=jax.ShapeDtypeStruct((width // HD, depth, padded), arrays[0].dtype),
        in_specs=[pl.BlockSpec(memory_space=pltpu.VMEM)] * (len(parts) + 2),
        out_specs=pl.BlockSpec(memory_space=pltpu.VMEM),
        compiler_params=pltpu.CompilerParams(vmem_limit_bytes=24 << 20),
    )(*arrays, scale, extra)


def join_kernel(parts, width, blocks_ref, out_ref, extra_ref):
    depth = out_ref.shape[0]
    low = low_half((depth, LANES))
    extra_ref[...] = jnp.zeros_like(extra_ref)

    @pl.loop(0, width // LANES)
    def _(m):
        for pair in range((parts + 1) // 2):
            lanes = slice(pair * LANES, (pair + 1) * LANES)
            even = blocks_ref[2 * m, :, lanes].astype(jnp.float32)
            odd = blocks_ref[2 * m + 1, :, lanes].astype(jnp.float32)
            first = pl.ds(pl.multiple_of(2 * pair * width + m * LANES, LANES), LANES)
            out_ref[:, first] = jnp.where(low, even, swap_halves(odd))
            if 2 * pair + 1 < parts:
                second = pl.ds(pl.multiple_of((2 * pair + 1) * width + m * LANES, LANES), LANES)
                out_ref[:, second] = jnp.where(low, swap_halves(even), odd)
            else:
                extra_ref[...] += even + odd


def join_blocks(blocks, parts):
    count, depth, _ = blocks.shape
    width = count * HD
    return pl.pallas_call(
        functools.partial(join_kernel, parts, width),
        out_shape=(
            jax.ShapeDtypeStruct((depth, parts * width), jnp.float32),
            jax.ShapeDtypeStruct((depth, LANES), jnp.float32),
        ),
        in_specs=[pl.BlockSpec(memory_space=pltpu.VMEM)],
        out_specs=(pl.BlockSpec(memory_space=pltpu.VMEM), pl.BlockSpec(memory_space=pltpu.VMEM)),
        compiler_params=pltpu.CompilerParams(vmem_limit_bytes=24 << 20),
    )(blocks)


SIDE = 256


def turned(block, lane):
    shift = ROT // 2
    return jnp.where(lane % HD < shift, pltpu.roll(block, LANES - shift, 1), pltpu.roll(block, shift, 1))


def gelu(t):
    inner = math.sqrt(2.0 / math.pi) * (t + 0.044715 * (t * t * t))
    return 0.5 * t * (1.0 + jnp.tanh(inner))


def gelu_slope(t):
    slope = math.sqrt(2.0 / math.pi)
    bent = jnp.tanh(slope * (t + 0.044715 * (t * t * t)))
    return 0.5 * (1.0 + bent) + 0.5 * t * (1.0 - bent * bent) * slope * (1.0 + 3.0 * 0.044715 * (t * t))


def allowed_keys(start, first_query, keys):
    query = first_query + lax.broadcasted_iota(jnp.int32, (SIDE, keys), 0)
    key = lax.broadcasted_iota(jnp.int32, (SIDE, keys), 1)
    return (key >= start) & (key <= query)


def forward_kernel(depth, shard_rows, joint_width, hat_ref, weights_ref, bias_ref, cos_ref, sin_ref, start_ref, out_bias_ref, grad_ref,
                   qk_ref, mid_ref, joined_ref, out_ref, grads_ref, keys_ref, values_ref, *scratch):
    seq = hat_ref.shape[0]
    here = pl.program_id(0)
    low = low_half((SIDE, LANES))
    lane = lax.broadcasted_iota(jnp.int32, (SIDE, LANES), 1)
    scaling = HD ** (-0.5)
    gather = Gather(depth, shard_rows, grad_ref, grads_ref, *scratch)
    chunks = seq // SIDE
    slots = spread_steps([gather.me.greet] + gather.steps, depth * chunks, [gather.finish])
    for q in range(chunks):
        run_slots(slots, here, q, depth, chunks)
        rows = slice(q * SIDE, (q + 1) * SIDE)
        joint = jnp.dot(hat_ref[rows, :], weights_ref[:, :joint_width], preferred_element_type=jnp.float32) + bias_ref[...]
        qk = joint[:, :LANES]
        qk = (qk * cos_ref[rows, :] + turned(qk, lane) * sin_ref[rows, :])
        keys_ref[rows, :] = swap_halves(qk).astype(jnp.bfloat16)
        query = jnp.where(low, qk * scaling, 0.0).astype(jnp.bfloat16)
        qk_ref[rows, :] = qk.astype(jnp.bfloat16)
        values_ref[rows, :] = jnp.where(low, joint[:, LANES : 2 * LANES], 0.0).astype(jnp.bfloat16)
        count = (q + 1) * SIDE
        scores = lax.dot_general(query, keys_ref[:count, :], NT, preferred_element_type=jnp.float32)
        scores = jnp.where(allowed_keys(start_ref[rows, :], q * SIDE, count), scores, negative)
        largest = jnp.max(scores, -1, keepdims=True)
        weights = jnp.exp(scores - largest)
        total = jnp.sum(weights, -1, keepdims=True)
        weights = (weights * (1.0 / total)).astype(jnp.bfloat16)
        attended = jnp.dot(weights, values_ref[:count, :], preferred_element_type=jnp.float32)
        lse = largest + jnp.log(total)
        mid_ref[rows, : 2 * LANES] = joint[:, LANES : 3 * LANES]
        mid_ref[rows, 2 * LANES :] = jnp.where(low, joint[:, 3 * LANES :], lse)
        joined_ref[rows, :LANES] = jnp.where(low, attended, gelu(joint[:, LANES : 2 * LANES])).astype(jnp.bfloat16)
        joined_ref[rows, LANES : 2 * LANES] = gelu(joint[:, 2 * LANES : 3 * LANES]).astype(jnp.bfloat16)
        joined_ref[rows, 2 * LANES :] = jnp.where(low, gelu(joint[:, 3 * LANES :]), 0.0).astype(jnp.bfloat16)
        branch = lax.dot_general(joined_ref[rows, :], weights_ref[:, joint_width:], NT, preferred_element_type=jnp.float32)
        out_ref[rows, :] = (branch + out_bias_ref[...]).astype(jnp.bfloat16)

    @pl.when(here == pl.num_programs(0) - 1)
    def _():
        for step in slots[-1]:
            step()


def spread_steps(steps, count, after):
    slots = [[] for _ in range(count + 1)]
    for n, step in enumerate(steps):
        slots[max(n - 1, 0) * (count - 1) // max(len(steps) - 2, 1) if n else 0].append(step)
    slots[-1] = list(after)
    return slots


def run_slots(slots, here, q, blocks, chunks):
    for block in range(blocks):
        steps = slots[block * chunks + q]
        if steps:

            @pl.when(here == block)
            def _():
                for step in steps:
                    step()


def forward(hat_all, weights, joint_width, bias, cosine, sine, start, out_bias, grads, depth, seq, collective_id):
    tokens, width = hat_all.shape
    joined_width = weights.shape[1] - joint_width

    def rows(columns):
        return pl.BlockSpec((seq, columns), lambda b: (b, 0))

    def whole(array):
        return pl.BlockSpec(array.shape, lambda b: (0, 0), pipeline_mode=pl.Buffered(1))

    return pl.pallas_call(
        functools.partial(forward_kernel, depth, grads.shape[0], joint_width),
        grid=(tokens // seq,),
        out_shape=(
            jax.ShapeDtypeStruct((tokens, LANES), jnp.bfloat16),
            jax.ShapeDtypeStruct((tokens, joined_width), jnp.float32),
            jax.ShapeDtypeStruct((tokens, joined_width), jnp.bfloat16),
            jax.ShapeDtypeStruct((tokens, width), jnp.bfloat16),
            jax.ShapeDtypeStruct((tokens, width), jnp.bfloat16),
        ),
        in_specs=[rows(width), whole(weights), whole(bias), rows(LANES), rows(LANES), rows(1), whole(out_bias), pl.BlockSpec(memory_space=pl.ANY)],
        out_specs=(rows(LANES), rows(joined_width), rows(joined_width), rows(width), pl.BlockSpec(memory_space=pl.ANY)),
        scratch_shapes=[pltpu.VMEM((seq, LANES), jnp.bfloat16), pltpu.VMEM((seq, LANES), jnp.bfloat16)] + Gather.scratch(depth),
        compiler_params=pltpu.CompilerParams(collective_id=collective_id, has_side_effects=True, vmem_limit_bytes=56 << 20),
    )(hat_all, weights, bias, cosine, sine, start, out_bias, grads)


def backward_kernel(depth, shard_rows, joint_width, grad_ref, weights_ref, qk_ref, mid_ref, cos_ref, sin_ref, start_ref, branch_ref,
                    d_joint_ref, d_hat_ref, sums_ref, own_ref, keys_ref, values_ref, d_key_ref, d_value_ref, d_query_ref, *scratch):
    seq = grad_ref.shape[0]
    low = low_half((SIDE, LANES))
    lane = lax.broadcasted_iota(jnp.int32, (SIDE, LANES), 1)
    scaling = HD ** (-0.5)
    d_key_ref[...] = jnp.zeros_like(d_key_ref)
    d_value_ref[...] = jnp.zeros_like(d_value_ref)

    here = pl.program_id(0)
    scatter = Scatter(depth, shard_rows, branch_ref, own_ref, *scratch)
    chunks = seq // SIDE
    slots = spread_steps([scatter.me.greet] + scatter.steps, depth * 2 * chunks, [scatter.finish])

    @pl.when(here == 0)
    def _():
        sums_ref[...] = jnp.zeros_like(sums_ref)

    for q in range(chunks):
        run_slots(slots, here, q, depth, 2 * chunks)
        rows = slice(q * SIDE, (q + 1) * SIDE)
        d_joined = jnp.dot(grad_ref[rows, :], weights_ref[:, joint_width:], preferred_element_type=jnp.float32)
        qk = qk_ref[rows, :].astype(jnp.float32)
        keys_ref[rows, :] = jnp.where(low, swap_halves(qk), 0.0).astype(jnp.bfloat16)
        query = jnp.where(low, qk * scaling, 0.0).astype(jnp.bfloat16)
        values_ref[rows, :] = jnp.where(low, mid_ref[rows, :LANES], 0.0).astype(jnp.bfloat16)
        d_out = jnp.where(low, d_joined[:, :LANES], 0.0).astype(jnp.bfloat16)
        count = (q + 1) * SIDE
        lse = mid_ref[rows, 3 * LANES - 1 : 3 * LANES]
        scores = lax.dot_general(query, keys_ref[:count, :], NT, preferred_element_type=jnp.float32)
        weights = jnp.where(allowed_keys(start_ref[rows, :], q * SIDE, count), jnp.exp(scores - lse), 0.0)
        d_weights = lax.dot_general(d_out, values_ref[:count, :], NT, preferred_element_type=jnp.float32)
        moved = weights * d_weights
        d_scores = (moved - weights * jnp.sum(moved, -1, keepdims=True)).astype(jnp.bfloat16)
        weights = weights.astype(jnp.bfloat16)
        d_query_ref[rows, :] = jnp.dot(d_scores, keys_ref[:count, :], preferred_element_type=jnp.float32) * scaling
        d_key_ref[:count, :] += lax.dot_general(d_scores, query, TN, preferred_element_type=jnp.float32)
        d_value_ref[:count, :] += lax.dot_general(weights, d_out, TN, preferred_element_type=jnp.float32)
        d_joint_ref[rows, LANES : 2 * LANES] = (d_joined[:, :LANES] * gelu_slope(mid_ref[rows, :LANES])).astype(jnp.bfloat16)
        d_joint_ref[rows, 2 * LANES : 3 * LANES] = (
            d_joined[:, LANES : 2 * LANES] * gelu_slope(mid_ref[rows, LANES : 2 * LANES])
        ).astype(jnp.bfloat16)
        d_joint_ref[rows, 3 * LANES :] = jnp.where(
            low, d_joined[:, 2 * LANES :] * gelu_slope(mid_ref[rows, 2 * LANES :]), 0.0
        ).astype(jnp.bfloat16)
    for q in range(chunks):
        run_slots(slots, here, chunks + q, depth, 2 * chunks)
        rows = slice(q * SIDE, (q + 1) * SIDE)
        d_qk = jnp.where(low, d_query_ref[rows, :], swap_halves(d_key_ref[rows, :]))
        d_qk = d_qk * cos_ref[rows, :] - turned(d_qk, lane) * sin_ref[rows, :]
        d_joint_ref[rows, :LANES] = d_qk.astype(jnp.bfloat16)
        d_joint_ref[rows, LANES : 2 * LANES] = jnp.where(
            low, d_value_ref[rows, :], d_joint_ref[rows, LANES : 2 * LANES].astype(jnp.float32)
        ).astype(jnp.bfloat16)
        d_joint = d_joint_ref[rows, :]
        sums_ref[...] += jnp.sum(d_joint.astype(jnp.float32), 0, keepdims=True)
        d_hat = lax.dot_general(d_joint, weights_ref[:, :joint_width], NT, preferred_element_type=jnp.float32)
        d_hat_ref[rows, :] = d_hat.astype(jnp.bfloat16)

    @pl.when(here == pl.num_programs(0) - 1)
    def _():
        for step in slots[-1]:
            step()


def backward(grad_all, weights, joint_width, qk, mid, cosine, sine, start, branch, depth, seq, collective_id):
    tokens, width = grad_all.shape
    joined_width = weights.shape[1] - joint_width
    own = tokens // (depth * 8)

    def rows(columns):
        return pl.BlockSpec((seq, columns), lambda b: (b, 0))

    def whole(array):
        return pl.BlockSpec(array.shape, lambda b: (0, 0), pipeline_mode=pl.Buffered(1))

    return pl.pallas_call(
        functools.partial(backward_kernel, depth, own, joint_width),
        grid=(tokens // seq,),
        out_shape=(
            jax.ShapeDtypeStruct((tokens, joint_width), jnp.bfloat16),
            jax.ShapeDtypeStruct((tokens, width), jnp.bfloat16),
            jax.ShapeDtypeStruct((1, joint_width), jnp.float32),
            jax.ShapeDtypeStruct((own, width), jnp.bfloat16),
        ),
        in_specs=[rows(width), whole(weights), rows(LANES), rows(joined_width), rows(LANES), rows(LANES), rows(1), pl.BlockSpec(memory_space=pl.ANY)],
        out_specs=(
            rows(joint_width),
            rows(width),
            pl.BlockSpec((1, joint_width), lambda b: (0, 0)),
            pl.BlockSpec((own, width), lambda b: (0, 0)),
        ),
        scratch_shapes=[pltpu.VMEM((seq, LANES), jnp.bfloat16)] * 2
        + [pltpu.VMEM((seq, LANES), jnp.float32)] * 3
        + Scatter.scratch(depth, (own, width), branch.dtype),
        compiler_params=pltpu.CompilerParams(collective_id=collective_id, has_side_effects=True, vmem_limit_bytes=63 << 20),
    )(grad_all, weights, qk, mid, cosine, sine, start, branch)


def exchange(blocks):
    return lax.all_to_all(blocks, AXES, split_axis=0, concat_axis=0, tiled=True)


def on_device(
    hidden_in, w_in_t, in_bias, ln_gain, ln_shift, w_out_t, out_bias, segment_ids, out_grad
):
    depth = lax.axis_size("dp")
    devices = depth * lax.axis_size("ctx")
    ctx = lax.axis_index("ctx")
    me = lax.axis_index("dp") * lax.axis_size("ctx") + ctx
    tok_rows, model_width = hidden_in.shape[1:]
    seq_len = segment_ids.shape[1]
    tokens = devices * tok_rows
    own = model_width // devices
    in_parts = in_bias.shape[0]
    out_parts = w_out_t.shape[1] // model_width
    in_width, out_width = in_parts * own, out_parts * own

    gain, shift = ln_gain.astype(jnp.float32).T, ln_shift.astype(jnp.float32).T
    own_seg = lax.dynamic_slice_in_dim(segment_ids[0], ctx * tok_rows, tok_rows)
    begin = jnp.sum((segment_ids < own_seg[:, None]).astype(jnp.int32), 1)
    begin = jnp.stack([begin // 256, begin % 256]).reshape(-1, own).T.astype(jnp.float32)
    extra = jnp.concatenate(
        [jnp.zeros((own, LANES // 2)), gain, shift, begin, jnp.zeros((own, LANES // 2 - 2 - begin.shape[1]))], 1
    )
    got = exchange(split_blocks((w_in_t.T, w_out_t), (in_parts, out_parts), gain, extra))
    joint_width = (in_parts + 1) // 2 * LANES

    inputs = hidden_in[0].astype(jnp.float32)
    average = jnp.mean(inputs, -1, keepdims=True)
    centred = inputs - average
    inv_std = lax.rsqrt(jnp.mean(centred * centred, -1, keepdims=True) + epsilon)
    hat = centred * inv_std
    hat_all = gather_all(hat.astype(jnp.bfloat16), depth, 0)

    weights = got.reshape(model_width, -1)
    w_in = weights[:, :joint_width]
    gain_all = w_in[:, in_width : in_width + 1].astype(jnp.float32)
    shift_all = w_in[:, in_width + 1 : in_width + 2].astype(jnp.float32)
    begin = got[:, :, in_width + 2 : in_width + 2 + 2 * tok_rows // own].astype(jnp.int32)
    begin = begin.transpose(0, 2, 1).reshape(devices, 2, tok_rows)
    begin = (begin[:, 0] * 256 + begin[:, 1]).reshape(tokens)
    positions = (jnp.arange(tokens) % seq_len - begin).astype(jnp.float32)
    half = ROT // 2
    lane = jnp.arange(LANES) % HD
    frequency = jnp.where(lane < ROT, 10000.0 ** (-2.0 * (lane % half).astype(jnp.float32) / ROT), 0.0)
    angles = positions[:, None] * frequency[None, :]
    cosine = jnp.cos(angles)
    sine = jnp.sin(angles) * jnp.where(lane < half, -1.0, 1.0)[None]
    bias = in_bias.astype(jnp.float32).reshape(1, in_width)
    bias = jnp.pad(bias, ((0, 0), (0, joint_width - in_width)))
    bias = bias + jnp.sum(shift_all / gain_all * w_in.astype(jnp.float32), 0, keepdims=True)
    column = jnp.arange(model_width) // own
    out_row = jnp.where(column == me, jnp.tile(out_bias.astype(jnp.float32), devices), 0.0)[None]
    start = begin[:, None]
    qk, mid, joined, branch, g_all = forward(
        hat_all, weights, joint_width, bias, cosine, sine, start, out_row, out_grad[0], depth, seq_len, 1
    )
    d_joint, d_hat_part, joint_sums, branch_own = backward(
        g_all, weights, joint_width, qk, mid, cosine, sine, start, branch, depth, seq_len, 2
    )
    result = (inputs + branch_own.astype(jnp.float32)).astype(jnp.bfloat16)
    grad_out_local = lax.dot_general(g_all, joined, TN, preferred_element_type=jnp.float32).astype(jnp.bfloat16)
    back_out = exchange(grad_out_local.reshape(devices, own, -1))
    grad_hat = lax.dot_general(hat_all, d_joint, TN, preferred_element_type=jnp.float32)
    weight_in = w_in.astype(jnp.float32)
    gain_part = jnp.sum(weight_in * grad_hat, 1, keepdims=True) / gain_all
    shift_part = jnp.sum(weight_in * joint_sums, 1, keepdims=True) / gain_all
    back_lane = jnp.arange(joint_width)[None]
    grad_in_local = gain_all * grad_hat + shift_all * joint_sums
    grad_in_local = jnp.where(back_lane == in_width, gain_part, grad_in_local)
    grad_in_local = jnp.where(back_lane == in_width + 1, shift_part, grad_in_local).astype(jnp.bfloat16)
    back_in = exchange(grad_in_local.reshape(devices, own, -1))
    d_hat = scatter_sum(d_hat_part, depth, 3, jnp.float32)
    d_input = inv_std * (
        d_hat - jnp.mean(d_hat, -1, keepdims=True) - hat * jnp.mean(d_hat * hat, -1, keepdims=True)
    ) + out_grad[0].astype(jnp.float32)

    grad_w_out, _ = join_blocks(back_out, out_parts)
    grad_w_in, vectors = join_blocks(back_in, in_parts)
    g_columns = lax.dynamic_slice_in_dim(g_all, me * own, own, 1)
    return (
        result[None],
        d_input[None],
        grad_w_in.T,
        joint_sums[:, :in_width].reshape(in_parts, own),
        vectors[:, LANES // 2][None],
        vectors[:, LANES // 2 + 1][None],
        grad_w_out,
        jnp.sum(g_columns.astype(jnp.float32), 0),
    )


def solution(mesh):
    in_specs = (
        P("dp", "ctx", None),
        P(None, ("dp", "ctx")),
        P(None, ("dp", "ctx")),
        P(None, ("dp", "ctx")),
        P(None, ("dp", "ctx")),
        P(("dp", "ctx"), None),
        P(("dp", "ctx")),
        P("dp", None),
        P("dp", "ctx", None),
    )
    out_specs = (
        P("dp", "ctx", None),
        P("dp", "ctx", None),
        P(None, ("dp", "ctx")),
        P(None, ("dp", "ctx")),
        P(None, ("dp", "ctx")),
        P(None, ("dp", "ctx")),
        P(("dp", "ctx"), None),
        P(("dp", "ctx")),
    )
    tensor_parallel = mesh.shape["ctx"] == 8 and mesh.shape["dp"] * 8 == H
    body = on_device if tensor_parallel else on_device_gathered
    return jax.shard_map(
        body, mesh=mesh, in_specs=in_specs, out_specs=out_specs, check_vma=False
    )
```

```python
import functools
import math

import jax
import jax.numpy as jnp
from jax import lax
from jax.experimental import pallas as pl
from jax.experimental.pallas import tpu as pltpu
from jax.sharding import PartitionSpec as P

H = 32
HD = 64
ROT = 32
KEY_BLOCK = 512


epsilon = 1e-05
negative = -1e30


def rotation_tables(positions):
    half_dims = ROT // 2
    frequency = 10000.0 ** (-2.0 * jnp.arange(half_dims, dtype=jnp.float32) / ROT)
    angles = positions[:, None] * frequency[None, :]
    return (jnp.cos(angles)[:, None, :], jnp.sin(angles)[:, None, :])


def rotate(heads_in, cosine_table, sine_table, direction):
    half_dims = ROT // 2
    first_half = heads_in[..., :half_dims]
    second_half = heads_in[..., half_dims:ROT]
    return jnp.concatenate(
        [
            first_half * cosine_table - direction * second_half * sine_table,
            second_half * cosine_table + direction * first_half * sine_table,
            heads_in[..., ROT:],
        ],
        -1,
    )


def masked_scores(queries, key_rows, key_seg, key_index, query_seg, query_index):
    scaling = queries.shape[2] ** (-0.5)
    scores = (
        jnp.einsum("thd,khd->htk", queries, key_rows, preferred_element_type=jnp.float32) * scaling
    )
    allowed = (query_seg[:, None] == key_seg[None, :]) & (
        query_index[:, None] >= key_index[None, :]
    )
    return (jnp.where(allowed[None], scores, negative), allowed)


def score_grads(
    query_part,
    dout_part,
    lse_part,
    dot_part,
    query_seg,
    query_index,
    key_rows,
    value_rows,
    key_seg,
    key_index,
):
    scores, allowed = masked_scores(
        query_part, key_rows, key_seg, key_index, query_seg, query_index
    )
    weights = jnp.where(allowed[None], jnp.exp(scores - lse_part[..., None]), 0.0)
    d_weights = jnp.einsum(
        "thd,khd->htk", dout_part, value_rows, preferred_element_type=jnp.float32
    )
    d_scores = (weights * (d_weights - dot_part[..., None])).astype(jnp.bfloat16)
    return (weights.astype(jnp.bfloat16), d_scores)


def key_grads(
    key_rows,
    value_rows,
    key_seg,
    key_index,
    query_src,
    dout_src,
    lse_src,
    dot_src,
    seg_src,
    index_src,
    query_block,
):
    key_count = key_rows.shape[0]
    scaling = HD ** (-0.5)
    block_count = query_src.shape[0] // query_block

    def query_step(running, block_no):
        weights_low, d_scores = score_grads(
            query_src,
            dout_src,
            lse_src,
            dot_src,
            seg_src,
            index_src,
            key_rows,
            value_rows,
            key_seg,
            key_index,
        )
        d_key = (
            running[0]
            + jnp.einsum("htk,thd->khd", d_scores, query_src, preferred_element_type=jnp.float32)
            * scaling
        )
        d_value = running[1] + jnp.einsum(
            "htk,thd->khd", weights_low, dout_src, preferred_element_type=jnp.float32
        )
        return ((d_key, d_value), None)

    zero_heads = jnp.zeros((key_count, H, HD), jnp.float32)
    (d_key, d_value), _ = lax.scan(query_step, (zero_heads, zero_heads), jnp.arange(block_count))
    return (d_key.reshape(key_count, H * HD), d_value.reshape(key_count, H * HD))


def on_device_gathered(
    hidden_in, w_in_t, in_bias, ln_gain, ln_shift, w_out_t, out_bias, segment_ids, out_grad
):
    inputs = hidden_in[0].astype(jnp.float32)
    tok_rows, model_width = inputs.shape
    seg_row = segment_ids[0]
    seq_len = seg_row.shape[0]
    offset = lax.axis_index("ctx") * tok_rows
    index_all = jnp.arange(seq_len, dtype=jnp.int32)
    earlier = jnp.concatenate([seg_row[:1], seg_row[:-1]])
    begins = jnp.where((index_all == 0) | (seg_row != earlier), index_all, 0)
    positions = (index_all - lax.cummax(begins, axis=0)).astype(jnp.float32)
    local_pos = lax.dynamic_slice_in_dim(positions, offset, tok_rows)
    query_seg = lax.dynamic_slice_in_dim(seg_row, offset, tok_rows)
    query_index = offset + jnp.arange(tok_rows, dtype=jnp.int32)
    cosine_table, sine_table = rotation_tables(local_pos)
    scaling = HD ** (-0.5)
    average = jnp.mean(inputs, -1, keepdims=True)
    centred = inputs - average
    inv_std = lax.rsqrt(jnp.mean(centred * centred, -1, keepdims=True) + epsilon)
    normed_hat = centred * inv_std
    joint_width = w_in_t.shape[0]
    bias_rows = in_bias.shape[0]
    weight_piece = lax.all_gather(w_in_t, ("dp", "ctx"), axis=1, tiled=True)
    bias_piece = lax.all_gather(in_bias, ("dp", "ctx"), axis=1, tiled=True)
    gain_piece = lax.all_gather(ln_gain, ("dp", "ctx"), axis=1, tiled=True)
    shift_piece = lax.all_gather(ln_shift, ("dp", "ctx"), axis=1, tiled=True)
    normed_piece = (
        normed_hat * gain_piece.astype(jnp.float32) + shift_piece.astype(jnp.float32)
    ).astype(jnp.bfloat16)
    summed = lax.dot_general(
        normed_piece, weight_piece, (((1,), (1,)), ((), ())), preferred_element_type=jnp.float32
    )
    gain_all = gain_piece.astype(jnp.float32)
    bias_all = bias_piece.astype(jnp.float32)
    projected, normed, gain_all, bias_all = (summed, normed_piece, gain_all, bias_all)
    projected = projected + bias_all.reshape(1, joint_width)
    queries = rotate(
        projected[:, :model_width].reshape(tok_rows, H, HD), cosine_table, sine_table, 1.0
    ).astype(jnp.bfloat16)
    keys_new = (
        rotate(
            projected[:, model_width : 2 * model_width].reshape(tok_rows, H, HD),
            cosine_table,
            sine_table,
            1.0,
        )
        .astype(jnp.bfloat16)
        .reshape(tok_rows, model_width)
    )
    values_new = projected[:, 2 * model_width : 3 * model_width].astype(jnp.bfloat16)
    pre_gelu = projected[:, 3 * model_width :]
    keys_all, values_all = (
        lax.all_gather(keys_new, "ctx", axis=0, tiled=True),
        lax.all_gather(values_new, "ctx", axis=0, tiled=True),
    )
    block_count = seq_len // KEY_BLOCK

    def key_slice(first_key, key_count):
        key_rows = lax.dynamic_slice_in_dim(keys_all, first_key, key_count, 0).reshape(
            key_count, H, HD
        )
        value_rows = lax.dynamic_slice_in_dim(values_all, first_key, key_count, 0).reshape(
            key_count, H, HD
        )
        key_seg = lax.dynamic_slice_in_dim(seg_row, first_key, key_count)
        key_index = first_key + jnp.arange(key_count, dtype=jnp.int32)
        return (key_rows, value_rows, key_seg, key_index)

    def stats_step(running, block_no):
        running_max, running_sum = running
        key_rows, value_rows, key_seg, key_index = key_slice(block_no * KEY_BLOCK, KEY_BLOCK)
        scores, allowed = masked_scores(
            queries, key_rows, key_seg, key_index, query_seg, query_index
        )
        new_max = jnp.maximum(running_max, jnp.max(scores, -1))
        weights = jnp.where(allowed[None], jnp.exp(scores - new_max[..., None]), 0.0)
        running_sum = running_sum * jnp.exp(running_max - new_max) + jnp.sum(weights, -1)
        return ((new_max, running_sum), None)

    stats_init = (
        jnp.full((H, tok_rows), negative, jnp.float32),
        jnp.zeros((H, tok_rows), jnp.float32),
    )
    (final_max, final_sum), _ = lax.scan(stats_step, stats_init, jnp.arange(block_count))
    log_total = final_max + jnp.log(final_sum)

    def value_step(attended, block_no):
        key_rows, value_rows, key_seg, key_index = key_slice(block_no * KEY_BLOCK, KEY_BLOCK)
        scores, allowed = masked_scores(
            queries, key_rows, key_seg, key_index, query_seg, query_index
        )
        weights = jnp.where(allowed[None], jnp.exp(scores - log_total[..., None]), 0.0).astype(
            jnp.bfloat16
        )
        attended = attended + jnp.einsum(
            "htk,khd->thd", weights, value_rows, preferred_element_type=jnp.float32
        )
        return (attended, None)

    attended, _ = lax.scan(
        value_step, jnp.zeros((tok_rows, H, HD), jnp.float32), jnp.arange(block_count)
    )
    hidden = jax.nn.gelu(pre_gelu, approximate=True).astype(jnp.bfloat16)
    joined = jnp.concatenate(
        [attended.reshape(tok_rows, model_width).astype(jnp.bfloat16), hidden], 1
    )
    weight_piece, bias_piece = lax.all_gather(
        (w_out_t, out_bias), ("dp", "ctx"), axis=0, tiled=True
    )
    branch = (
        lax.dot_general(
            joined, weight_piece, (((1,), (1,)), ((), ())), preferred_element_type=jnp.float32
        )
        + bias_piece.astype(jnp.float32)[None, :]
    )
    result = (inputs + branch).astype(jnp.bfloat16)
    cotangent = out_grad[0]
    grad_part = cotangent
    d_joined = jnp.dot(
        grad_part,
        lax.all_gather(w_out_t, ("dp", "ctx"), axis=0, tiled=True),
        preferred_element_type=jnp.float32,
    )
    d_attn = d_joined[:, :model_width].astype(jnp.bfloat16).reshape(tok_rows, H, HD)

    def gelu_tanh(pre_values):
        return jax.nn.gelu(pre_values, approximate=True)

    _, gelu_pull = jax.vjp(gelu_tanh, pre_gelu)
    d_pre = gelu_pull(d_joined[:, model_width:])[0]
    row_dots = jnp.einsum("thd,thd->ht", d_attn.astype(jnp.float32), attended)

    def query_grad_step(d_query, block_no):
        key_rows, value_rows, key_seg, key_index = key_slice(block_no * KEY_BLOCK, KEY_BLOCK)
        _, d_scores = score_grads(
            queries,
            d_attn,
            log_total,
            row_dots,
            query_seg,
            query_index,
            key_rows,
            value_rows,
            key_seg,
            key_index,
        )
        d_query = (
            d_query
            + jnp.einsum("htk,khd->thd", d_scores, key_rows, preferred_element_type=jnp.float32)
            * scaling
        )
        return (d_query, None)

    d_query, _ = lax.scan(
        query_grad_step, jnp.zeros((tok_rows, H, HD), jnp.float32), jnp.arange(block_count)
    )
    count = lax.axis_size("ctx") * tok_rows
    sub_rows = math.gcd(count, KEY_BLOCK)

    def sub_step(carry_none, block_no):
        key_rows, value_rows, key_seg, key_index = key_slice(block_no * sub_rows, sub_rows)
        d_key, d_value = key_grads(
            key_rows,
            value_rows,
            key_seg,
            key_index,
            queries,
            d_attn,
            log_total,
            row_dots,
            query_seg,
            query_index,
            tok_rows,
        )
        return (carry_none, jnp.concatenate([d_key, d_value], 1))

    _, stacked = lax.scan(sub_step, jnp.zeros((), jnp.float32), jnp.arange(count // sub_rows))
    d_kv = lax.psum_scatter(
        stacked.reshape(count, 2 * model_width).astype(jnp.bfloat16),
        "ctx",
        scatter_dimension=0,
        tiled=True,
    ).astype(jnp.float32)
    d_key_local, d_value_local = (d_kv[:, :model_width], d_kv[:, model_width:])
    d_query_pre = rotate(d_query, cosine_table, sine_table, -1.0).reshape(tok_rows, model_width)
    d_key_pre = rotate(
        d_key_local.reshape(tok_rows, H, HD), cosine_table, sine_table, -1.0
    ).reshape(tok_rows, model_width)
    d_joint = jnp.concatenate([d_query_pre, d_key_pre, d_value_local, d_pre], 1).astype(
        jnp.bfloat16
    )
    d_normed = jnp.dot(
        d_joint,
        lax.all_gather(w_in_t, ("dp", "ctx"), axis=1, tiled=True),
        preferred_element_type=jnp.float32,
    )
    grad_part = cotangent
    in_term = lax.dot_general(
        normed, d_joint, (((0,), (0,)), ((), ())), preferred_element_type=jnp.float32
    )
    out_term = lax.dot_general(
        grad_part, joined, (((0,), (0,)), ((), ())), preferred_element_type=jnp.float32
    )
    grad_rows = lax.psum_scatter(
        jnp.concatenate([in_term, out_term], 1), ("dp", "ctx"), scatter_dimension=0, tiled=True
    )
    grad_w_in = grad_rows[:, :joint_width].T
    grad_w_out = grad_rows[:, joint_width:]
    grad_bias_in = jnp.sum(d_joint.astype(jnp.float32), 0).reshape(bias_rows, model_width)
    grad_gain_row = jnp.sum(d_normed * normed_hat, 0, keepdims=True)
    grad_shift_row = jnp.sum(d_normed, 0, keepdims=True)
    grad_bias_out = jnp.sum(cotangent.astype(jnp.float32), 0, keepdims=True)
    grad_in_bias, grad_gain, grad_shift, grad_out_row = (
        lax.psum_scatter(grad_bias_in, ("dp", "ctx"), scatter_dimension=1, tiled=True),
        lax.psum_scatter(grad_gain_row, ("dp", "ctx"), scatter_dimension=1, tiled=True),
        lax.psum_scatter(grad_shift_row, ("dp", "ctx"), scatter_dimension=1, tiled=True),
        lax.psum_scatter(grad_bias_out, ("dp", "ctx"), scatter_dimension=1, tiled=True),
    )
    d_hat = d_normed * gain_all
    d_input = inv_std * (
        d_hat
        - jnp.mean(d_hat, -1, keepdims=True)
        - normed_hat * jnp.mean(d_hat * normed_hat, -1, keepdims=True)
    ) + cotangent.astype(jnp.float32)
    return (
        result[None],
        d_input[None],
        grad_w_in,
        grad_in_bias,
        grad_gain,
        grad_shift,
        grad_w_out,
        grad_out_row[0],
    )


AXES = ("dp", "ctx")
MESH = pl.DeviceIdType.MESH
class Place:
    def __init__(self, depth):
        self.depth = depth
        self.top = depth - 1
        self.z = lax.axis_index("dp")
        self.c = lax.axis_index("ctx")
        y, x, self.core = self.c // 4, (self.c // 2) % 2, self.c % 2
        self.first_stride = jnp.where(self.core == 0, 2, 4)
        self.last_stride = jnp.where(self.core == 0, 4, 2)
        self.f = jnp.where(self.core == 0, x, y)
        self.l = jnp.where(self.core == 0, y, x)

    def ctx(self, f, l, core):
        return f * self.first_stride + l * self.last_stride + core

    def shard(self, z, f, l, core=None):
        return z * 8 + self.ctx(f, l, self.core if core is None else core)

    def first(self):
        return {"dp": self.z, "ctx": self.ctx(1 - self.f, self.l, self.core)}

    def last(self):
        return {"dp": self.z, "ctx": self.ctx(self.f, 1 - self.l, self.core)}

    def sibling(self):
        return {"dp": self.z, "ctx": self.ctx(self.f, self.l, 1 - self.core)}

    def above(self):
        return {"dp": self.z + 1, "ctx": self.c}

    def below(self):
        return {"dp": self.z - 1, "ctx": self.c}

    def greet(self):
        barrier = pltpu.get_barrier_semaphore()
        for device in (self.first(), self.last(), self.sibling()):
            pl.semaphore_signal(barrier, inc=1, device_id=device, device_id_type=MESH)

        @pl.when(self.z > 0)
        def _():
            pl.semaphore_signal(barrier, inc=1, device_id=self.below(), device_id_type=MESH)

        @pl.when(self.z < self.top)
        def _():
            pl.semaphore_signal(barrier, inc=1, device_id=self.above(), device_id_type=MESH)

        ends = jnp.where(self.z > 0, 1, 0) + jnp.where(self.z < self.top, 1, 0)
        pl.semaphore_wait(barrier, 3 + ends)

    def partner(self, k):
        return {"dp": self.z ^ (k // 8), "ctx": self.c ^ (k % 8)}

    def greet_all(self):
        barrier = pltpu.get_barrier_semaphore()
        for k in range(1, self.depth * 8):
            pl.semaphore_signal(barrier, inc=1, device_id=self.partner(k), device_id_type=MESH)
        pl.semaphore_wait(barrier, self.depth * 8 - 1)

    def choose(self, rule):
        value = jnp.int32(0)
        for z in range(self.depth):
            value = jnp.where(self.z == z, rule(z), value)
        return value

    def near(self, step):
        return self.choose(lambda z: sorted([q for q in range(self.depth) if q != z], key=lambda q: (abs(q - z), q))[step])

    def far(self, step):
        def rule(z):
            ups, downs = list(range(self.top, z, -1)), list(range(z))
            return ((ups + downs if 2 * z < self.depth else downs + ups) + [z])[step]

        return self.choose(rule)


def layer_norm(inputs):
    centred = inputs - jnp.mean(inputs, -1, keepdims=True)
    inv_std = lax.rsqrt(jnp.mean(centred * centred, -1, keepdims=True) + epsilon)
    return centred * inv_std, inv_std


def push(source, target, send, receive, device):
    return pltpu.make_async_remote_copy(
        src_ref=source, dst_ref=target, send_sem=send, recv_sem=receive, device_id=device, device_id_type=MESH
    )


class Gather:
    def __init__(self, me, full, offset, rows, route, own_ref, all_ref, local, sends, arrivals):
        self.me, self.full, self.offset, self.rows, self.route = me, full, offset, rows, route
        self.own_ref, self.all_ref, self.sends, self.arrivals = own_ref.at[pl.ds(offset, rows)], all_ref, sends, arrivals
        self.keep = pltpu.make_async_copy(self.own_ref, self.block(me.shard(me.z, me.f, me.l)), local)
        self.used, self.drains = 0, []
        zs = [me.z] + [me.near(step) for step in range(me.top)]
        pairs = [(z, f) for z in zs for f in (me.f, 1 - me.f)]
        self.steps = [self.begin]
        for n, pair in enumerate(pairs):
            if n:
                self.steps.append(functools.partial(self.relay, n, *pair))
                self.steps.append(functools.partial(self.cross, *pairs[n - 1]))
        self.steps.append(functools.partial(self.cross, *pairs[-1]))

    def block(self, shard):
        return self.all_ref.at[pl.ds(pl.multiple_of(shard * self.full + self.offset, self.rows), self.rows)]

    def send(self, source, shard, device, when=None):
        slot = self.used
        self.used += 1

        def start():
            push(source, self.block(shard), self.sends.at[slot], self.arrivals.at[shard], device).start()

        def drain():
            push(self.own_ref, self.block(0), self.sends.at[slot], self.arrivals.at[0], self.me.sibling()).wait_send()

        if when is None:
            start()
            self.drains.append(drain)
        else:
            pl.when(when())(start)
            self.drains.append(lambda: pl.when(when())(drain))

    def arrived(self, shard):
        push(self.own_ref, self.block(shard), self.sends.at[0], self.arrivals.at[shard], self.me.sibling()).wait_recv()

    def begin(self):
        me = self.me
        shard = me.shard(me.z, me.f, me.l)
        self.send(self.own_ref, shard, me.above(), lambda: me.z < me.top)
        self.send(self.own_ref, shard, me.below(), lambda: me.z > 0)
        self.send(self.own_ref, shard, me.first())
        self.send(self.own_ref, shard, me.last())
        self.send(self.own_ref, shard, me.sibling())
        self.keep.start()

    def relay(self, n, z, f):
        me = self.me
        shard = me.shard(z, f, me.l)
        block = self.block(shard)
        self.arrived(shard)
        if self.route == "zf":
            if n % 2 == 0:
                self.send(block, shard, me.above(), lambda: (z < me.z) & (me.z < me.top))
                self.send(block, shard, me.below(), lambda: (z > me.z) & (me.z > 0))
                self.send(block, shard, me.first())
        else:
            self.send(block, shard, me.above(), lambda: ((z < me.z) if n > 1 else (z == me.z)) & (me.z < me.top))
            self.send(block, shard, me.below(), lambda: ((z > me.z) if n > 1 else (z == me.z)) & (me.z > 0))
        self.send(block, shard, me.last())
        self.send(block, shard, me.sibling())

    def cross(self, z, f):
        me = self.me
        shard = me.shard(z, f, 1 - me.l)
        self.arrived(shard)
        self.send(self.block(shard), shard, me.sibling())

    def finish(self):
        me = self.me
        for z in range(me.depth):
            for f in range(2):
                for l in range(2):
                    self.arrived(me.shard(z, f, l, 1 - me.core))
        self.keep.wait()
        for drain in self.drains:
            drain()


class Exchange:
    def __init__(self, me, blocks_ref, got_ref, local, sends, arrivals):
        self.me, self.blocks_ref, self.got_ref, self.sends, self.arrivals = me, blocks_ref, got_ref, sends, arrivals
        self.mine = me.z * 8 + me.c
        self.keep = pltpu.make_async_copy(blocks_ref.at[self.mine], got_ref.at[self.mine], local)
        order = [high * 8 + low for low in range(8) for high in EXCHANGE_ORDER if high < me.depth]
        self.order = [k for k in order if k]
        self.steps = [functools.partial(self.start, k) for k in self.order] + [self.keep.start]

    def copy(self, k):
        peer = self.me.partner(k)
        other = peer["dp"] * 8 + peer["ctx"]
        return push(self.blocks_ref.at[other], self.got_ref.at[self.mine], self.sends.at[k], self.arrivals.at[k], peer)

    def start(self, k):
        self.copy(k).start()

    def finish(self):
        for k in self.order:
            self.copy(k).wait_recv()
        for k in self.order:
            self.copy(k).wait_send()
        self.keep.wait()

    @staticmethod
    def scratch(depth):
        return [pltpu.SemaphoreType.DMA(()), pltpu.SemaphoreType.DMA((depth * 8,)), pltpu.SemaphoreType.DMA((depth * 8,))]


EXCHANGE_ORDER = (0, 1, 2, 3)
ROUTES = ("zf", "zf")
ADD_ROWS = 32


def merged(main, side, ahead=0):
    steps, done = list(main[:ahead]), 0
    rest = main[ahead:]
    for n, step in enumerate(rest):
        upto = (n + 1) * len(side) // len(rest)
        steps += side[done:upto] + [step]
        done = upto
    return steps


def interleaved(parts):
    most = max(len(part.steps) for part in parts)
    return [part.steps[n] for n in range(most) for part in parts if n < len(part.steps)]


def gather_parts(depth, full, routes, own_ref, all_ref, scratch):
    me = Place(depth)
    rows = full // len(routes)
    return [
        Gather(me, full, n * rows, rows, route, own_ref, all_ref, *scratch[3 * n : 3 * n + 3]) for n, route in enumerate(routes)
    ]


def gather_scratch(depth, routes):
    return [
        pltpu.SemaphoreType.DMA(()),
        pltpu.SemaphoreType.DMA((9 + 8 * (depth - 1) + 2 * depth,)),
        pltpu.SemaphoreType.DMA((depth * 8,)),
    ] * len(routes)


class Scatter:
    def __init__(self, me, full, offset, rows, route, part_ref, out_ref, sums, from_sib, from_last, from_first, from_below, from_above,
                 loads, send_sib, send_last, send_first, send_line, got_sib, got_last, got_first, got_below, got_above):
        self.me, self.full, self.offset, self.rows, self.route, self.step = me, full, offset, rows, route, min(rows, ADD_ROWS)
        self.part_ref, self.out_ref, self.sums, self.loads = part_ref, out_ref, sums, loads
        self.sib, self.last, self.first = (from_sib, send_sib, got_sib), (from_last, send_last, got_last), (from_first, send_first, got_first)
        self.up, self.down = (from_below, send_line, got_below), (from_above, send_line, got_above)
        self.zs = [me.far(i) for i in range(me.depth)]
        chip = [functools.partial(self.chip, z) for z in self.zs]
        plane = [functools.partial(self.plane, z) for z in self.zs]
        line = [functools.partial(self.line, z) for z in self.zs[:-1]] + [self.final]
        lag = 1 if route == "zf" else 0
        self.steps = [self.begin] + chip
        for i in range(me.depth + lag):
            self.steps += plane[i : i + 1] + (line[i - lag : i - lag + 1] if i >= lag else [])

    def source(self, z, f, l, core):
        row = self.me.shard(z, f, l, core) * self.full + self.offset
        return self.part_ref.at[pl.ds(pl.multiple_of(row, self.rows), self.rows)]

    def at(self, z, f, l):
        return z * 4 + f * 2 + l

    def add(self, target, source):
        @pl.loop(0, self.rows // self.step)
        def _(i):
            part = pl.ds(pl.multiple_of(i * self.step, self.step), self.step)
            target[part, :] = target[part, :] + source[part, :]

    def copy(self, stage, source, slot, device, send_slot=None):
        landing, send, got = stage
        return push(source, landing.at[slot], send.at[slot if send_slot is None else send_slot], got.at[slot], device)

    def to_sibling(self, z, f, l):
        return self.copy(self.sib, self.source(z, f, l, 1 - self.me.core), self.at(z, l, f), self.me.sibling())

    def to_last(self, z, f):
        me = self.me
        return self.copy(self.last, self.sums.at[self.at(z, f, 1 - me.l)], z * 2 + f, me.last())

    def to_first(self, z):
        me = self.me
        return self.copy(self.first, self.sums.at[self.at(z, 1 - me.f, me.l)], z, me.first())

    def held(self, z, f):
        return self.sums.at[self.at(z, f, self.me.l)]

    def slot(self, z, f):
        return z if self.route == "zf" else z * 2 + f

    def along(self, z, f):
        slot = self.slot(z, f)
        return (
            lambda: self.copy(self.up, self.held(z, f), slot, self.me.above()),
            lambda: self.copy(self.down, self.held(z, f), slot, self.me.below()),
        )

    def load(self, z, f, l):
        k = self.at(z, f, l)
        return pltpu.make_async_copy(self.source(z, f, l, self.me.core), self.sums.at[k], self.loads.at[k])

    def pairs(self):
        me = self.me
        return [(f, l) for l in (1 - me.l, me.l) for f in (1 - me.f, me.f)]

    def sides(self):
        return (self.me.f,) if self.route == "zf" else (1 - self.me.f, self.me.f)

    def begin(self):
        me = self.me
        for z in self.zs:
            for f in (1 - me.f, me.f):
                for l in (1 - me.l, me.l):
                    self.to_sibling(z, f, l).start()
            for f, l in self.pairs():
                self.load(z, f, l).start()

    def chip(self, z):
        me = self.me
        for n, (f, l) in enumerate(self.pairs()):
            k = self.at(z, f, l)
            self.load(z, f, l).wait()
            self.copy(self.sib, self.sums.at[k], k, me.sibling()).wait_recv()
            self.add(self.sums.at[k], self.sib[0].at[k])
            if n in (1, 2):
                self.to_last(z, self.pairs()[n - 1][0]).start()

    def plane(self, z):
        me = self.me
        for f in (1 - me.f, me.f):
            self.to_last(z, f).wait_recv()
            self.add(self.held(z, f), self.last[0].at[z * 2 + f])
        if self.route == "zf":
            self.to_first(z).start()

    def from_other_half(self, z):
        self.to_first(z).wait_recv()
        self.add(self.held(z, self.me.f), self.first[0].at[z])

    def line(self, z):
        me = self.me
        if self.route == "zf":
            self.from_other_half(z)
        for f in self.sides():
            upward, downward = self.along(z, f)

            @pl.when((z > me.z) & (me.z > 0))
            def _():
                upward().wait_recv()
                self.add(self.held(z, f), self.up[0].at[self.slot(z, f)])

            @pl.when((z < me.z) & (me.z < me.top))
            def _():
                downward().wait_recv()
                self.add(self.held(z, f), self.down[0].at[self.slot(z, f)])

            @pl.when(z > me.z)
            def _():
                upward().start()

            @pl.when(z < me.z)
            def _():
                downward().start()

    def final(self):
        me = self.me
        z = me.z
        if self.route == "zf":
            self.from_other_half(z)
        for f in self.sides():
            upward, downward = self.along(z, f)

            @pl.when(z > 0)
            def _():
                upward().wait_recv()
                self.add(self.held(z, f), self.up[0].at[self.slot(z, f)])

            @pl.when(z < me.top)
            def _():
                downward().wait_recv()
                self.add(self.held(z, f), self.down[0].at[self.slot(z, f)])

        if self.route != "zf":
            self.to_first(z).start()
            self.from_other_half(z)
        self.out_ref[pl.ds(self.offset, self.rows), :] = self.held(z, me.f)[...].astype(self.out_ref.dtype)

    def finish(self):
        me = self.me
        for i, z in enumerate(self.zs):
            for f, l in self.pairs():
                self.to_sibling(z, f, l).wait_send()
            for f in (1 - me.f, me.f):
                self.to_last(z, f).wait_send()
            if self.route == "zf" or i == me.top:
                self.to_first(z).wait_send()
            if i < me.top:
                for f in self.sides():
                    self.along(z, f)[0]().wait_send()


def scatter_parts(depth, full, routes, part_ref, out_ref, scratch):
    me = Place(depth)
    rows = full // len(routes)
    each = len(scratch) // len(routes)
    return [
        Scatter(me, full, n * rows, rows, route, part_ref, out_ref, *scratch[each * n : each * (n + 1)]) for n, route in enumerate(routes)
    ]


def scatter_scratch(depth, full, width, dtype, routes):
    dma = pltpu.SemaphoreType.DMA
    scratch = []
    for route in routes:
        line = depth if route == "zf" else depth * 2
        counts = [depth * 4, depth * 4, depth * 2, depth, line, line]
        sems = [depth * 4, depth * 4, depth * 2, depth, line, depth * 4, depth * 2, depth, line, line]
        scratch += [pltpu.VMEM((count, full // len(routes), width), dtype) for count in counts]
        scratch += [dma((count,)) for count in sems]
    return scratch


LANES = 128
NT = (((1,), (1,)), ((), ()))
TN = (((0,), (0,)), ((), ()))


def low_half(shape):
    return lax.broadcasted_iota(jnp.int32, shape, 1) < LANES // 2


def swap_halves(block):
    return pltpu.roll(block, LANES // 2, 1)


def split_blocks(parts, width, *refs):
    scale_ref, extra_ref, out_ref = refs[len(parts) :]
    depth = out_ref.shape[1]
    low = low_half((depth, LANES))

    @pl.loop(0, width // LANES)
    def _(m):
        base = 0
        for count, rows_ref in zip(parts, refs):
            for pair in range((count + 1) // 2):

                def piece(part):
                    lanes = pl.ds(pl.multiple_of(part * width + m * LANES, LANES), LANES)
                    values = rows_ref[:, lanes].astype(jnp.float32)
                    return values * scale_ref[...] if base == 0 else values

                first = piece(2 * pair)
                if 2 * pair + 1 < count:
                    second = piece(2 * pair + 1)
                    even = jnp.where(low, first, swap_halves(second))
                    odd = jnp.where(low, swap_halves(first), second)
                else:
                    rest = extra_ref[...] if base == 0 else jnp.zeros_like(first)
                    even = jnp.where(low, first, rest)
                    odd = jnp.where(low, swap_halves(first), rest)
                lanes = slice((base + pair) * LANES, (base + pair + 1) * LANES)
                out_ref[2 * m, :, lanes] = even.astype(out_ref.dtype)
                out_ref[2 * m + 1, :, lanes] = odd.astype(out_ref.dtype)
            base += (count + 1) // 2

def head_kernel(depth, full, routes, parts_out, width, inputs_ref, w_in_ref, w_out_ref, scale_ref, extra_ref, all_ref, got_ref,
                hat_ref, blocks_ref, w_in, w_out, loads, *scratch):
    copies = [
        pltpu.make_async_copy(source, target, loads.at[n]) for n, (source, target) in enumerate(((w_in_ref, w_in), (w_out_ref, w_out)))
    ]
    for copy in copies:
        copy.start()

    @pl.loop(0, full // 32)
    def _(i):
        rows = pl.ds(pl.multiple_of(i * 32, 32), 32)
        hat_ref[rows, :] = layer_norm(inputs_ref[rows, :].astype(jnp.float32))[0].astype(hat_ref.dtype)

    count = len(gather_scratch(depth, routes))
    parts = gather_parts(depth, full, routes, hat_ref, all_ref, scratch[:count])
    exchange = Exchange(parts[0].me, blocks_ref, got_ref, *scratch[count:])
    parts[0].me.greet_all()
    steps = interleaved(parts)
    for step in steps[: len(parts)]:
        step()
    for copy in copies:
        copy.wait()
    split_blocks(parts_out, width, w_in, w_out, scale_ref, extra_ref, blocks_ref)
    for step in merged(steps[len(parts) :], exchange.steps):
        step()
    for part in parts + [exchange]:
        part.finish()


def head(inputs, w_in, w_out, parts_out, scale, extra, depth, routes, collective_id):
    rows, width = inputs.shape
    own = w_in.shape[0]
    devices = depth * 8
    blocks = (devices, own, sum((count + 1) // 2 for count in parts_out) * LANES)
    here, vmem = pl.BlockSpec(memory_space=pl.ANY), pl.BlockSpec(memory_space=pltpu.VMEM)
    return pl.pallas_call(
        functools.partial(head_kernel, depth, rows, routes, parts_out, width),
        out_shape=(
            jax.ShapeDtypeStruct((devices * rows, width), inputs.dtype),
            jax.ShapeDtypeStruct(blocks, inputs.dtype),
        ),
        in_specs=[vmem, here, here, vmem, vmem],
        out_specs=(here, here),
        scratch_shapes=[
            pltpu.VMEM((rows, width), inputs.dtype),
            pltpu.VMEM(blocks, inputs.dtype),
            pltpu.VMEM(w_in.shape, w_in.dtype),
            pltpu.VMEM(w_out.shape, w_out.dtype),
            pltpu.SemaphoreType.DMA((2,)),
        ]
        + gather_scratch(depth, routes)
        + Exchange.scratch(depth),
        compiler_params=pltpu.CompilerParams(collective_id=collective_id, has_side_effects=True, vmem_limit_bytes=32 << 20),
    )(inputs, w_in, w_out, scale, extra)


def join_kernel(parts, width, blocks_ref, out_ref, extra_ref):
    depth = out_ref.shape[0]
    low = low_half((depth, LANES))
    extra_ref[...] = jnp.zeros_like(extra_ref)

    @pl.loop(0, width // LANES)
    def _(m):
        for pair in range((parts + 1) // 2):
            lanes = slice(pair * LANES, (pair + 1) * LANES)
            even = blocks_ref[2 * m, :, lanes].astype(jnp.float32)
            odd = blocks_ref[2 * m + 1, :, lanes].astype(jnp.float32)
            first = pl.ds(pl.multiple_of(2 * pair * width + m * LANES, LANES), LANES)
            out_ref[:, first] = jnp.where(low, even, swap_halves(odd))
            if 2 * pair + 1 < parts:
                second = pl.ds(pl.multiple_of((2 * pair + 1) * width + m * LANES, LANES), LANES)
                out_ref[:, second] = jnp.where(low, swap_halves(even), odd)
            else:
                extra_ref[...] += even + odd


def join_blocks(blocks, parts):
    count, depth, _ = blocks.shape
    width = count * HD
    return pl.pallas_call(
        functools.partial(join_kernel, parts, width),
        out_shape=(
            jax.ShapeDtypeStruct((depth, parts * width), jnp.float32),
            jax.ShapeDtypeStruct((depth, LANES), jnp.float32),
        ),
        in_specs=[pl.BlockSpec(memory_space=pltpu.VMEM)],
        out_specs=(pl.BlockSpec(memory_space=pltpu.VMEM), pl.BlockSpec(memory_space=pltpu.VMEM)),
        compiler_params=pltpu.CompilerParams(vmem_limit_bytes=24 << 20),
    )(blocks)


SIDE = 256


def turned(block, lane):
    shift = ROT // 2
    return jnp.where(lane % HD < shift, pltpu.roll(block, LANES - shift, 1), pltpu.roll(block, shift, 1))


def gelu(t):
    inner = math.sqrt(2.0 / math.pi) * (t + 0.044715 * (t * t * t))
    return 0.5 * t * (1.0 + jnp.tanh(inner))


def gelu_slope(t):
    slope = math.sqrt(2.0 / math.pi)
    bent = jnp.tanh(slope * (t + 0.044715 * (t * t * t)))
    return 0.5 * (1.0 + bent) + 0.5 * t * (1.0 - bent * bent) * slope * (1.0 + 3.0 * 0.044715 * (t * t))


def allowed_keys(start, first_query, keys):
    query = first_query + lax.broadcasted_iota(jnp.int32, (SIDE, keys), 0)
    key = lax.broadcasted_iota(jnp.int32, (SIDE, keys), 1)
    return (key >= start) & (key <= query)


def document_starts(weights_ref, lanes, first, count):
    pieces = []
    for shard in range(count):
        rows = pl.ds(pl.multiple_of((first + shard) * HD, HD), HD)
        block = weights_ref[rows, lanes].astype(jnp.float32)
        pieces += [block[:, HD + 2 + n : HD + 3 + n] * 256.0 + block[:, HD + 4 + n : HD + 5 + n] for n in range(2)]
    return jnp.concatenate(pieces, 0)


def forward_kernel(depth, shard_rows, joint_width, routes, hat_ref, weights_ref, bias_ref, waves_ref, out_bias_ref, grad_ref,
                   qk_ref, mid_ref, cos_ref, sin_ref, joined_ref, out_ref, grads_ref, keys_ref, values_ref, shift_ref, *scratch):
    seq = hat_ref.shape[0]
    here = pl.program_id(0)
    low = low_half((SIDE, LANES))
    lane = lax.broadcasted_iota(jnp.int32, (SIDE, LANES), 1)
    scaling = HD ** (-0.5)
    parts = gather_parts(depth, shard_rows, routes, grad_ref, grads_ref, scratch)
    chunks = seq // SIDE
    slots = spread_steps([parts[0].me.greet] + interleaved(parts), len(parts), depth * 2 * chunks, [part.finish for part in parts])
    side_lanes = slice(joint_width - LANES, joint_width)

    for q in range(chunks):
        run_slots(slots, here, 2 * q, depth, 2 * chunks)
        if q == 0:

            @pl.when(here == 0)
            def _():
                total = bias_ref[...]
                for n in range(weights_ref.shape[0] // SIDE):
                    some = slice(n * SIDE, (n + 1) * SIDE)
                    side = weights_ref[some, side_lanes].astype(jnp.float32)
                    ratio = side[:, HD + 1 : HD + 2] / side[:, HD : HD + 1]
                    total = total + jnp.sum(ratio * weights_ref[some, :joint_width].astype(jnp.float32), 0, keepdims=True)
                shift_ref[...] = total

        rows = slice(q * SIDE, (q + 1) * SIDE)
        joint = jnp.dot(hat_ref[rows, :], weights_ref[:, :joint_width], preferred_element_type=jnp.float32) + shift_ref[...]
        per_chunk = SIDE // shard_rows
        start = document_starts(weights_ref, side_lanes, (here * chunks + q) * per_chunk, per_chunk)
        index = q * SIDE + lax.broadcasted_iota(jnp.int32, (SIDE, 1), 0)
        angles = (index.astype(jnp.float32) - start) * waves_ref[0:1, :]
        cosine, sine = jnp.cos(angles), jnp.sin(angles) * waves_ref[1:2, :]
        cos_ref[rows, :] = cosine
        sin_ref[rows, :] = sine
        qk = joint[:, :LANES]
        qk = qk * cosine + turned(qk, lane) * sine
        keys_ref[rows, :] = swap_halves(qk).astype(jnp.bfloat16)
        query = jnp.where(low, qk * scaling, 0.0).astype(jnp.bfloat16)
        qk_ref[rows, :] = qk.astype(jnp.bfloat16)
        values_ref[rows, :] = jnp.where(low, joint[:, LANES : 2 * LANES], 0.0).astype(jnp.bfloat16)
        count = (q + 1) * SIDE
        scores = lax.dot_general(query, keys_ref[:count, :], NT, preferred_element_type=jnp.float32)
        scores = jnp.where(allowed_keys(start.astype(jnp.int32), q * SIDE, count), scores, negative)
        largest = jnp.max(scores, -1, keepdims=True)
        weights = jnp.exp(scores - largest)
        total = jnp.sum(weights, -1, keepdims=True)
        weights = (weights * (1.0 / total)).astype(jnp.bfloat16)
        attended = jnp.dot(weights, values_ref[:count, :], preferred_element_type=jnp.float32)
        run_slots(slots, here, 2 * q + 1, depth, 2 * chunks)
        lse = largest + jnp.log(total)
        mid_ref[rows, : 2 * LANES] = joint[:, LANES : 3 * LANES]
        mid_ref[rows, 2 * LANES :] = jnp.where(low, joint[:, 3 * LANES :], lse)
        joined_ref[rows, :LANES] = jnp.where(low, attended, gelu(joint[:, LANES : 2 * LANES])).astype(jnp.bfloat16)
        joined_ref[rows, LANES : 2 * LANES] = gelu(joint[:, 2 * LANES : 3 * LANES]).astype(jnp.bfloat16)
        joined_ref[rows, 2 * LANES :] = jnp.where(low, gelu(joint[:, 3 * LANES :]), 0.0).astype(jnp.bfloat16)
        branch = lax.dot_general(joined_ref[rows, :], weights_ref[:, joint_width:], NT, preferred_element_type=jnp.float32)
        out_ref[rows, :] = (branch + out_bias_ref[...]).astype(jnp.bfloat16)

    @pl.when(here == pl.num_programs(0) - 1)
    def _():
        for step in slots[-1]:
            step()


def spread_steps(steps, ahead, count, after):
    slots = [[] for _ in range(count + 1)]
    slots[0] += steps[: 1 + ahead]
    rest = steps[1 + ahead :]
    for n, step in enumerate(rest):
        slots[n * count // len(rest)].append(step)
    slots[-1] = list(after)
    return slots


def run_slots(slots, here, q, blocks, chunks, first=0):
    for block in range(blocks):
        steps = slots[block * chunks + q]
        if steps:

            @pl.when(here == block + first)
            def _():
                for step in steps:
                    step()


def forward(hat_all, weights, joint_width, bias, waves, out_bias, grads, depth, seq, routes, collective_id):
    tokens, width = hat_all.shape
    joined_width = weights.shape[1] - joint_width

    def rows(columns):
        return pl.BlockSpec((seq, columns), lambda b: (b, 0))

    def whole(array):
        return pl.BlockSpec(array.shape, lambda b: (0, 0), pipeline_mode=pl.Buffered(1))

    def out(columns, kind):
        return jax.ShapeDtypeStruct((tokens, columns), kind)

    return pl.pallas_call(
        functools.partial(forward_kernel, depth, grads.shape[0], joint_width, routes),
        grid=(tokens // seq,),
        out_shape=(
            out(LANES, jnp.bfloat16),
            out(joined_width, jnp.float32),
            out(LANES, jnp.float32),
            out(LANES, jnp.float32),
            out(joined_width, jnp.bfloat16),
            out(width, jnp.bfloat16),
            out(width, jnp.bfloat16),
        ),
        in_specs=[rows(width), whole(weights), whole(bias), whole(waves), whole(out_bias), pl.BlockSpec(memory_space=pl.ANY)],
        out_specs=(
            rows(LANES), rows(joined_width), rows(LANES), rows(LANES), rows(joined_width), rows(width),
            pl.BlockSpec(memory_space=pl.ANY),
        ),
        scratch_shapes=[pltpu.VMEM((seq, LANES), jnp.bfloat16)] * 2
        + [pltpu.VMEM((1, joint_width), jnp.float32)]
        + gather_scratch(depth, routes),
        compiler_params=pltpu.CompilerParams(collective_id=collective_id, has_side_effects=True, vmem_limit_bytes=56 << 20),
    )(hat_all, weights, bias, waves, out_bias, grads)


LATEST = 27


def backward_kernel(depth, shard_rows, joint_width, routes, grad_ref, hat_ref, weights_ref, qk_ref, mid_ref, cos_ref, sin_ref, branch_ref,
                    d_hat_ref, sums_ref, back_ref, own_ref,
                    keys_ref, values_ref, d_key_ref, d_value_ref, d_query_ref, d_joint_ref, total_ref, *scratch):
    seq = qk_ref.shape[0]
    chunks = seq // SIDE
    here, stage = pl.program_id(0), pl.program_id(1)
    low = low_half((SIDE, LANES))
    lane = lax.broadcasted_iota(jnp.int32, (SIDE, LANES), 1)
    scaling = HD ** (-0.5)
    side_lanes = slice(joint_width - LANES, joint_width)
    parts = scatter_parts(depth, shard_rows, routes, branch_ref, own_ref, scratch)
    main, ahead = interleaved(parts), (1 + depth) * len(parts)
    slots = [[] for _ in range(depth * 2 * chunks)] + [[part.finish for part in parts]]
    slots[0] += [parts[0].me.greet] + main[: len(parts)]
    for n, step in enumerate(main[len(parts) : ahead]):
        slots[1 + n // len(parts)].append(step)
    for n, step in enumerate(main[ahead:]):
        slots[1 + depth + n * LATEST // (len(main) - ahead)].append(step)

    def first_stage(q, rows):
        if q == 0:
            d_key_ref[...] = jnp.zeros_like(d_key_ref)
            d_value_ref[...] = jnp.zeros_like(d_value_ref)

            @pl.when(here == 0)
            def _():
                sums_ref[...] = jnp.zeros_like(sums_ref)
                total_ref[...] = jnp.zeros_like(total_ref)

        d_joined = jnp.dot(grad_ref[...], weights_ref[:, joint_width:], preferred_element_type=jnp.float32)
        per_chunk = SIDE // shard_rows
        start = document_starts(weights_ref, side_lanes, (here * chunks + q) * per_chunk, per_chunk).astype(jnp.int32)
        qk = qk_ref[rows, :].astype(jnp.float32)
        keys_ref[rows, :] = jnp.where(low, swap_halves(qk), 0.0).astype(jnp.bfloat16)
        query = jnp.where(low, qk * scaling, 0.0).astype(jnp.bfloat16)
        values_ref[rows, :] = jnp.where(low, mid_ref[rows, :LANES], 0.0).astype(jnp.bfloat16)
        d_out = jnp.where(low, d_joined[:, :LANES], 0.0).astype(jnp.bfloat16)
        count = (q + 1) * SIDE
        lse = mid_ref[rows, 3 * LANES - 1 : 3 * LANES]
        scores = lax.dot_general(query, keys_ref[:count, :], NT, preferred_element_type=jnp.float32)
        weights = jnp.where(allowed_keys(start, q * SIDE, count), jnp.exp(scores - lse), 0.0)
        d_weights = lax.dot_general(d_out, values_ref[:count, :], NT, preferred_element_type=jnp.float32)
        moved = weights * d_weights
        d_scores = (moved - weights * jnp.sum(moved, -1, keepdims=True)).astype(jnp.bfloat16)
        weights = weights.astype(jnp.bfloat16)
        d_query_ref[rows, :] = jnp.dot(d_scores, keys_ref[:count, :], preferred_element_type=jnp.float32) * scaling
        d_key_ref[:count, :] += lax.dot_general(d_scores, query, TN, preferred_element_type=jnp.float32)
        d_value_ref[:count, :] += lax.dot_general(weights, d_out, TN, preferred_element_type=jnp.float32)
        d_joint_ref[rows, LANES : 2 * LANES] = (d_joined[:, :LANES] * gelu_slope(mid_ref[rows, :LANES])).astype(jnp.bfloat16)
        d_joint_ref[rows, 2 * LANES : 3 * LANES] = (
            d_joined[:, LANES : 2 * LANES] * gelu_slope(mid_ref[rows, LANES : 2 * LANES])
        ).astype(jnp.bfloat16)
        d_joint_ref[rows, 3 * LANES :] = jnp.where(
            low, d_joined[:, 2 * LANES :] * gelu_slope(mid_ref[rows, 2 * LANES :]), 0.0
        ).astype(jnp.bfloat16)

    def second_stage(q, rows):
        d_qk = jnp.where(low, d_query_ref[rows, :], swap_halves(d_key_ref[rows, :]))
        d_qk = d_qk * cos_ref[rows, :] - turned(d_qk, lane) * sin_ref[rows, :]
        d_joint_ref[rows, :LANES] = d_qk.astype(jnp.bfloat16)
        d_joint_ref[rows, LANES : 2 * LANES] = jnp.where(
            low, d_value_ref[rows, :], d_joint_ref[rows, LANES : 2 * LANES].astype(jnp.float32)
        ).astype(jnp.bfloat16)
        d_joint = d_joint_ref[rows, :]
        sums_ref[...] += jnp.sum(d_joint.astype(jnp.float32), 0, keepdims=True)
        d_hat = lax.dot_general(d_joint, weights_ref[:, :joint_width], NT, preferred_element_type=jnp.float32)
        d_hat_ref[...] = d_hat.astype(jnp.bfloat16)
        if q % 2 == 1:
            both = slice(rows.start - SIDE, rows.stop)
            total_ref[...] += lax.dot_general(d_joint_ref[both, :], hat_ref[...], TN, preferred_element_type=jnp.float32)

    for at in range(2 * chunks):

        @pl.when(stage == at)
        def _():
            run_slots(slots, here, at, depth, 2 * chunks)
            rows = slice(at % chunks * SIDE, (at % chunks + 1) * SIDE)
            if at < chunks:
                first_stage(at, rows)
            else:
                second_stage(at - chunks, rows)

    @pl.when((here == pl.num_programs(0) - 1) & (stage == 2 * chunks - 1))
    def _():
        side_lane = lax.broadcasted_iota(jnp.int32, (SIDE, LANES), 1)
        for n in range(back_ref.shape[0] // SIDE):
            some = slice(n * SIDE, (n + 1) * SIDE)
            side = weights_ref[some, side_lanes].astype(jnp.float32)
            gain, shift = side[:, HD : HD + 1], side[:, HD + 1 : HD + 2]
            weight = weights_ref[some, :joint_width].astype(jnp.float32)
            total = total_ref[:, some].T
            back = gain * total + shift * sums_ref[...]
            gain_part = jnp.sum(weight * total, 1, keepdims=True) / gain
            shift_part = jnp.sum(weight * sums_ref[...], 1, keepdims=True) / gain
            last = jnp.where(side_lane == HD, gain_part, back[:, side_lanes])
            last = jnp.where(side_lane == HD + 1, shift_part, last)
            back_ref[some, : joint_width - LANES] = back[:, : joint_width - LANES].astype(jnp.bfloat16)
            back_ref[some, side_lanes] = last.astype(jnp.bfloat16)
        for step in slots[-1]:
            step()


def backward(grad_all, hat_all, weights, joint_width, qk, mid, cosine, sine, branch, depth, seq, routes, collective_id):
    tokens, width = grad_all.shape
    joined_width = weights.shape[1] - joint_width
    own = tokens // (depth * 8)
    chunks = seq // SIDE

    def rows(columns):
        return pl.BlockSpec((seq, columns), lambda b, s: (b, 0))

    def whole(shape, **mode):
        return pl.BlockSpec(shape, lambda b, s: (0, 0), **mode)

    def early(columns):
        return pl.BlockSpec((SIDE, columns), lambda b, s: (b * chunks + jnp.minimum(s, chunks - 1), 0))

    def late(columns):
        return pl.BlockSpec((SIDE, columns), lambda b, s: (b * chunks + jnp.maximum(s - chunks, 0), 0))

    return pl.pallas_call(
        functools.partial(backward_kernel, depth, own, joint_width, routes),
        grid=(tokens // seq, 2 * chunks),
        out_shape=(
            jax.ShapeDtypeStruct((tokens, width), jnp.bfloat16),
            jax.ShapeDtypeStruct((1, joint_width), jnp.float32),
            jax.ShapeDtypeStruct((width, joint_width), jnp.bfloat16),
            jax.ShapeDtypeStruct((own, width), jnp.bfloat16),
        ),
        in_specs=[
            early(width),
            pl.BlockSpec((2 * SIDE, width), lambda b, s: ((b * chunks + jnp.maximum(s - chunks, 0)) // 2, 0)),
            whole(weights.shape, pipeline_mode=pl.Buffered(1)),
            rows(LANES), rows(joined_width), rows(LANES), rows(LANES), pl.BlockSpec(memory_space=pl.ANY),
        ],
        out_specs=(late(width), whole((1, joint_width)), whole((width, joint_width)), whole((own, width))),
        scratch_shapes=[pltpu.VMEM((seq, LANES), jnp.bfloat16)] * 2
        + [pltpu.VMEM((seq, LANES), jnp.float32)] * 3
        + [pltpu.VMEM((seq, joint_width), jnp.bfloat16), pltpu.VMEM((joint_width, width), jnp.float32)]
        + scatter_scratch(depth, own, width, branch.dtype, routes),
        compiler_params=pltpu.CompilerParams(collective_id=collective_id, has_side_effects=True, vmem_limit_bytes=63 << 20),
    )(grad_all, hat_all, weights, qk, mid, cosine, sine, branch)


def tail_kernel(depth, full, routes, joined_ref, grads_ref, part_ref, blocks_ref, inputs_ref, grad_ref,
                out_ref, column_ref, got_in_ref, got_out_ref, total_ref, back_ref, *scratch):
    here = pl.program_id(0)
    count = len(scatter_scratch(depth, full, 1, part_ref.dtype, routes))
    each = len(Exchange.scratch(depth))
    parts = scatter_parts(depth, full, routes, part_ref, out_ref, scratch[:count])
    me = parts[0].me
    early = Exchange(me, blocks_ref, got_in_ref, *scratch[count : count + each])
    late = Exchange(me, back_ref, got_out_ref, *scratch[count + each :])
    chunks = part_ref.shape[0] // grads_ref.shape[0]
    main, ahead = interleaved(parts), (1 + depth) * len(parts)
    slots = [[] for _ in range(chunks)]
    slots[0] += [me.greet_all] + main[: len(parts)] + early.steps
    for n, step in enumerate(main[len(parts) : ahead]):
        slots[1 + n // len(parts)].append(step)
    slots[-1] += main[ahead : ahead + len(parts)]
    for at in range(chunks):
        run_slots(slots, here, at, 1, chunks, at)

    @pl.when(here == 0)
    def _():
        total_ref[...] = jnp.zeros_like(total_ref)
        column_ref[...] = jnp.zeros_like(column_ref)

    grads = grads_ref[...]
    column_ref[...] += jnp.sum(grads.astype(jnp.float32), 0, keepdims=True)
    total_ref[...] += lax.dot_general(joined_ref[...], grads, TN, preferred_element_type=jnp.float32)

    @pl.when(here == chunks - 1)
    def _():
        depth_rows = back_ref.shape[1]
        for n in range(total_ref.shape[1] // SIDE):
            turned_part = total_ref[:, n * SIDE : (n + 1) * SIDE].T.astype(back_ref.dtype)
            for m in range(SIDE // depth_rows):
                back_ref[n * (SIDE // depth_rows) + m] = turned_part[m * depth_rows : (m + 1) * depth_rows]
        for step in late.steps + main[ahead + len(parts) :]:
            step()

        @pl.loop(0, full // 32)
        def _(i):
            rows = pl.ds(pl.multiple_of(i * 32, 32), 32)
            hat, inv_std = layer_norm(inputs_ref[rows, :].astype(jnp.float32))
            d_hat = out_ref[rows, :]
            d_hat = d_hat - jnp.mean(d_hat, -1, keepdims=True) - hat * jnp.mean(d_hat * hat, -1, keepdims=True)
            out_ref[rows, :] = inv_std * d_hat + grad_ref[rows, :].astype(jnp.float32)

        for part in parts + [early, late]:
            part.finish()


def tail(joined, grads_all, part, blocks, inputs, grads, depth, routes, collective_id):
    tokens, width = part.shape
    joined_width = joined.shape[1]
    devices = depth * 8
    rows = tokens // devices
    chunk = 2 * SIDE
    back = (devices, width // devices, joined_width)
    here = pl.BlockSpec(memory_space=pl.ANY)

    def whole(shape, **mode):
        return pl.BlockSpec(shape, lambda i: (0, 0), **mode)

    def some(columns):
        return pl.BlockSpec((chunk, columns), lambda i: (i, 0))

    once = {"pipeline_mode": pl.Buffered(1)}
    return pl.pallas_call(
        functools.partial(tail_kernel, depth, rows, routes),
        grid=(tokens // chunk,),
        out_shape=(
            jax.ShapeDtypeStruct((rows, width), jnp.float32),
            jax.ShapeDtypeStruct((1, width), jnp.float32),
            jax.ShapeDtypeStruct(blocks.shape, blocks.dtype),
            jax.ShapeDtypeStruct(back, joined.dtype),
        ),
        in_specs=[some(joined_width), some(width), here, here, whole(inputs.shape, **once), whole(grads.shape, **once)],
        out_specs=(whole((rows, width)), whole((1, width)), here, here),
        scratch_shapes=[pltpu.VMEM((joined_width, width), jnp.float32), pltpu.VMEM(back, joined.dtype)]
        + scatter_scratch(depth, rows, width, part.dtype, routes)
        + Exchange.scratch(depth)
        + Exchange.scratch(depth),
        compiler_params=pltpu.CompilerParams(collective_id=collective_id, has_side_effects=True, vmem_limit_bytes=60 << 20),
    )(joined, grads_all, part, blocks, inputs, grads)


def on_device(
    hidden_in, w_in_t, in_bias, ln_gain, ln_shift, w_out_t, out_bias, segment_ids, out_grad
):
    depth = lax.axis_size("dp")
    devices = depth * lax.axis_size("ctx")
    ctx = lax.axis_index("ctx")
    me = lax.axis_index("dp") * lax.axis_size("ctx") + ctx
    tok_rows, model_width = hidden_in.shape[1:]
    seq_len = segment_ids.shape[1]
    own = model_width // devices
    in_parts = in_bias.shape[0]
    out_parts = w_out_t.shape[1] // model_width
    in_width = in_parts * own
    joint_width = (in_parts + 1) // 2 * LANES

    gain, shift = ln_gain.astype(jnp.float32).T, ln_shift.astype(jnp.float32).T
    own_seg = lax.dynamic_slice_in_dim(segment_ids[0], ctx * tok_rows, tok_rows)
    begin = jnp.sum((segment_ids < own_seg[:, None]).astype(jnp.int32), 1)
    begin = jnp.stack([begin // 256, begin % 256]).reshape(-1, own).T.astype(jnp.float32)
    extra = jnp.concatenate(
        [jnp.zeros((own, LANES // 2)), gain, shift, begin, jnp.zeros((own, LANES // 2 - 2 - begin.shape[1]))], 1
    )
    inputs = hidden_in[0]
    hat_all, got = head(inputs, w_in_t.T, w_out_t, (in_parts, out_parts), gain, extra, depth, ("zf", "fz"), 0)

    weights = got.reshape(model_width, -1)
    half = ROT // 2
    lane = jnp.arange(LANES) % HD
    frequency = 10000.0 ** (-2.0 * (lane % half).astype(jnp.float32) / ROT)
    waves = jnp.stack([jnp.where(lane < ROT, frequency, 0.0), jnp.where(lane < half, -1.0, 1.0)])
    bias = jnp.pad(in_bias.astype(jnp.float32).reshape(1, in_width), ((0, 0), (0, joint_width - in_width)))
    column = jnp.arange(model_width) // own
    out_row = jnp.where(column == me, jnp.tile(out_bias.astype(jnp.float32), devices), 0.0)[None]
    qk, mid, cosine, sine, joined, branch, g_all = forward(
        hat_all, weights, joint_width, bias, waves, out_row, out_grad[0], depth, seq_len, ("zf", "fz"), 1
    )
    d_hat_part, joint_sums, back_in, branch_own = backward(
        g_all, hat_all, weights, joint_width, qk, mid, cosine, sine, branch, depth, seq_len, ROUTES, 2
    )
    result = (inputs.astype(jnp.float32) + branch_own.astype(jnp.float32)).astype(jnp.bfloat16)
    d_input, column_sums, back_in, back_out = tail(
        joined, g_all, d_hat_part, back_in.reshape(devices, own, -1), inputs, out_grad[0], depth, ROUTES, 3
    )
    grad_w_out, _ = join_blocks(back_out, out_parts)
    grad_w_in, vectors = join_blocks(back_in, in_parts)
    return (
        result[None],
        d_input[None],
        grad_w_in.T,
        joint_sums[:, :in_width].reshape(in_parts, own),
        vectors[:, LANES // 2][None],
        vectors[:, LANES // 2 + 1][None],
        grad_w_out,
        lax.dynamic_slice_in_dim(column_sums[0], me * own, own),
    )


def solution(mesh):
    in_specs = (
        P("dp", "ctx", None),
        P(None, ("dp", "ctx")),
        P(None, ("dp", "ctx")),
        P(None, ("dp", "ctx")),
        P(None, ("dp", "ctx")),
        P(("dp", "ctx"), None),
        P(("dp", "ctx")),
        P("dp", None),
        P("dp", "ctx", None),
    )
    out_specs = (
        P("dp", "ctx", None),
        P("dp", "ctx", None),
        P(None, ("dp", "ctx")),
        P(None, ("dp", "ctx")),
        P(None, ("dp", "ctx")),
        P(None, ("dp", "ctx")),
        P(("dp", "ctx"), None),
        P(("dp", "ctx")),
    )
    tensor_parallel = mesh.shape["ctx"] == 8 and mesh.shape["dp"] * 8 == H
    body = on_device if tensor_parallel else on_device_gathered
    return jax.shard_map(
        body, mesh=mesh, in_specs=in_specs, out_specs=out_specs, check_vma=False
    )
```

```python
import functools
import math

import jax
import jax.numpy as jnp
import numpy as np
from jax import lax
from jax.experimental import pallas as pl
from jax.experimental.pallas import tpu as pltpu
from jax.sharding import PartitionSpec as P

H = 32
HD = 64
ROT = 32
KEY_BLOCK = 512


epsilon = 1e-05
negative = -1e30


def rotation_tables(positions):
    half_dims = ROT // 2
    frequency = 10000.0 ** (-2.0 * jnp.arange(half_dims, dtype=jnp.float32) / ROT)
    angles = positions[:, None] * frequency[None, :]
    return (jnp.cos(angles)[:, None, :], jnp.sin(angles)[:, None, :])


def rotate(heads_in, cosine_table, sine_table, direction):
    half_dims = ROT // 2
    first_half = heads_in[..., :half_dims]
    second_half = heads_in[..., half_dims:ROT]
    return jnp.concatenate(
        [
            first_half * cosine_table - direction * second_half * sine_table,
            second_half * cosine_table + direction * first_half * sine_table,
            heads_in[..., ROT:],
        ],
        -1,
    )


def masked_scores(queries, key_rows, key_seg, key_index, query_seg, query_index):
    scaling = queries.shape[2] ** (-0.5)
    scores = (
        jnp.einsum("thd,khd->htk", queries, key_rows, preferred_element_type=jnp.float32) * scaling
    )
    allowed = (query_seg[:, None] == key_seg[None, :]) & (
        query_index[:, None] >= key_index[None, :]
    )
    return (jnp.where(allowed[None], scores, negative), allowed)


def score_grads(
    query_part,
    dout_part,
    lse_part,
    dot_part,
    query_seg,
    query_index,
    key_rows,
    value_rows,
    key_seg,
    key_index,
):
    scores, allowed = masked_scores(
        query_part, key_rows, key_seg, key_index, query_seg, query_index
    )
    weights = jnp.where(allowed[None], jnp.exp(scores - lse_part[..., None]), 0.0)
    d_weights = jnp.einsum(
        "thd,khd->htk", dout_part, value_rows, preferred_element_type=jnp.float32
    )
    d_scores = (weights * (d_weights - dot_part[..., None])).astype(jnp.bfloat16)
    return (weights.astype(jnp.bfloat16), d_scores)


def key_grads(
    key_rows,
    value_rows,
    key_seg,
    key_index,
    query_src,
    dout_src,
    lse_src,
    dot_src,
    seg_src,
    index_src,
    query_block,
):
    key_count = key_rows.shape[0]
    scaling = HD ** (-0.5)
    block_count = query_src.shape[0] // query_block

    def query_step(running, block_no):
        weights_low, d_scores = score_grads(
            query_src,
            dout_src,
            lse_src,
            dot_src,
            seg_src,
            index_src,
            key_rows,
            value_rows,
            key_seg,
            key_index,
        )
        d_key = (
            running[0]
            + jnp.einsum("htk,thd->khd", d_scores, query_src, preferred_element_type=jnp.float32)
            * scaling
        )
        d_value = running[1] + jnp.einsum(
            "htk,thd->khd", weights_low, dout_src, preferred_element_type=jnp.float32
        )
        return ((d_key, d_value), None)

    zero_heads = jnp.zeros((key_count, H, HD), jnp.float32)
    (d_key, d_value), _ = lax.scan(query_step, (zero_heads, zero_heads), jnp.arange(block_count))
    return (d_key.reshape(key_count, H * HD), d_value.reshape(key_count, H * HD))


def on_device_gathered(
    hidden_in, w_in_t, in_bias, ln_gain, ln_shift, w_out_t, out_bias, segment_ids, out_grad
):
    inputs = hidden_in[0].astype(jnp.float32)
    tok_rows, model_width = inputs.shape
    seg_row = segment_ids[0]
    seq_len = seg_row.shape[0]
    offset = lax.axis_index("ctx") * tok_rows
    index_all = jnp.arange(seq_len, dtype=jnp.int32)
    earlier = jnp.concatenate([seg_row[:1], seg_row[:-1]])
    begins = jnp.where((index_all == 0) | (seg_row != earlier), index_all, 0)
    positions = (index_all - lax.cummax(begins, axis=0)).astype(jnp.float32)
    local_pos = lax.dynamic_slice_in_dim(positions, offset, tok_rows)
    query_seg = lax.dynamic_slice_in_dim(seg_row, offset, tok_rows)
    query_index = offset + jnp.arange(tok_rows, dtype=jnp.int32)
    cosine_table, sine_table = rotation_tables(local_pos)
    scaling = HD ** (-0.5)
    average = jnp.mean(inputs, -1, keepdims=True)
    centred = inputs - average
    inv_std = lax.rsqrt(jnp.mean(centred * centred, -1, keepdims=True) + epsilon)
    normed_hat = centred * inv_std
    joint_width = w_in_t.shape[0]
    bias_rows = in_bias.shape[0]
    weight_piece = lax.all_gather(w_in_t, ("dp", "ctx"), axis=1, tiled=True)
    bias_piece = lax.all_gather(in_bias, ("dp", "ctx"), axis=1, tiled=True)
    gain_piece = lax.all_gather(ln_gain, ("dp", "ctx"), axis=1, tiled=True)
    shift_piece = lax.all_gather(ln_shift, ("dp", "ctx"), axis=1, tiled=True)
    normed_piece = (
        normed_hat * gain_piece.astype(jnp.float32) + shift_piece.astype(jnp.float32)
    ).astype(jnp.bfloat16)
    summed = lax.dot_general(
        normed_piece, weight_piece, (((1,), (1,)), ((), ())), preferred_element_type=jnp.float32
    )
    gain_all = gain_piece.astype(jnp.float32)
    bias_all = bias_piece.astype(jnp.float32)
    projected, normed, gain_all, bias_all = (summed, normed_piece, gain_all, bias_all)
    projected = projected + bias_all.reshape(1, joint_width)
    queries = rotate(
        projected[:, :model_width].reshape(tok_rows, H, HD), cosine_table, sine_table, 1.0
    ).astype(jnp.bfloat16)
    keys_new = (
        rotate(
            projected[:, model_width : 2 * model_width].reshape(tok_rows, H, HD),
            cosine_table,
            sine_table,
            1.0,
        )
        .astype(jnp.bfloat16)
        .reshape(tok_rows, model_width)
    )
    values_new = projected[:, 2 * model_width : 3 * model_width].astype(jnp.bfloat16)
    pre_gelu = projected[:, 3 * model_width :]
    keys_all, values_all = (
        lax.all_gather(keys_new, "ctx", axis=0, tiled=True),
        lax.all_gather(values_new, "ctx", axis=0, tiled=True),
    )
    block_count = seq_len // KEY_BLOCK

    def key_slice(first_key, key_count):
        key_rows = lax.dynamic_slice_in_dim(keys_all, first_key, key_count, 0).reshape(
            key_count, H, HD
        )
        value_rows = lax.dynamic_slice_in_dim(values_all, first_key, key_count, 0).reshape(
            key_count, H, HD
        )
        key_seg = lax.dynamic_slice_in_dim(seg_row, first_key, key_count)
        key_index = first_key + jnp.arange(key_count, dtype=jnp.int32)
        return (key_rows, value_rows, key_seg, key_index)

    def stats_step(running, block_no):
        running_max, running_sum = running
        key_rows, value_rows, key_seg, key_index = key_slice(block_no * KEY_BLOCK, KEY_BLOCK)
        scores, allowed = masked_scores(
            queries, key_rows, key_seg, key_index, query_seg, query_index
        )
        new_max = jnp.maximum(running_max, jnp.max(scores, -1))
        weights = jnp.where(allowed[None], jnp.exp(scores - new_max[..., None]), 0.0)
        running_sum = running_sum * jnp.exp(running_max - new_max) + jnp.sum(weights, -1)
        return ((new_max, running_sum), None)

    stats_init = (
        jnp.full((H, tok_rows), negative, jnp.float32),
        jnp.zeros((H, tok_rows), jnp.float32),
    )
    (final_max, final_sum), _ = lax.scan(stats_step, stats_init, jnp.arange(block_count))
    log_total = final_max + jnp.log(final_sum)

    def value_step(attended, block_no):
        key_rows, value_rows, key_seg, key_index = key_slice(block_no * KEY_BLOCK, KEY_BLOCK)
        scores, allowed = masked_scores(
            queries, key_rows, key_seg, key_index, query_seg, query_index
        )
        weights = jnp.where(allowed[None], jnp.exp(scores - log_total[..., None]), 0.0).astype(
            jnp.bfloat16
        )
        attended = attended + jnp.einsum(
            "htk,khd->thd", weights, value_rows, preferred_element_type=jnp.float32
        )
        return (attended, None)

    attended, _ = lax.scan(
        value_step, jnp.zeros((tok_rows, H, HD), jnp.float32), jnp.arange(block_count)
    )
    hidden = jax.nn.gelu(pre_gelu, approximate=True).astype(jnp.bfloat16)
    joined = jnp.concatenate(
        [attended.reshape(tok_rows, model_width).astype(jnp.bfloat16), hidden], 1
    )
    weight_piece, bias_piece = lax.all_gather(
        (w_out_t, out_bias), ("dp", "ctx"), axis=0, tiled=True
    )
    branch = (
        lax.dot_general(
            joined, weight_piece, (((1,), (1,)), ((), ())), preferred_element_type=jnp.float32
        )
        + bias_piece.astype(jnp.float32)[None, :]
    )
    result = (inputs + branch).astype(jnp.bfloat16)
    cotangent = out_grad[0]
    grad_part = cotangent
    d_joined = jnp.dot(
        grad_part,
        lax.all_gather(w_out_t, ("dp", "ctx"), axis=0, tiled=True),
        preferred_element_type=jnp.float32,
    )
    d_attn = d_joined[:, :model_width].astype(jnp.bfloat16).reshape(tok_rows, H, HD)

    def gelu_tanh(pre_values):
        return jax.nn.gelu(pre_values, approximate=True)

    _, gelu_pull = jax.vjp(gelu_tanh, pre_gelu)
    d_pre = gelu_pull(d_joined[:, model_width:])[0]
    row_dots = jnp.einsum("thd,thd->ht", d_attn.astype(jnp.float32), attended)

    def query_grad_step(d_query, block_no):
        key_rows, value_rows, key_seg, key_index = key_slice(block_no * KEY_BLOCK, KEY_BLOCK)
        _, d_scores = score_grads(
            queries,
            d_attn,
            log_total,
            row_dots,
            query_seg,
            query_index,
            key_rows,
            value_rows,
            key_seg,
            key_index,
        )
        d_query = (
            d_query
            + jnp.einsum("htk,khd->thd", d_scores, key_rows, preferred_element_type=jnp.float32)
            * scaling
        )
        return (d_query, None)

    d_query, _ = lax.scan(
        query_grad_step, jnp.zeros((tok_rows, H, HD), jnp.float32), jnp.arange(block_count)
    )
    count = lax.axis_size("ctx") * tok_rows
    sub_rows = math.gcd(count, KEY_BLOCK)

    def sub_step(carry_none, block_no):
        key_rows, value_rows, key_seg, key_index = key_slice(block_no * sub_rows, sub_rows)
        d_key, d_value = key_grads(
            key_rows,
            value_rows,
            key_seg,
            key_index,
            queries,
            d_attn,
            log_total,
            row_dots,
            query_seg,
            query_index,
            tok_rows,
        )
        return (carry_none, jnp.concatenate([d_key, d_value], 1))

    _, stacked = lax.scan(sub_step, jnp.zeros((), jnp.float32), jnp.arange(count // sub_rows))
    d_kv = lax.psum_scatter(
        stacked.reshape(count, 2 * model_width).astype(jnp.bfloat16),
        "ctx",
        scatter_dimension=0,
        tiled=True,
    ).astype(jnp.float32)
    d_key_local, d_value_local = (d_kv[:, :model_width], d_kv[:, model_width:])
    d_query_pre = rotate(d_query, cosine_table, sine_table, -1.0).reshape(tok_rows, model_width)
    d_key_pre = rotate(
        d_key_local.reshape(tok_rows, H, HD), cosine_table, sine_table, -1.0
    ).reshape(tok_rows, model_width)
    d_joint = jnp.concatenate([d_query_pre, d_key_pre, d_value_local, d_pre], 1).astype(
        jnp.bfloat16
    )
    d_normed = jnp.dot(
        d_joint,
        lax.all_gather(w_in_t, ("dp", "ctx"), axis=1, tiled=True),
        preferred_element_type=jnp.float32,
    )
    grad_part = cotangent
    in_term = lax.dot_general(
        normed, d_joint, (((0,), (0,)), ((), ())), preferred_element_type=jnp.float32
    )
    out_term = lax.dot_general(
        grad_part, joined, (((0,), (0,)), ((), ())), preferred_element_type=jnp.float32
    )
    grad_rows = lax.psum_scatter(
        jnp.concatenate([in_term, out_term], 1), ("dp", "ctx"), scatter_dimension=0, tiled=True
    )
    grad_w_in = grad_rows[:, :joint_width].T
    grad_w_out = grad_rows[:, joint_width:]
    grad_bias_in = jnp.sum(d_joint.astype(jnp.float32), 0).reshape(bias_rows, model_width)
    grad_gain_row = jnp.sum(d_normed * normed_hat, 0, keepdims=True)
    grad_shift_row = jnp.sum(d_normed, 0, keepdims=True)
    grad_bias_out = jnp.sum(cotangent.astype(jnp.float32), 0, keepdims=True)
    grad_in_bias, grad_gain, grad_shift, grad_out_row = (
        lax.psum_scatter(grad_bias_in, ("dp", "ctx"), scatter_dimension=1, tiled=True),
        lax.psum_scatter(grad_gain_row, ("dp", "ctx"), scatter_dimension=1, tiled=True),
        lax.psum_scatter(grad_shift_row, ("dp", "ctx"), scatter_dimension=1, tiled=True),
        lax.psum_scatter(grad_bias_out, ("dp", "ctx"), scatter_dimension=1, tiled=True),
    )
    d_hat = d_normed * gain_all
    d_input = inv_std * (
        d_hat
        - jnp.mean(d_hat, -1, keepdims=True)
        - normed_hat * jnp.mean(d_hat * normed_hat, -1, keepdims=True)
    ) + cotangent.astype(jnp.float32)
    return (
        result[None],
        d_input[None],
        grad_w_in,
        grad_in_bias,
        grad_gain,
        grad_shift,
        grad_w_out,
        grad_out_row[0],
    )


AXES = ("dp", "ctx")
MESH = pl.DeviceIdType.MESH
class Place:
    def __init__(self, depth):
        self.depth = depth
        self.top = depth - 1
        self.z = lax.axis_index("dp")
        self.c = lax.axis_index("ctx")
        y, x, self.core = self.c // 4, (self.c // 2) % 2, self.c % 2
        self.first_stride = jnp.where(self.core == 0, 2, 4)
        self.last_stride = jnp.where(self.core == 0, 4, 2)
        self.f = jnp.where(self.core == 0, x, y)
        self.l = jnp.where(self.core == 0, y, x)

    def ctx(self, f, l, core):
        return f * self.first_stride + l * self.last_stride + core

    def shard(self, z, f, l, core=None):
        return z * 8 + self.ctx(f, l, self.core if core is None else core)

    def first(self):
        return {"dp": self.z, "ctx": self.ctx(1 - self.f, self.l, self.core)}

    def last(self):
        return {"dp": self.z, "ctx": self.ctx(self.f, 1 - self.l, self.core)}

    def sibling(self):
        return {"dp": self.z, "ctx": self.ctx(self.f, self.l, 1 - self.core)}

    def above(self):
        return {"dp": self.z + 1, "ctx": self.c}

    def below(self):
        return {"dp": self.z - 1, "ctx": self.c}

    def greet(self):
        barrier = pltpu.get_barrier_semaphore()
        for device in (self.first(), self.last(), self.sibling()):
            pl.semaphore_signal(barrier, inc=1, device_id=device, device_id_type=MESH)

        @pl.when(self.z > 0)
        def _():
            pl.semaphore_signal(barrier, inc=1, device_id=self.below(), device_id_type=MESH)

        @pl.when(self.z < self.top)
        def _():
            pl.semaphore_signal(barrier, inc=1, device_id=self.above(), device_id_type=MESH)

        ends = jnp.where(self.z > 0, 1, 0) + jnp.where(self.z < self.top, 1, 0)
        pl.semaphore_wait(barrier, 3 + ends)

    def partner(self, k):
        return {"dp": self.z ^ (k // 8), "ctx": self.c ^ (k % 8)}

    def greet_all(self):
        barrier = pltpu.get_barrier_semaphore()
        for k in range(1, self.depth * 8):
            pl.semaphore_signal(barrier, inc=1, device_id=self.partner(k), device_id_type=MESH)
        pl.semaphore_wait(barrier, self.depth * 8 - 1)

    def choose(self, rule):
        value = jnp.int32(0)
        for z in range(self.depth):
            value = jnp.where(self.z == z, rule(z), value)
        return value

    def near(self, step):
        return self.choose(lambda z: sorted([q for q in range(self.depth) if q != z], key=lambda q: (abs(q - z), q))[step])

    def far(self, step):
        def rule(z):
            ups, downs = list(range(self.top, z, -1)), list(range(z))
            return ((ups + downs if 2 * z < self.depth else downs + ups) + [z])[step]

        return self.choose(rule)


def layer_norm(inputs):
    centred = inputs - jnp.mean(inputs, -1, keepdims=True)
    inv_std = lax.rsqrt(jnp.mean(centred * centred, -1, keepdims=True) + epsilon)
    return centred * inv_std, inv_std


def push(source, target, send, receive, device):
    return pltpu.make_async_remote_copy(
        src_ref=source, dst_ref=target, send_sem=send, recv_sem=receive, device_id=device, device_id_type=MESH
    )


class Gather:
    def __init__(self, me, full, offset, rows, route, own_ref, all_ref, local, sends, arrivals):
        self.me, self.full, self.offset, self.rows, self.route = me, full, offset, rows, route
        self.own_ref, self.all_ref, self.sends, self.arrivals = own_ref.at[pl.ds(offset, rows)], all_ref, sends, arrivals
        self.keep = pltpu.make_async_copy(self.own_ref, self.block(me.shard(me.z, me.f, me.l)), local)
        self.used, self.drains = 0, []
        zs = [me.z] + [me.near(step) for step in range(me.top)]
        pairs = [(z, f) for z in zs for f in (me.f, 1 - me.f)]
        self.steps = [self.begin]
        for n, pair in enumerate(pairs):
            if n:
                self.steps.append(functools.partial(self.relay, n, *pair))
                self.steps.append(functools.partial(self.cross, *pairs[n - 1]))
        self.steps.append(functools.partial(self.cross, *pairs[-1]))

    def block(self, shard):
        return self.all_ref.at[pl.ds(pl.multiple_of(shard * self.full + self.offset, self.rows), self.rows)]

    def send(self, source, shard, device, when=None):
        slot = self.used
        self.used += 1

        def start():
            push(source, self.block(shard), self.sends.at[slot], self.arrivals.at[shard], device).start()

        def drain():
            push(self.own_ref, self.block(0), self.sends.at[slot], self.arrivals.at[0], self.me.sibling()).wait_send()

        if when is None:
            start()
            self.drains.append(drain)
        else:
            pl.when(when())(start)
            self.drains.append(lambda: pl.when(when())(drain))

    def arrived(self, shard):
        push(self.own_ref, self.block(shard), self.sends.at[0], self.arrivals.at[shard], self.me.sibling()).wait_recv()

    def begin(self):
        me = self.me
        shard = me.shard(me.z, me.f, me.l)
        self.send(self.own_ref, shard, me.above(), lambda: me.z < me.top)
        self.send(self.own_ref, shard, me.below(), lambda: me.z > 0)
        self.send(self.own_ref, shard, me.first())
        self.send(self.own_ref, shard, me.last())
        self.send(self.own_ref, shard, me.sibling())
        self.keep.start()

    def relay(self, n, z, f):
        me = self.me
        shard = me.shard(z, f, me.l)
        block = self.block(shard)
        self.arrived(shard)
        if self.route == "zf":
            if n % 2 == 0:
                self.send(block, shard, me.above(), lambda: (z < me.z) & (me.z < me.top))
                self.send(block, shard, me.below(), lambda: (z > me.z) & (me.z > 0))
                self.send(block, shard, me.first())
        else:
            self.send(block, shard, me.above(), lambda: ((z < me.z) if n > 1 else (z == me.z)) & (me.z < me.top))
            self.send(block, shard, me.below(), lambda: ((z > me.z) if n > 1 else (z == me.z)) & (me.z > 0))
        self.send(block, shard, me.last())
        self.send(block, shard, me.sibling())

    def cross(self, z, f):
        me = self.me
        shard = me.shard(z, f, 1 - me.l)
        self.arrived(shard)
        self.send(self.block(shard), shard, me.sibling())

    def finish(self):
        me = self.me
        for z in range(me.depth):
            for f in range(2):
                for l in range(2):
                    self.arrived(me.shard(z, f, l, 1 - me.core))
        self.keep.wait()
        for drain in self.drains:
            drain()


class Exchange:
    def __init__(self, me, blocks_ref, got_ref, local, sends, arrivals):
        self.me, self.blocks_ref, self.got_ref, self.sends, self.arrivals = me, blocks_ref, got_ref, sends, arrivals
        self.mine = me.z * 8 + me.c
        self.keep = pltpu.make_async_copy(blocks_ref.at[self.mine], got_ref.at[self.mine], local)
        order = [high * 8 + low for low in LOWS for high in range(me.depth)]
        self.order = [k for k in order if k]
        self.steps = [functools.partial(self.start, k) for k in self.order] + [self.keep.start]

    def copy(self, k):
        peer = self.me.partner(k)
        other = peer["dp"] * 8 + peer["ctx"]
        return push(self.blocks_ref.at[other], self.got_ref.at[self.mine], self.sends.at[k], self.arrivals.at[k], peer)

    def start(self, k):
        self.copy(k).start()

    def finish(self):
        for k in self.order:
            self.copy(k).wait_recv()
        for k in self.order:
            self.copy(k).wait_send()
        self.keep.wait()

    @staticmethod
    def scratch(depth):
        return [pltpu.SemaphoreType.DMA(()), pltpu.SemaphoreType.DMA((depth * 8,)), pltpu.SemaphoreType.DMA((depth * 8,))]


LOWS = (0, 1, 2, 3, 4, 5, 6, 7)
ROUTES = ("zf", "zf")
ADD_ROWS = 32


def merged(main, side, ahead=0):
    steps, done = list(main[:ahead]), 0
    rest = main[ahead:]
    for n, step in enumerate(rest):
        upto = (n + 1) * len(side) // len(rest)
        steps += side[done:upto] + [step]
        done = upto
    return steps


def interleaved(parts):
    most = max(len(part.steps) for part in parts)
    return [part.steps[n] for n in range(most) for part in parts if n < len(part.steps)]


def gather_parts(depth, full, routes, own_ref, all_ref, scratch):
    me = Place(depth)
    rows = full // len(routes)
    return [
        Gather(me, full, n * rows, rows, route, own_ref, all_ref, *scratch[3 * n : 3 * n + 3]) for n, route in enumerate(routes)
    ]


def gather_scratch(depth, routes):
    return [
        pltpu.SemaphoreType.DMA(()),
        pltpu.SemaphoreType.DMA((9 + 8 * (depth - 1) + 2 * depth,)),
        pltpu.SemaphoreType.DMA((depth * 8,)),
    ] * len(routes)


class Scatter:
    def __init__(self, me, full, offset, rows, route, part_ref, out_ref, sums, from_sib, from_last, from_first, from_below, from_above,
                 loads, send_sib, send_last, send_first, send_line, got_sib, got_last, got_first, got_below, got_above):
        self.me, self.full, self.offset, self.rows, self.route, self.step = me, full, offset, rows, route, min(rows, ADD_ROWS)
        self.part_ref, self.out_ref, self.sums, self.loads = part_ref, out_ref, sums, loads
        self.sib, self.last, self.first = (from_sib, send_sib, got_sib), (from_last, send_last, got_last), (from_first, send_first, got_first)
        self.up, self.down = (from_below, send_line, got_below), (from_above, send_line, got_above)
        self.zs = [me.far(i) for i in range(me.depth)]
        chip = [functools.partial(self.chip, z) for z in self.zs]
        plane = [functools.partial(self.plane, z) for z in self.zs]
        line = [functools.partial(self.line, z) for z in self.zs[:-1]] + [self.final]
        lag = 1 if route == "zf" else 0
        self.steps = [self.begin] + chip
        for i in range(me.depth + lag):
            self.steps += plane[i : i + 1] + (line[i - lag : i - lag + 1] if i >= lag else [])

    def source(self, z, f, l, core):
        row = self.me.shard(z, f, l, core) * self.full + self.offset
        return self.part_ref.at[pl.ds(pl.multiple_of(row, self.rows), self.rows)]

    def at(self, z, f, l):
        return z * 4 + f * 2 + l

    def add(self, target, source):
        @pl.loop(0, self.rows // self.step)
        def _(i):
            part = pl.ds(pl.multiple_of(i * self.step, self.step), self.step)
            target[part, :] = target[part, :] + source[part, :]

    def copy(self, stage, source, slot, device, send_slot=None):
        landing, send, got = stage
        return push(source, landing.at[slot], send.at[slot if send_slot is None else send_slot], got.at[slot], device)

    def to_sibling(self, z, f, l):
        return self.copy(self.sib, self.source(z, f, l, 1 - self.me.core), self.at(z, l, f), self.me.sibling())

    def to_last(self, z, f):
        me = self.me
        return self.copy(self.last, self.sums.at[self.at(z, f, 1 - me.l)], z * 2 + f, me.last())

    def to_first(self, z):
        me = self.me
        return self.copy(self.first, self.sums.at[self.at(z, 1 - me.f, me.l)], z, me.first())

    def held(self, z, f):
        return self.sums.at[self.at(z, f, self.me.l)]

    def slot(self, z, f):
        return z if self.route == "zf" else z * 2 + f

    def along(self, z, f):
        slot = self.slot(z, f)
        return (
            lambda: self.copy(self.up, self.held(z, f), slot, self.me.above()),
            lambda: self.copy(self.down, self.held(z, f), slot, self.me.below()),
        )

    def load(self, z, f, l):
        k = self.at(z, f, l)
        return pltpu.make_async_copy(self.source(z, f, l, self.me.core), self.sums.at[k], self.loads.at[k])

    def pairs(self):
        me = self.me
        return [(f, l) for l in (1 - me.l, me.l) for f in (1 - me.f, me.f)]

    def sides(self):
        return (self.me.f,) if self.route == "zf" else (1 - self.me.f, self.me.f)

    def begin(self):
        me = self.me
        for z in self.zs:
            for f in (1 - me.f, me.f):
                for l in (1 - me.l, me.l):
                    self.to_sibling(z, f, l).start()
            for f, l in self.pairs():
                self.load(z, f, l).start()

    def chip(self, z):
        me = self.me
        for n, (f, l) in enumerate(self.pairs()):
            k = self.at(z, f, l)
            self.load(z, f, l).wait()
            self.copy(self.sib, self.sums.at[k], k, me.sibling()).wait_recv()
            self.add(self.sums.at[k], self.sib[0].at[k])
            if n in (1, 2):
                self.to_last(z, self.pairs()[n - 1][0]).start()

    def plane(self, z):
        me = self.me
        for f in (1 - me.f, me.f):
            self.to_last(z, f).wait_recv()
            self.add(self.held(z, f), self.last[0].at[z * 2 + f])
        if self.route == "zf":
            self.to_first(z).start()

    def from_other_half(self, z):
        self.to_first(z).wait_recv()
        self.add(self.held(z, self.me.f), self.first[0].at[z])

    def line(self, z):
        me = self.me
        if self.route == "zf":
            self.from_other_half(z)
        for f in self.sides():
            upward, downward = self.along(z, f)

            @pl.when((z > me.z) & (me.z > 0))
            def _():
                upward().wait_recv()
                self.add(self.held(z, f), self.up[0].at[self.slot(z, f)])

            @pl.when((z < me.z) & (me.z < me.top))
            def _():
                downward().wait_recv()
                self.add(self.held(z, f), self.down[0].at[self.slot(z, f)])

            @pl.when(z > me.z)
            def _():
                upward().start()

            @pl.when(z < me.z)
            def _():
                downward().start()

    def final(self):
        me = self.me
        z = me.z
        if self.route == "zf":
            self.from_other_half(z)
        for f in self.sides():
            upward, downward = self.along(z, f)

            @pl.when(z > 0)
            def _():
                upward().wait_recv()
                self.add(self.held(z, f), self.up[0].at[self.slot(z, f)])

            @pl.when(z < me.top)
            def _():
                downward().wait_recv()
                self.add(self.held(z, f), self.down[0].at[self.slot(z, f)])

        if self.route != "zf":
            self.to_first(z).start()
            self.from_other_half(z)
        self.out_ref[pl.ds(self.offset, self.rows), :] = self.held(z, me.f)[...].astype(self.out_ref.dtype)

    def finish(self):
        me = self.me
        for i, z in enumerate(self.zs):
            for f, l in self.pairs():
                self.to_sibling(z, f, l).wait_send()
            for f in (1 - me.f, me.f):
                self.to_last(z, f).wait_send()
            if self.route == "zf" or i == me.top:
                self.to_first(z).wait_send()
            if i < me.top:
                for f in self.sides():
                    self.along(z, f)[0]().wait_send()


def scatter_parts(depth, full, routes, part_ref, out_ref, scratch):
    me = Place(depth)
    rows = full // len(routes)
    each = len(scratch) // len(routes)
    return [
        Scatter(me, full, n * rows, rows, route, part_ref, out_ref, *scratch[each * n : each * (n + 1)]) for n, route in enumerate(routes)
    ]


def scatter_scratch(depth, full, width, dtype, routes):
    dma = pltpu.SemaphoreType.DMA
    scratch = []
    for route in routes:
        line = depth if route == "zf" else depth * 2
        counts = [depth * 4, depth * 4, depth * 2, depth, line, line]
        sems = [depth * 4, depth * 4, depth * 2, depth, line, depth * 4, depth * 2, depth, line, line]
        scratch += [pltpu.VMEM((count, full // len(routes), width), dtype) for count in counts]
        scratch += [dma((count,)) for count in sems]
    return scratch


LANES = 128
NT = (((1,), (1,)), ((), ()))
TN = (((0,), (0,)), ((), ()))


def low_half(shape):
    return lax.broadcasted_iota(jnp.int32, shape, 1) < LANES // 2


def swap_halves(block):
    return pltpu.roll(block, LANES // 2, 1)


def split_blocks(parts, width, *refs):
    scale_ref, extra_ref, out_ref = refs[len(parts) :]
    depth = out_ref.shape[1]
    low = low_half((depth, LANES))

    @pl.loop(0, width // LANES)
    def _(m):
        base = 0
        for count, rows_ref in zip(parts, refs):
            for pair in range((count + 1) // 2):

                def piece(part):
                    lanes = pl.ds(pl.multiple_of(part * width + m * LANES, LANES), LANES)
                    values = rows_ref[:, lanes].astype(jnp.float32)
                    return values * scale_ref[...] if base == 0 else values

                first = piece(2 * pair)
                if 2 * pair + 1 < count:
                    second = piece(2 * pair + 1)
                    even = jnp.where(low, first, swap_halves(second))
                    odd = jnp.where(low, swap_halves(first), second)
                else:
                    rest = extra_ref[...] if base == 0 else jnp.zeros_like(first)
                    even = jnp.where(low, first, rest)
                    odd = jnp.where(low, swap_halves(first), rest)
                lanes = slice((base + pair) * LANES, (base + pair + 1) * LANES)
                out_ref[2 * m, :, lanes] = even.astype(out_ref.dtype)
                out_ref[2 * m + 1, :, lanes] = odd.astype(out_ref.dtype)
            base += (count + 1) // 2

def head_kernel(depth, full, routes, parts_out, width, inputs_ref, w_in_ref, w_out_ref, scale_ref, extra_ref, all_ref, got_ref,
                hat_ref, blocks_ref, w_in, w_out, loads, *scratch):
    copies = [
        pltpu.make_async_copy(source, target, loads.at[n]) for n, (source, target) in enumerate(((w_in_ref, w_in), (w_out_ref, w_out)))
    ]
    for copy in copies:
        copy.start()

    @pl.loop(0, full // 32)
    def _(i):
        rows = pl.ds(pl.multiple_of(i * 32, 32), 32)
        hat_ref[rows, :] = layer_norm(inputs_ref[rows, :].astype(jnp.float32))[0].astype(hat_ref.dtype)

    count = len(gather_scratch(depth, routes))
    parts = gather_parts(depth, full, routes, hat_ref, all_ref, scratch[:count])
    exchange = Exchange(parts[0].me, blocks_ref, got_ref, *scratch[count:])
    parts[0].me.greet_all()
    steps = interleaved(parts)
    for step in steps[: len(parts)]:
        step()
    for copy in copies:
        copy.wait()
    split_blocks(parts_out, width, w_in, w_out, scale_ref, extra_ref, blocks_ref)
    for step in merged(steps[len(parts) :], exchange.steps):
        step()
    for part in parts + [exchange]:
        part.finish()


def head(inputs, w_in, w_out, parts_out, scale, extra, depth, routes, collective_id):
    rows, width = inputs.shape
    own = w_in.shape[0]
    devices = depth * 8
    blocks = (devices, own, sum((count + 1) // 2 for count in parts_out) * LANES)
    here, vmem = pl.BlockSpec(memory_space=pl.ANY), pl.BlockSpec(memory_space=pltpu.VMEM)
    return pl.pallas_call(
        functools.partial(head_kernel, depth, rows, routes, parts_out, width),
        out_shape=(
            jax.ShapeDtypeStruct((devices * rows, width), inputs.dtype),
            jax.ShapeDtypeStruct(blocks, inputs.dtype),
        ),
        in_specs=[vmem, here, here, vmem, vmem],
        out_specs=(here, here),
        scratch_shapes=[
            pltpu.VMEM((rows, width), inputs.dtype),
            pltpu.VMEM(blocks, inputs.dtype),
            pltpu.VMEM(w_in.shape, w_in.dtype),
            pltpu.VMEM(w_out.shape, w_out.dtype),
            pltpu.SemaphoreType.DMA((2,)),
        ]
        + gather_scratch(depth, routes)
        + Exchange.scratch(depth),
        compiler_params=pltpu.CompilerParams(collective_id=collective_id, has_side_effects=True, vmem_limit_bytes=HEAD_VMEM),
    )(inputs, w_in, w_out, scale, extra)


def join_kernel(parts, width, blocks_ref, out_ref, extra_ref):
    depth = out_ref.shape[0]
    low = low_half((depth, LANES))
    extra_ref[...] = jnp.zeros_like(extra_ref)

    @pl.loop(0, width // LANES)
    def _(m):
        for pair in range((parts + 1) // 2):
            lanes = slice(pair * LANES, (pair + 1) * LANES)
            even = blocks_ref[2 * m, :, lanes].astype(jnp.float32)
            odd = blocks_ref[2 * m + 1, :, lanes].astype(jnp.float32)
            first = pl.ds(pl.multiple_of(2 * pair * width + m * LANES, LANES), LANES)
            out_ref[:, first] = jnp.where(low, even, swap_halves(odd))
            if 2 * pair + 1 < parts:
                second = pl.ds(pl.multiple_of((2 * pair + 1) * width + m * LANES, LANES), LANES)
                out_ref[:, second] = jnp.where(low, swap_halves(even), odd)
            else:
                extra_ref[...] += even + odd


def join_blocks(blocks, parts):
    count, depth, _ = blocks.shape
    width = count * HD
    return pl.pallas_call(
        functools.partial(join_kernel, parts, width),
        out_shape=(
            jax.ShapeDtypeStruct((depth, parts * width), jnp.float32),
            jax.ShapeDtypeStruct((depth, LANES), jnp.float32),
        ),
        in_specs=[pl.BlockSpec(memory_space=pltpu.VMEM)],
        out_specs=(pl.BlockSpec(memory_space=pltpu.VMEM), pl.BlockSpec(memory_space=pltpu.VMEM)),
        compiler_params=pltpu.CompilerParams(vmem_limit_bytes=24 << 20),
    )(blocks)


SIDE = 256
HEAD_VMEM = 62 << 20


def turned(block, lane):
    shift = ROT // 2
    return jnp.where(lane % HD < shift, pltpu.roll(block, LANES - shift, 1), pltpu.roll(block, shift, 1))


def gelu_and_slope(t):
    scale = math.sqrt(2.0 / math.pi)
    square = t * t
    bent = jnp.tanh(scale * (t + 0.044715 * (square * t)))
    half = 0.5 * (1.0 + bent)
    return t * half, half + 0.5 * t * (1.0 - bent * bent) * scale * (1.0 + 3.0 * 0.044715 * square)


def allowed_keys(start, first_query, keys):
    query = first_query + lax.broadcasted_iota(jnp.int32, (SIDE, keys), 0)
    key = lax.broadcasted_iota(jnp.int32, (SIDE, keys), 1)
    return (key >= start) & (key <= query)


def document_starts(weights_ref, lanes, first, count):
    pieces = []
    for shard in range(count):
        rows = pl.ds(pl.multiple_of((first + shard) * HD, HD), HD)
        block = weights_ref[rows, lanes].astype(jnp.float32)
        pieces += [block[:, HD + 2 + n : HD + 3 + n] * 256.0 + block[:, HD + 4 + n : HD + 5 + n] for n in range(2)]
    return jnp.concatenate(pieces, 0)


def forward_kernel(depth, shard_rows, joint_width, routes, hat_ref, weights_ref, bias_ref, waves_ref, out_bias_ref, grad_ref,
                   qk_ref, mid_ref, cos_ref, sin_ref, joined_ref, out_ref, grads_ref, keys_ref, values_ref, shift_ref, *scratch):
    seq = hat_ref.shape[0]
    here = pl.program_id(0)
    low = low_half((SIDE, LANES))
    lane = lax.broadcasted_iota(jnp.int32, (SIDE, LANES), 1)
    scaling = HD ** (-0.5)
    parts = gather_parts(depth, shard_rows, routes, grad_ref, grads_ref, scratch)
    chunks = seq // SIDE
    slots = spread_steps([parts[0].me.greet] + interleaved(parts), len(parts), depth * 2 * chunks, IDLE, [part.finish for part in parts])
    side_lanes = slice(joint_width - LANES, joint_width)

    for q in range(chunks):
        run_slots(slots, here, 2 * q, depth, 2 * chunks)
        if q == 0:

            @pl.when(here == 0)
            def _():
                total = bias_ref[...]
                for n in range(weights_ref.shape[0] // SIDE):
                    some = slice(n * SIDE, (n + 1) * SIDE)
                    side = weights_ref[some, side_lanes].astype(jnp.float32)
                    ratio = side[:, HD + 1 : HD + 2] / side[:, HD : HD + 1]
                    total = total + jnp.sum(ratio * weights_ref[some, :joint_width].astype(jnp.float32), 0, keepdims=True)
                shift_ref[...] = total

        rows = slice(q * SIDE, (q + 1) * SIDE)
        joint = jnp.dot(hat_ref[rows, :], weights_ref[:, :joint_width], preferred_element_type=jnp.float32) + shift_ref[...]
        per_chunk = SIDE // shard_rows
        start = document_starts(weights_ref, side_lanes, (here * chunks + q) * per_chunk, per_chunk)
        index = q * SIDE + lax.broadcasted_iota(jnp.int32, (SIDE, 1), 0)
        angles = (index.astype(jnp.float32) - start) * waves_ref[0:1, :]
        cosine, sine = jnp.cos(angles), jnp.sin(angles) * waves_ref[1:2, :]
        cos_ref[rows, :] = cosine
        sin_ref[rows, :] = sine
        qk = joint[:, :LANES]
        qk = qk * cosine + turned(qk, lane) * sine
        keys_ref[rows, :] = swap_halves(qk).astype(jnp.bfloat16)
        query = jnp.where(low, qk * scaling, 0.0).astype(jnp.bfloat16)
        qk_ref[rows, :] = qk.astype(jnp.bfloat16)
        values_ref[rows, :] = jnp.where(low, joint[:, LANES : 2 * LANES], 0.0).astype(jnp.bfloat16)
        count = (q + 1) * SIDE
        scores = lax.dot_general(query, keys_ref[:count, :], NT, preferred_element_type=jnp.float32)
        scores = jnp.where(allowed_keys(start.astype(jnp.int32), q * SIDE, count), scores, negative)
        largest = jnp.max(scores, -1, keepdims=True)
        weights = jnp.exp(scores - largest)
        total = jnp.sum(weights, -1, keepdims=True)
        weights = (weights * (1.0 / total)).astype(jnp.bfloat16)
        attended = jnp.dot(weights, values_ref[:count, :], preferred_element_type=jnp.float32)
        run_slots(slots, here, 2 * q + 1, depth, 2 * chunks)
        lse = largest + jnp.log(total)
        hidden, slope = gelu_and_slope(joint[:, LANES : 2 * LANES])
        mid_ref[rows, :LANES] = jnp.where(low, joint[:, LANES : 2 * LANES], slope)
        joined_ref[rows, :LANES] = jnp.where(low, attended, hidden).astype(jnp.bfloat16)
        hidden, slope = gelu_and_slope(joint[:, 2 * LANES : 3 * LANES])
        mid_ref[rows, LANES : 2 * LANES] = slope
        joined_ref[rows, LANES : 2 * LANES] = hidden.astype(jnp.bfloat16)
        hidden, slope = gelu_and_slope(jnp.where(low, joint[:, 3 * LANES :], 0.0))
        mid_ref[rows, 2 * LANES :] = jnp.where(low, slope, lse)
        joined_ref[rows, 2 * LANES :] = hidden.astype(jnp.bfloat16)
        branch = lax.dot_general(joined_ref[rows, :], weights_ref[:, joint_width:], NT, preferred_element_type=jnp.float32)
        out_ref[rows, :] = (branch + out_bias_ref[...]).astype(jnp.bfloat16)

    @pl.when(here == pl.num_programs(0) - 1)
    def _():
        for step in slots[-1]:
            step()


def spread_steps(steps, ahead, count, idle, after):
    slots = [[] for _ in range(count + 1)]
    slots[0] += steps[: 1 + ahead]
    rest = steps[1 + ahead :]
    for n, step in enumerate(rest):
        slots[min(n * (count - idle) // len(rest), count)].append(step)
    slots[-1] += after
    return slots


def run_slots(slots, here, q, blocks, chunks, first=0):
    for block in range(blocks):
        steps = slots[block * chunks + q]
        if steps:

            @pl.when(here == block + first)
            def _():
                for step in steps:
                    step()


def forward(hat_all, weights, joint_width, bias, waves, out_bias, grads, depth, seq, routes, collective_id):
    tokens, width = hat_all.shape
    joined_width = weights.shape[1] - joint_width

    def rows(columns):
        return pl.BlockSpec((seq, columns), lambda b: (b, 0))

    def whole(array):
        return pl.BlockSpec(array.shape, lambda b: (0, 0), pipeline_mode=pl.Buffered(1))

    def out(columns, kind):
        return jax.ShapeDtypeStruct((tokens, columns), kind)

    return pl.pallas_call(
        functools.partial(forward_kernel, depth, grads.shape[0], joint_width, routes),
        grid=(tokens // seq,),
        out_shape=(
            out(LANES, jnp.bfloat16),
            out(joined_width, jnp.float32),
            out(LANES, jnp.float32),
            out(LANES, jnp.float32),
            out(joined_width, jnp.bfloat16),
            out(width, jnp.bfloat16),
            out(width, jnp.bfloat16),
        ),
        in_specs=[rows(width), whole(weights), whole(bias), whole(waves), whole(out_bias), pl.BlockSpec(memory_space=pl.ANY)],
        out_specs=(
            rows(LANES), rows(joined_width), rows(LANES), rows(LANES), rows(joined_width), rows(width),
            pl.BlockSpec(memory_space=pl.ANY),
        ),
        scratch_shapes=[pltpu.VMEM((seq, LANES), jnp.bfloat16)] * 2
        + [pltpu.VMEM((1, joint_width), jnp.float32)]
        + gather_scratch(depth, routes),
        compiler_params=pltpu.CompilerParams(collective_id=collective_id, has_side_effects=True, vmem_limit_bytes=63 << 20),
    )(hat_all, weights, bias, waves, out_bias, grads)


LATEST = 30
IDLE = -4


def backward_kernel(depth, shard_rows, joint_width, routes, grad_ref, hat_ref, weights_ref, qk_ref, mid_ref, cos_ref, sin_ref, branch_ref,
                    d_hat_ref, sums_ref, back_ref, own_ref,
                    keys_ref, values_ref, d_key_ref, d_value_ref, d_query_ref, d_joint_ref, total_ref, *scratch):
    seq = qk_ref.shape[0]
    chunks = seq // SIDE
    here, stage = pl.program_id(0), pl.program_id(1)
    low = low_half((SIDE, LANES))
    lane = lax.broadcasted_iota(jnp.int32, (SIDE, LANES), 1)
    scaling = HD ** (-0.5)
    side_lanes = slice(joint_width - LANES, joint_width)
    parts = scatter_parts(depth, shard_rows, routes, branch_ref, own_ref, scratch)
    main, ahead = interleaved(parts), (1 + depth) * len(parts)
    slots = [[] for _ in range(depth * 2 * chunks)] + [[part.finish for part in parts]]
    slots[0] += [parts[0].me.greet] + main[: len(parts)]
    for n, step in enumerate(main[len(parts) : ahead]):
        slots[1 + n // len(parts)].append(step)
    due = slots[:-1] + [[]]
    for n, step in enumerate(main[ahead:]):
        due[min(1 + depth + n * LATEST // (len(main) - ahead), len(due) - 1)].append(step)
    slots = due[:-1] + [due[-1] + slots[-1]]

    def first_stage(q, rows):
        if q == 0:
            d_key_ref[...] = jnp.zeros_like(d_key_ref)
            d_value_ref[...] = jnp.zeros_like(d_value_ref)

            @pl.when(here == 0)
            def _():
                sums_ref[...] = jnp.zeros_like(sums_ref)
                total_ref[...] = jnp.zeros_like(total_ref)

        d_joined = jnp.dot(grad_ref[...], weights_ref[:, joint_width:], preferred_element_type=jnp.float32)
        per_chunk = SIDE // shard_rows
        start = document_starts(weights_ref, side_lanes, (here * chunks + q) * per_chunk, per_chunk).astype(jnp.int32)
        qk = qk_ref[rows, :].astype(jnp.float32)
        keys_ref[rows, :] = jnp.where(low, swap_halves(qk), 0.0).astype(jnp.bfloat16)
        query = jnp.where(low, qk * scaling, 0.0).astype(jnp.bfloat16)
        values_ref[rows, :] = jnp.where(low, mid_ref[rows, :LANES], 0.0).astype(jnp.bfloat16)
        d_out = jnp.where(low, d_joined[:, :LANES], 0.0).astype(jnp.bfloat16)
        count = (q + 1) * SIDE
        lse = mid_ref[rows, 3 * LANES - 1 : 3 * LANES]
        scores = lax.dot_general(query, keys_ref[:count, :], NT, preferred_element_type=jnp.float32)
        weights = jnp.where(allowed_keys(start, q * SIDE, count), jnp.exp(scores - lse), 0.0)
        d_weights = lax.dot_general(d_out, values_ref[:count, :], NT, preferred_element_type=jnp.float32)
        moved = weights * d_weights
        d_scores = (moved - weights * jnp.sum(moved, -1, keepdims=True)).astype(jnp.bfloat16)
        weights = weights.astype(jnp.bfloat16)
        d_query_ref[rows, :] = jnp.dot(d_scores, keys_ref[:count, :], preferred_element_type=jnp.float32) * scaling
        d_key_ref[:count, :] += lax.dot_general(d_scores, query, TN, preferred_element_type=jnp.float32)
        d_value_ref[:count, :] += lax.dot_general(weights, d_out, TN, preferred_element_type=jnp.float32)
        d_joint_ref[rows, LANES : 2 * LANES] = (d_joined[:, :LANES] * mid_ref[rows, :LANES]).astype(jnp.bfloat16)
        d_joint_ref[rows, 2 * LANES : 3 * LANES] = (
            d_joined[:, LANES : 2 * LANES] * mid_ref[rows, LANES : 2 * LANES]
        ).astype(jnp.bfloat16)
        d_joint_ref[rows, 3 * LANES :] = jnp.where(
            low, d_joined[:, 2 * LANES :] * mid_ref[rows, 2 * LANES :], 0.0
        ).astype(jnp.bfloat16)

    def second_stage(q, rows):
        d_qk = jnp.where(low, d_query_ref[rows, :], swap_halves(d_key_ref[rows, :]))
        d_qk = d_qk * cos_ref[rows, :] - turned(d_qk, lane) * sin_ref[rows, :]
        d_joint_ref[rows, :LANES] = d_qk.astype(jnp.bfloat16)
        d_joint_ref[rows, LANES : 2 * LANES] = jnp.where(
            low, d_value_ref[rows, :], d_joint_ref[rows, LANES : 2 * LANES].astype(jnp.float32)
        ).astype(jnp.bfloat16)
        d_joint = d_joint_ref[rows, :]
        sums_ref[...] += jnp.sum(d_joint.astype(jnp.float32), 0, keepdims=True)
        d_hat = lax.dot_general(d_joint, weights_ref[:, :joint_width], NT, preferred_element_type=jnp.float32)
        d_hat_ref[...] = d_hat.astype(jnp.bfloat16)
        if q % 2 == 1:
            both = slice(rows.start - SIDE, rows.stop)
            total_ref[...] += lax.dot_general(d_joint_ref[both, :], hat_ref[...], TN, preferred_element_type=jnp.float32)

    for at in range(2 * chunks):

        @pl.when(stage == at)
        def _():
            run_slots(slots, here, at, depth, 2 * chunks)
            rows = slice(at % chunks * SIDE, (at % chunks + 1) * SIDE)
            if at < chunks:
                first_stage(at, rows)
            else:
                second_stage(at - chunks, rows)

    @pl.when((here == pl.num_programs(0) - 1) & (stage == 2 * chunks - 1))
    def _():
        side_lane = lax.broadcasted_iota(jnp.int32, (SIDE, LANES), 1)
        for n in range(back_ref.shape[0] // SIDE):
            some = slice(n * SIDE, (n + 1) * SIDE)
            side = weights_ref[some, side_lanes].astype(jnp.float32)
            gain, shift = side[:, HD : HD + 1], side[:, HD + 1 : HD + 2]
            weight = weights_ref[some, :joint_width].astype(jnp.float32)
            total = total_ref[:, some].T
            back = gain * total + shift * sums_ref[...]
            gain_part = jnp.sum(weight * total, 1, keepdims=True) / gain
            shift_part = jnp.sum(weight * sums_ref[...], 1, keepdims=True) / gain
            last = jnp.where(side_lane == HD, gain_part, back[:, side_lanes])
            last = jnp.where(side_lane == HD + 1, shift_part, last)
            back_ref[some, : joint_width - LANES] = back[:, : joint_width - LANES].astype(jnp.bfloat16)
            back_ref[some, side_lanes] = last.astype(jnp.bfloat16)
        for step in slots[-1]:
            step()


def backward(grad_all, hat_all, weights, joint_width, qk, mid, cosine, sine, branch, depth, seq, routes, collective_id):
    tokens, width = grad_all.shape
    joined_width = weights.shape[1] - joint_width
    own = tokens // (depth * 8)
    chunks = seq // SIDE

    def rows(columns):
        return pl.BlockSpec((seq, columns), lambda b, s: (b, 0))

    def whole(shape, **mode):
        return pl.BlockSpec(shape, lambda b, s: (0, 0), **mode)

    def early(columns):
        return pl.BlockSpec((SIDE, columns), lambda b, s: (b * chunks + jnp.minimum(s, chunks - 1), 0))

    def late(columns):
        return pl.BlockSpec((SIDE, columns), lambda b, s: (b * chunks + jnp.maximum(s - chunks, 0), 0))

    return pl.pallas_call(
        functools.partial(backward_kernel, depth, own, joint_width, routes),
        grid=(tokens // seq, 2 * chunks),
        out_shape=(
            jax.ShapeDtypeStruct((tokens, width), jnp.bfloat16),
            jax.ShapeDtypeStruct((1, joint_width), jnp.float32),
            jax.ShapeDtypeStruct((width, joint_width), jnp.bfloat16),
            jax.ShapeDtypeStruct((own, width), jnp.bfloat16),
        ),
        in_specs=[
            early(width),
            pl.BlockSpec((2 * SIDE, width), lambda b, s: ((b * chunks + jnp.maximum(s - chunks, 0)) // 2, 0)),
            whole(weights.shape, pipeline_mode=pl.Buffered(1)),
            rows(LANES), rows(joined_width), rows(LANES), rows(LANES), pl.BlockSpec(memory_space=pl.ANY),
        ],
        out_specs=(late(width), whole((1, joint_width)), whole((width, joint_width)), whole((own, width))),
        scratch_shapes=[pltpu.VMEM((seq, LANES), jnp.bfloat16)] * 2
        + [pltpu.VMEM((seq, LANES), jnp.float32)] * 3
        + [pltpu.VMEM((seq, joint_width), jnp.bfloat16), pltpu.VMEM((joint_width, width), jnp.float32)]
        + scatter_scratch(depth, own, width, branch.dtype, routes),
        compiler_params=pltpu.CompilerParams(collective_id=collective_id, has_side_effects=True, vmem_limit_bytes=63 << 20),
    )(grad_all, hat_all, weights, qk, mid, cosine, sine, branch)


def TAIL(side, main):
    return side + main


def tail_kernel(depth, full, routes, joined_ref, grads_ref, part_ref, blocks_ref, inputs_ref, grad_ref,
                out_ref, column_ref, got_in_ref, got_out_ref, total_ref, back_ref, *scratch):
    here = pl.program_id(0)
    count = len(scatter_scratch(depth, full, 1, part_ref.dtype, routes))
    each = len(Exchange.scratch(depth))
    parts = scatter_parts(depth, full, routes, part_ref, out_ref, scratch[:count])
    me = parts[0].me
    early = Exchange(me, blocks_ref, got_in_ref, *scratch[count : count + each])
    late = Exchange(me, back_ref, got_out_ref, *scratch[count + each :])
    chunks = part_ref.shape[0] // grads_ref.shape[0]
    main, ahead = interleaved(parts), (1 + depth) * len(parts)
    slots = [[] for _ in range(chunks)]
    slots[0] += [me.greet_all] + main[: len(parts)] + early.steps
    for n, step in enumerate(main[len(parts) : ahead]):
        slots[1 + n // len(parts)].append(step)
    slots[-1] += main[ahead : ahead + len(parts)]
    for at in range(chunks):
        run_slots(slots, here, at, 1, chunks, at)

    @pl.when(here == 0)
    def _():
        total_ref[...] = jnp.zeros_like(total_ref)
        column_ref[...] = jnp.zeros_like(column_ref)

    grads = grads_ref[...]
    column_ref[...] += jnp.sum(grads.astype(jnp.float32), 0, keepdims=True)
    total_ref[...] += lax.dot_general(joined_ref[...], grads, TN, preferred_element_type=jnp.float32)

    @pl.when(here == chunks - 1)
    def _():
        depth_rows = back_ref.shape[1]
        for n in range(total_ref.shape[1] // SIDE):
            turned_part = total_ref[:, n * SIDE : (n + 1) * SIDE].T.astype(back_ref.dtype)
            for m in range(SIDE // depth_rows):
                back_ref[n * (SIDE // depth_rows) + m] = turned_part[m * depth_rows : (m + 1) * depth_rows]
        for step in TAIL(late.steps, main[ahead + len(parts) :]):
            step()

        @pl.loop(0, full // 32)
        def _(i):
            rows = pl.ds(pl.multiple_of(i * 32, 32), 32)
            hat, inv_std = layer_norm(inputs_ref[rows, :].astype(jnp.float32))
            d_hat = out_ref[rows, :]
            d_hat = d_hat - jnp.mean(d_hat, -1, keepdims=True) - hat * jnp.mean(d_hat * hat, -1, keepdims=True)
            out_ref[rows, :] = inv_std * d_hat + grad_ref[rows, :].astype(jnp.float32)

        for part in parts + [early, late]:
            part.finish()


def tail(joined, grads_all, part, blocks, inputs, grads, depth, routes, collective_id):
    tokens, width = part.shape
    joined_width = joined.shape[1]
    devices = depth * 8
    rows = tokens // devices
    chunk = 2 * SIDE
    back = (devices, width // devices, joined_width)
    here = pl.BlockSpec(memory_space=pl.ANY)

    def whole(shape, **mode):
        return pl.BlockSpec(shape, lambda i: (0, 0), **mode)

    def some(columns):
        return pl.BlockSpec((chunk, columns), lambda i: (i, 0))

    once = {"pipeline_mode": pl.Buffered(1)}
    return pl.pallas_call(
        functools.partial(tail_kernel, depth, rows, routes),
        grid=(tokens // chunk,),
        out_shape=(
            jax.ShapeDtypeStruct((rows, width), jnp.float32),
            jax.ShapeDtypeStruct((1, width), jnp.float32),
            jax.ShapeDtypeStruct(blocks.shape, blocks.dtype),
            jax.ShapeDtypeStruct(back, joined.dtype),
        ),
        in_specs=[some(joined_width), some(width), here, here, whole(inputs.shape, **once), whole(grads.shape, **once)],
        out_specs=(whole((rows, width)), whole((1, width)), here, here),
        scratch_shapes=[pltpu.VMEM((joined_width, width), jnp.float32), pltpu.VMEM(back, joined.dtype)]
        + scatter_scratch(depth, rows, width, part.dtype, routes)
        + Exchange.scratch(depth)
        + Exchange.scratch(depth),
        compiler_params=pltpu.CompilerParams(collective_id=collective_id, has_side_effects=True, vmem_limit_bytes=60 << 20),
    )(joined, grads_all, part, blocks, inputs, grads)


def on_device(
    hidden_in, w_in_t, in_bias, ln_gain, ln_shift, w_out_t, out_bias, segment_ids, out_grad
):
    depth = lax.axis_size("dp")
    devices = depth * lax.axis_size("ctx")
    ctx = lax.axis_index("ctx")
    me = lax.axis_index("dp") * lax.axis_size("ctx") + ctx
    tok_rows, model_width = hidden_in.shape[1:]
    seq_len = segment_ids.shape[1]
    own = model_width // devices
    in_parts = in_bias.shape[0]
    out_parts = w_out_t.shape[1] // model_width
    in_width = in_parts * own
    joint_width = (in_parts + 1) // 2 * LANES

    gain, shift = ln_gain.astype(jnp.float32).T, ln_shift.astype(jnp.float32).T
    own_seg = lax.dynamic_slice_in_dim(segment_ids[0], ctx * tok_rows, tok_rows)
    begin = jnp.sum((segment_ids < own_seg[:, None]).astype(jnp.int32), 1)
    begin = jnp.stack([begin // 256, begin % 256]).reshape(-1, own).T.astype(jnp.float32)
    extra = jnp.concatenate(
        [jnp.zeros((own, LANES // 2)), gain, shift, begin, jnp.zeros((own, LANES // 2 - 2 - begin.shape[1]))], 1
    )
    inputs = hidden_in[0]
    hat_all, got = head(inputs, w_in_t.T, w_out_t, (in_parts, out_parts), gain, extra, depth, ("zf", "fz"), 0)

    weights = got.reshape(model_width, -1)
    half = ROT // 2
    lane = np.arange(LANES) % HD
    frequency = np.float32(10000.0) ** (-2.0 * (lane % half).astype(np.float32) / np.float32(ROT))
    waves = np.stack([np.where(lane < ROT, frequency, 0.0), np.where(lane < half, -1.0, 1.0)]).astype(np.float32)
    bias = jnp.pad(in_bias.astype(jnp.float32).reshape(1, in_width), ((0, 0), (0, joint_width - in_width)))
    column = jnp.arange(model_width) // own
    out_row = jnp.where(column == me, jnp.tile(out_bias.astype(jnp.float32), devices), 0.0)[None]
    qk, mid, cosine, sine, joined, branch, g_all = forward(
        hat_all, weights, joint_width, bias, waves, out_row, out_grad[0], depth, seq_len, ("zf", "fz"), 1
    )
    d_hat_part, joint_sums, back_in, branch_own = backward(
        g_all, hat_all, weights, joint_width, qk, mid, cosine, sine, branch, depth, seq_len, ("zf",) * 4, 2
    )
    result = (inputs.astype(jnp.float32) + branch_own.astype(jnp.float32)).astype(jnp.bfloat16)
    d_input, column_sums, back_in, back_out = tail(
        joined, g_all, d_hat_part, back_in.reshape(devices, own, -1), inputs, out_grad[0], depth, ("zf",), 3
    )
    grad_w_out, _ = join_blocks(back_out, out_parts)
    grad_w_in, vectors = join_blocks(back_in, in_parts)
    return (
        result[None],
        d_input[None],
        grad_w_in.T,
        joint_sums[:, :in_width].reshape(in_parts, own),
        vectors[:, LANES // 2][None],
        vectors[:, LANES // 2 + 1][None],
        grad_w_out,
        lax.dynamic_slice_in_dim(column_sums[0], me * own, own),
    )


def solution(mesh):
    in_specs = (
        P("dp", "ctx", None),
        P(None, ("dp", "ctx")),
        P(None, ("dp", "ctx")),
        P(None, ("dp", "ctx")),
        P(None, ("dp", "ctx")),
        P(("dp", "ctx"), None),
        P(("dp", "ctx")),
        P("dp", None),
        P("dp", "ctx", None),
    )
    out_specs = (
        P("dp", "ctx", None),
        P("dp", "ctx", None),
        P(None, ("dp", "ctx")),
        P(None, ("dp", "ctx")),
        P(None, ("dp", "ctx")),
        P(None, ("dp", "ctx")),
        P(("dp", "ctx"), None),
        P(("dp", "ctx")),
    )
    tensor_parallel = mesh.shape["ctx"] == 8 and mesh.shape["dp"] * 8 == H
    body = on_device if tensor_parallel else on_device_gathered
    return jax.shard_map(
        body, mesh=mesh, in_specs=in_specs, out_specs=out_specs, check_vma=False
    )
```

```python
import functools
import math

import jax
import jax.numpy as jnp
import numpy as np
from jax import lax
from jax.experimental import pallas as pl
from jax.experimental.pallas import tpu as pltpu
from jax.sharding import PartitionSpec as P

H = 32
HD = 64
ROT = 32
KEY_BLOCK = 512


epsilon = 1e-05
negative = -1e30


def rotation_tables(positions):
    half_dims = ROT // 2
    frequency = 10000.0 ** (-2.0 * jnp.arange(half_dims, dtype=jnp.float32) / ROT)
    angles = positions[:, None] * frequency[None, :]
    return (jnp.cos(angles)[:, None, :], jnp.sin(angles)[:, None, :])


def rotate(heads_in, cosine_table, sine_table, direction):
    half_dims = ROT // 2
    first_half = heads_in[..., :half_dims]
    second_half = heads_in[..., half_dims:ROT]
    return jnp.concatenate(
        [
            first_half * cosine_table - direction * second_half * sine_table,
            second_half * cosine_table + direction * first_half * sine_table,
            heads_in[..., ROT:],
        ],
        -1,
    )


def masked_scores(queries, key_rows, key_seg, key_index, query_seg, query_index):
    scaling = queries.shape[2] ** (-0.5)
    scores = (
        jnp.einsum("thd,khd->htk", queries, key_rows, preferred_element_type=jnp.float32) * scaling
    )
    allowed = (query_seg[:, None] == key_seg[None, :]) & (
        query_index[:, None] >= key_index[None, :]
    )
    return (jnp.where(allowed[None], scores, negative), allowed)


def score_grads(
    query_part,
    dout_part,
    lse_part,
    dot_part,
    query_seg,
    query_index,
    key_rows,
    value_rows,
    key_seg,
    key_index,
):
    scores, allowed = masked_scores(
        query_part, key_rows, key_seg, key_index, query_seg, query_index
    )
    weights = jnp.where(allowed[None], jnp.exp(scores - lse_part[..., None]), 0.0)
    d_weights = jnp.einsum(
        "thd,khd->htk", dout_part, value_rows, preferred_element_type=jnp.float32
    )
    d_scores = (weights * (d_weights - dot_part[..., None])).astype(jnp.bfloat16)
    return (weights.astype(jnp.bfloat16), d_scores)


def key_grads(
    key_rows,
    value_rows,
    key_seg,
    key_index,
    query_src,
    dout_src,
    lse_src,
    dot_src,
    seg_src,
    index_src,
    query_block,
):
    key_count = key_rows.shape[0]
    scaling = HD ** (-0.5)
    block_count = query_src.shape[0] // query_block

    def query_step(running, block_no):
        weights_low, d_scores = score_grads(
            query_src,
            dout_src,
            lse_src,
            dot_src,
            seg_src,
            index_src,
            key_rows,
            value_rows,
            key_seg,
            key_index,
        )
        d_key = (
            running[0]
            + jnp.einsum("htk,thd->khd", d_scores, query_src, preferred_element_type=jnp.float32)
            * scaling
        )
        d_value = running[1] + jnp.einsum(
            "htk,thd->khd", weights_low, dout_src, preferred_element_type=jnp.float32
        )
        return ((d_key, d_value), None)

    zero_heads = jnp.zeros((key_count, H, HD), jnp.float32)
    (d_key, d_value), _ = lax.scan(query_step, (zero_heads, zero_heads), jnp.arange(block_count))
    return (d_key.reshape(key_count, H * HD), d_value.reshape(key_count, H * HD))


def on_device_gathered(
    hidden_in, w_in_t, in_bias, ln_gain, ln_shift, w_out_t, out_bias, segment_ids, out_grad
):
    inputs = hidden_in[0].astype(jnp.float32)
    tok_rows, model_width = inputs.shape
    seg_row = segment_ids[0]
    seq_len = seg_row.shape[0]
    offset = lax.axis_index("ctx") * tok_rows
    index_all = jnp.arange(seq_len, dtype=jnp.int32)
    earlier = jnp.concatenate([seg_row[:1], seg_row[:-1]])
    begins = jnp.where((index_all == 0) | (seg_row != earlier), index_all, 0)
    positions = (index_all - lax.cummax(begins, axis=0)).astype(jnp.float32)
    local_pos = lax.dynamic_slice_in_dim(positions, offset, tok_rows)
    query_seg = lax.dynamic_slice_in_dim(seg_row, offset, tok_rows)
    query_index = offset + jnp.arange(tok_rows, dtype=jnp.int32)
    cosine_table, sine_table = rotation_tables(local_pos)
    scaling = HD ** (-0.5)
    average = jnp.mean(inputs, -1, keepdims=True)
    centred = inputs - average
    inv_std = lax.rsqrt(jnp.mean(centred * centred, -1, keepdims=True) + epsilon)
    normed_hat = centred * inv_std
    joint_width = w_in_t.shape[0]
    bias_rows = in_bias.shape[0]
    weight_piece = lax.all_gather(w_in_t, ("dp", "ctx"), axis=1, tiled=True)
    bias_piece = lax.all_gather(in_bias, ("dp", "ctx"), axis=1, tiled=True)
    gain_piece = lax.all_gather(ln_gain, ("dp", "ctx"), axis=1, tiled=True)
    shift_piece = lax.all_gather(ln_shift, ("dp", "ctx"), axis=1, tiled=True)
    normed_piece = (
        normed_hat * gain_piece.astype(jnp.float32) + shift_piece.astype(jnp.float32)
    ).astype(jnp.bfloat16)
    summed = lax.dot_general(
        normed_piece, weight_piece, (((1,), (1,)), ((), ())), preferred_element_type=jnp.float32
    )
    gain_all = gain_piece.astype(jnp.float32)
    bias_all = bias_piece.astype(jnp.float32)
    projected, normed, gain_all, bias_all = (summed, normed_piece, gain_all, bias_all)
    projected = projected + bias_all.reshape(1, joint_width)
    queries = rotate(
        projected[:, :model_width].reshape(tok_rows, H, HD), cosine_table, sine_table, 1.0
    ).astype(jnp.bfloat16)
    keys_new = (
        rotate(
            projected[:, model_width : 2 * model_width].reshape(tok_rows, H, HD),
            cosine_table,
            sine_table,
            1.0,
        )
        .astype(jnp.bfloat16)
        .reshape(tok_rows, model_width)
    )
    values_new = projected[:, 2 * model_width : 3 * model_width].astype(jnp.bfloat16)
    pre_gelu = projected[:, 3 * model_width :]
    keys_all, values_all = (
        lax.all_gather(keys_new, "ctx", axis=0, tiled=True),
        lax.all_gather(values_new, "ctx", axis=0, tiled=True),
    )
    block_count = seq_len // KEY_BLOCK

    def key_slice(first_key, key_count):
        key_rows = lax.dynamic_slice_in_dim(keys_all, first_key, key_count, 0).reshape(
            key_count, H, HD
        )
        value_rows = lax.dynamic_slice_in_dim(values_all, first_key, key_count, 0).reshape(
            key_count, H, HD
        )
        key_seg = lax.dynamic_slice_in_dim(seg_row, first_key, key_count)
        key_index = first_key + jnp.arange(key_count, dtype=jnp.int32)
        return (key_rows, value_rows, key_seg, key_index)

    def stats_step(running, block_no):
        running_max, running_sum = running
        key_rows, value_rows, key_seg, key_index = key_slice(block_no * KEY_BLOCK, KEY_BLOCK)
        scores, allowed = masked_scores(
            queries, key_rows, key_seg, key_index, query_seg, query_index
        )
        new_max = jnp.maximum(running_max, jnp.max(scores, -1))
        weights = jnp.where(allowed[None], jnp.exp(scores - new_max[..., None]), 0.0)
        running_sum = running_sum * jnp.exp(running_max - new_max) + jnp.sum(weights, -1)
        return ((new_max, running_sum), None)

    stats_init = (
        jnp.full((H, tok_rows), negative, jnp.float32),
        jnp.zeros((H, tok_rows), jnp.float32),
    )
    (final_max, final_sum), _ = lax.scan(stats_step, stats_init, jnp.arange(block_count))
    log_total = final_max + jnp.log(final_sum)

    def value_step(attended, block_no):
        key_rows, value_rows, key_seg, key_index = key_slice(block_no * KEY_BLOCK, KEY_BLOCK)
        scores, allowed = masked_scores(
            queries, key_rows, key_seg, key_index, query_seg, query_index
        )
        weights = jnp.where(allowed[None], jnp.exp(scores - log_total[..., None]), 0.0).astype(
            jnp.bfloat16
        )
        attended = attended + jnp.einsum(
            "htk,khd->thd", weights, value_rows, preferred_element_type=jnp.float32
        )
        return (attended, None)

    attended, _ = lax.scan(
        value_step, jnp.zeros((tok_rows, H, HD), jnp.float32), jnp.arange(block_count)
    )
    hidden = jax.nn.gelu(pre_gelu, approximate=True).astype(jnp.bfloat16)
    joined = jnp.concatenate(
        [attended.reshape(tok_rows, model_width).astype(jnp.bfloat16), hidden], 1
    )
    weight_piece, bias_piece = lax.all_gather(
        (w_out_t, out_bias), ("dp", "ctx"), axis=0, tiled=True
    )
    branch = (
        lax.dot_general(
            joined, weight_piece, (((1,), (1,)), ((), ())), preferred_element_type=jnp.float32
        )
        + bias_piece.astype(jnp.float32)[None, :]
    )
    result = (inputs + branch).astype(jnp.bfloat16)
    cotangent = out_grad[0]
    grad_part = cotangent
    d_joined = jnp.dot(
        grad_part,
        lax.all_gather(w_out_t, ("dp", "ctx"), axis=0, tiled=True),
        preferred_element_type=jnp.float32,
    )
    d_attn = d_joined[:, :model_width].astype(jnp.bfloat16).reshape(tok_rows, H, HD)

    def gelu_tanh(pre_values):
        return jax.nn.gelu(pre_values, approximate=True)

    _, gelu_pull = jax.vjp(gelu_tanh, pre_gelu)
    d_pre = gelu_pull(d_joined[:, model_width:])[0]
    row_dots = jnp.einsum("thd,thd->ht", d_attn.astype(jnp.float32), attended)

    def query_grad_step(d_query, block_no):
        key_rows, value_rows, key_seg, key_index = key_slice(block_no * KEY_BLOCK, KEY_BLOCK)
        _, d_scores = score_grads(
            queries,
            d_attn,
            log_total,
            row_dots,
            query_seg,
            query_index,
            key_rows,
            value_rows,
            key_seg,
            key_index,
        )
        d_query = (
            d_query
            + jnp.einsum("htk,khd->thd", d_scores, key_rows, preferred_element_type=jnp.float32)
            * scaling
        )
        return (d_query, None)

    d_query, _ = lax.scan(
        query_grad_step, jnp.zeros((tok_rows, H, HD), jnp.float32), jnp.arange(block_count)
    )
    count = lax.axis_size("ctx") * tok_rows
    sub_rows = math.gcd(count, KEY_BLOCK)

    def sub_step(carry_none, block_no):
        key_rows, value_rows, key_seg, key_index = key_slice(block_no * sub_rows, sub_rows)
        d_key, d_value = key_grads(
            key_rows,
            value_rows,
            key_seg,
            key_index,
            queries,
            d_attn,
            log_total,
            row_dots,
            query_seg,
            query_index,
            tok_rows,
        )
        return (carry_none, jnp.concatenate([d_key, d_value], 1))

    _, stacked = lax.scan(sub_step, jnp.zeros((), jnp.float32), jnp.arange(count // sub_rows))
    d_kv = lax.psum_scatter(
        stacked.reshape(count, 2 * model_width).astype(jnp.bfloat16),
        "ctx",
        scatter_dimension=0,
        tiled=True,
    ).astype(jnp.float32)
    d_key_local, d_value_local = (d_kv[:, :model_width], d_kv[:, model_width:])
    d_query_pre = rotate(d_query, cosine_table, sine_table, -1.0).reshape(tok_rows, model_width)
    d_key_pre = rotate(
        d_key_local.reshape(tok_rows, H, HD), cosine_table, sine_table, -1.0
    ).reshape(tok_rows, model_width)
    d_joint = jnp.concatenate([d_query_pre, d_key_pre, d_value_local, d_pre], 1).astype(
        jnp.bfloat16
    )
    d_normed = jnp.dot(
        d_joint,
        lax.all_gather(w_in_t, ("dp", "ctx"), axis=1, tiled=True),
        preferred_element_type=jnp.float32,
    )
    grad_part = cotangent
    in_term = lax.dot_general(
        normed, d_joint, (((0,), (0,)), ((), ())), preferred_element_type=jnp.float32
    )
    out_term = lax.dot_general(
        grad_part, joined, (((0,), (0,)), ((), ())), preferred_element_type=jnp.float32
    )
    grad_rows = lax.psum_scatter(
        jnp.concatenate([in_term, out_term], 1), ("dp", "ctx"), scatter_dimension=0, tiled=True
    )
    grad_w_in = grad_rows[:, :joint_width].T
    grad_w_out = grad_rows[:, joint_width:]
    grad_bias_in = jnp.sum(d_joint.astype(jnp.float32), 0).reshape(bias_rows, model_width)
    grad_gain_row = jnp.sum(d_normed * normed_hat, 0, keepdims=True)
    grad_shift_row = jnp.sum(d_normed, 0, keepdims=True)
    grad_bias_out = jnp.sum(cotangent.astype(jnp.float32), 0, keepdims=True)
    grad_in_bias, grad_gain, grad_shift, grad_out_row = (
        lax.psum_scatter(grad_bias_in, ("dp", "ctx"), scatter_dimension=1, tiled=True),
        lax.psum_scatter(grad_gain_row, ("dp", "ctx"), scatter_dimension=1, tiled=True),
        lax.psum_scatter(grad_shift_row, ("dp", "ctx"), scatter_dimension=1, tiled=True),
        lax.psum_scatter(grad_bias_out, ("dp", "ctx"), scatter_dimension=1, tiled=True),
    )
    d_hat = d_normed * gain_all
    d_input = inv_std * (
        d_hat
        - jnp.mean(d_hat, -1, keepdims=True)
        - normed_hat * jnp.mean(d_hat * normed_hat, -1, keepdims=True)
    ) + cotangent.astype(jnp.float32)
    return (
        result[None],
        d_input[None],
        grad_w_in,
        grad_in_bias,
        grad_gain,
        grad_shift,
        grad_w_out,
        grad_out_row[0],
    )


AXES = ("dp", "ctx")
MESH = pl.DeviceIdType.MESH
class Place:
    def __init__(self, depth):
        self.depth = depth
        self.top = depth - 1
        self.z = lax.axis_index("dp")
        self.c = lax.axis_index("ctx")
        y, x, self.core = self.c // 4, (self.c // 2) % 2, self.c % 2
        self.first_stride = jnp.where(self.core == 0, 2, 4)
        self.last_stride = jnp.where(self.core == 0, 4, 2)
        self.f = jnp.where(self.core == 0, x, y)
        self.l = jnp.where(self.core == 0, y, x)

    def ctx(self, f, l, core):
        return f * self.first_stride + l * self.last_stride + core

    def shard(self, z, f, l, core=None):
        return z * 8 + self.ctx(f, l, self.core if core is None else core)

    def first(self):
        return {"dp": self.z, "ctx": self.ctx(1 - self.f, self.l, self.core)}

    def last(self):
        return {"dp": self.z, "ctx": self.ctx(self.f, 1 - self.l, self.core)}

    def sibling(self):
        return {"dp": self.z, "ctx": self.ctx(self.f, self.l, 1 - self.core)}

    def above(self):
        return {"dp": self.z + 1, "ctx": self.c}

    def below(self):
        return {"dp": self.z - 1, "ctx": self.c}

    def greet(self):
        barrier = pltpu.get_barrier_semaphore()
        for device in (self.first(), self.last(), self.sibling()):
            pl.semaphore_signal(barrier, inc=1, device_id=device, device_id_type=MESH)

        @pl.when(self.z > 0)
        def _():
            pl.semaphore_signal(barrier, inc=1, device_id=self.below(), device_id_type=MESH)

        @pl.when(self.z < self.top)
        def _():
            pl.semaphore_signal(barrier, inc=1, device_id=self.above(), device_id_type=MESH)

        ends = jnp.where(self.z > 0, 1, 0) + jnp.where(self.z < self.top, 1, 0)
        pl.semaphore_wait(barrier, 3 + ends)

    def partner(self, k):
        return {"dp": self.z ^ (k // 8), "ctx": self.c ^ (k % 8)}

    def greet_all(self):
        barrier = pltpu.get_barrier_semaphore()
        for k in range(1, self.depth * 8):
            pl.semaphore_signal(barrier, inc=1, device_id=self.partner(k), device_id_type=MESH)
        pl.semaphore_wait(barrier, self.depth * 8 - 1)

    def choose(self, rule):
        value = jnp.int32(0)
        for z in range(self.depth):
            value = jnp.where(self.z == z, rule(z), value)
        return value

    def near(self, step):
        return self.choose(lambda z: sorted([q for q in range(self.depth) if q != z], key=lambda q: (abs(q - z), q))[step])

    def far(self, step):
        def rule(z):
            ups, downs = list(range(self.top, z, -1)), list(range(z))
            return ((ups + downs if 2 * z < self.depth else downs + ups) + [z])[step]

        return self.choose(rule)


def layer_norm(inputs):
    centred = inputs - jnp.mean(inputs, -1, keepdims=True)
    inv_std = lax.rsqrt(jnp.mean(centred * centred, -1, keepdims=True) + epsilon)
    return centred * inv_std, inv_std


def push(source, target, send, receive, device):
    return pltpu.make_async_remote_copy(
        src_ref=source, dst_ref=target, send_sem=send, recv_sem=receive, device_id=device, device_id_type=MESH
    )


class Gather:
    def __init__(self, me, full, offset, rows, route, own_ref, all_ref, local, sends, arrivals):
        self.me, self.full, self.offset, self.rows, self.route = me, full, offset, rows, route
        self.own_ref, self.all_ref, self.sends, self.arrivals = own_ref.at[pl.ds(offset, rows)], all_ref, sends, arrivals
        self.keep = pltpu.make_async_copy(self.own_ref, self.block(me.shard(me.z, me.f, me.l)), local)
        self.used, self.drains = 0, []
        zs = [me.z] + [me.near(step) for step in range(me.top)]
        pairs = [(z, f) for z in zs for f in (me.f, 1 - me.f)]
        self.steps = [self.begin]
        for n, pair in enumerate(pairs):
            if n:
                self.steps.append(functools.partial(self.relay, n, *pair))
                self.steps.append(functools.partial(self.cross, *pairs[n - 1]))
        self.steps.append(functools.partial(self.cross, *pairs[-1]))

    def block(self, shard):
        return self.all_ref.at[pl.ds(pl.multiple_of(shard * self.full + self.offset, self.rows), self.rows)]

    def send(self, source, shard, device, when=None):
        slot = self.used
        self.used += 1

        def start():
            push(source, self.block(shard), self.sends.at[slot], self.arrivals.at[shard], device).start()

        def drain():
            push(self.own_ref, self.block(0), self.sends.at[slot], self.arrivals.at[0], self.me.sibling()).wait_send()

        if when is None:
            start()
            self.drains.append(drain)
        else:
            pl.when(when())(start)
            self.drains.append(lambda: pl.when(when())(drain))

    def arrived(self, shard):
        push(self.own_ref, self.block(shard), self.sends.at[0], self.arrivals.at[shard], self.me.sibling()).wait_recv()

    def begin(self):
        me = self.me
        shard = me.shard(me.z, me.f, me.l)
        self.send(self.own_ref, shard, me.above(), lambda: me.z < me.top)
        self.send(self.own_ref, shard, me.below(), lambda: me.z > 0)
        self.send(self.own_ref, shard, me.first())
        self.send(self.own_ref, shard, me.last())
        self.send(self.own_ref, shard, me.sibling())
        self.keep.start()

    def relay(self, n, z, f):
        me = self.me
        shard = me.shard(z, f, me.l)
        block = self.block(shard)
        self.arrived(shard)
        if self.route == "zf":
            if n % 2 == 0:
                self.send(block, shard, me.above(), lambda: (z < me.z) & (me.z < me.top))
                self.send(block, shard, me.below(), lambda: (z > me.z) & (me.z > 0))
                self.send(block, shard, me.first())
        else:
            self.send(block, shard, me.above(), lambda: ((z < me.z) if n > 1 else (z == me.z)) & (me.z < me.top))
            self.send(block, shard, me.below(), lambda: ((z > me.z) if n > 1 else (z == me.z)) & (me.z > 0))
        self.send(block, shard, me.last())
        self.send(block, shard, me.sibling())

    def cross(self, z, f):
        me = self.me
        shard = me.shard(z, f, 1 - me.l)
        self.arrived(shard)
        self.send(self.block(shard), shard, me.sibling())

    def finish(self):
        me = self.me
        for z in range(me.depth):
            for f in range(2):
                for l in range(2):
                    self.arrived(me.shard(z, f, l, 1 - me.core))
        self.keep.wait()
        for drain in self.drains:
            drain()


class Exchange:
    def __init__(self, me, blocks_ref, got_ref, local, sends, arrivals):
        self.me, self.blocks_ref, self.got_ref, self.sends, self.arrivals = me, blocks_ref, got_ref, sends, arrivals
        self.mine = me.z * 8 + me.c
        self.keep = pltpu.make_async_copy(blocks_ref.at[self.mine], got_ref.at[self.mine], local)
        order = [high * 8 + low for low in LOWS for high in range(me.depth)]
        self.order = [k for k in order if k]
        self.steps = [functools.partial(self.start, k) for k in self.order] + [self.keep.start]

    def copy(self, k):
        peer = self.me.partner(k)
        other = peer["dp"] * 8 + peer["ctx"]
        return push(self.blocks_ref.at[other], self.got_ref.at[self.mine], self.sends.at[k], self.arrivals.at[k], peer)

    def start(self, k):
        self.copy(k).start()

    def finish(self):
        for k in self.order:
            self.copy(k).wait_recv()
        for k in self.order:
            self.copy(k).wait_send()
        self.keep.wait()

    @staticmethod
    def scratch(depth):
        return [pltpu.SemaphoreType.DMA(()), pltpu.SemaphoreType.DMA((depth * 8,)), pltpu.SemaphoreType.DMA((depth * 8,))]


LOWS = (0, 1, 2, 3, 4, 5, 6, 7)
ROUTES = ("zf", "zf")
ADD_ROWS = 32


def merged(main, side, ahead=0):
    steps, done = list(main[:ahead]), 0
    rest = main[ahead:]
    for n, step in enumerate(rest):
        upto = (n + 1) * len(side) // len(rest)
        steps += side[done:upto] + [step]
        done = upto
    return steps


def interleaved(parts):
    most = max(len(part.steps) for part in parts)
    return [part.steps[n] for n in range(most) for part in parts if n < len(part.steps)]


def gather_parts(depth, full, routes, own_ref, all_ref, scratch):
    me = Place(depth)
    rows = full // len(routes)
    return [
        Gather(me, full, n * rows, rows, route, own_ref, all_ref, *scratch[3 * n : 3 * n + 3]) for n, route in enumerate(routes)
    ]


def gather_scratch(depth, routes):
    return [
        pltpu.SemaphoreType.DMA(()),
        pltpu.SemaphoreType.DMA((9 + 8 * (depth - 1) + 2 * depth,)),
        pltpu.SemaphoreType.DMA((depth * 8,)),
    ] * len(routes)


class Scatter:
    def __init__(self, me, full, offset, rows, route, part_ref, out_ref, sums, from_sib, from_last, from_first, from_below, from_above,
                 loads, send_sib, send_last, send_first, send_line, got_sib, got_last, got_first, got_below, got_above):
        self.me, self.full, self.offset, self.rows, self.route, self.step = me, full, offset, rows, route, min(rows, ADD_ROWS)
        self.part_ref, self.out_ref, self.sums, self.loads = part_ref, out_ref, sums, loads
        self.sib, self.last, self.first = (from_sib, send_sib, got_sib), (from_last, send_last, got_last), (from_first, send_first, got_first)
        self.up, self.down = (from_below, send_line, got_below), (from_above, send_line, got_above)
        self.zs = [me.far(i) for i in range(me.depth)]
        chip = [functools.partial(self.chip, z) for z in self.zs]
        plane = [functools.partial(self.plane, z) for z in self.zs]
        line = [functools.partial(self.line, z) for z in self.zs[:-1]] + [self.final]
        lag = 1 if route == "zf" else 0
        self.steps = [self.begin] + chip
        for i in range(me.depth + lag):
            self.steps += plane[i : i + 1] + (line[i - lag : i - lag + 1] if i >= lag else [])

    def source(self, z, f, l, core):
        row = self.me.shard(z, f, l, core) * self.full + self.offset
        return self.part_ref.at[pl.ds(pl.multiple_of(row, self.rows), self.rows)]

    def at(self, z, f, l):
        return z * 4 + f * 2 + l

    def add(self, target, source):
        @pl.loop(0, self.rows // self.step)
        def _(i):
            part = pl.ds(pl.multiple_of(i * self.step, self.step), self.step)
            target[part, :] = target[part, :] + source[part, :]

    def copy(self, stage, source, slot, device, send_slot=None):
        landing, send, got = stage
        return push(source, landing.at[slot], send.at[slot if send_slot is None else send_slot], got.at[slot], device)

    def to_sibling(self, z, f, l):
        return self.copy(self.sib, self.source(z, f, l, 1 - self.me.core), self.at(z, l, f), self.me.sibling())

    def to_last(self, z, f):
        me = self.me
        return self.copy(self.last, self.sums.at[self.at(z, f, 1 - me.l)], z * 2 + f, me.last())

    def to_first(self, z):
        me = self.me
        return self.copy(self.first, self.sums.at[self.at(z, 1 - me.f, me.l)], z, me.first())

    def held(self, z, f):
        return self.sums.at[self.at(z, f, self.me.l)]

    def slot(self, z, f):
        return z if self.route == "zf" else z * 2 + f

    def along(self, z, f):
        slot = self.slot(z, f)
        return (
            lambda: self.copy(self.up, self.held(z, f), slot, self.me.above()),
            lambda: self.copy(self.down, self.held(z, f), slot, self.me.below()),
        )

    def load(self, z, f, l):
        k = self.at(z, f, l)
        return pltpu.make_async_copy(self.source(z, f, l, self.me.core), self.sums.at[k], self.loads.at[k])

    def pairs(self):
        me = self.me
        return [(f, l) for l in (1 - me.l, me.l) for f in (1 - me.f, me.f)]

    def sides(self):
        return (self.me.f,) if self.route == "zf" else (1 - self.me.f, self.me.f)

    def begin(self):
        me = self.me
        for z in self.zs:
            for f in (1 - me.f, me.f):
                for l in (1 - me.l, me.l):
                    self.to_sibling(z, f, l).start()
            for f, l in self.pairs():
                self.load(z, f, l).start()

    def chip(self, z):
        me = self.me
        for n, (f, l) in enumerate(self.pairs()):
            k = self.at(z, f, l)
            self.load(z, f, l).wait()
            self.copy(self.sib, self.sums.at[k], k, me.sibling()).wait_recv()
            self.add(self.sums.at[k], self.sib[0].at[k])
            if n in (1, 2):
                self.to_last(z, self.pairs()[n - 1][0]).start()

    def plane(self, z):
        me = self.me
        for f in (1 - me.f, me.f):
            self.to_last(z, f).wait_recv()
            self.add(self.held(z, f), self.last[0].at[z * 2 + f])
        if self.route == "zf":
            self.to_first(z).start()

    def from_other_half(self, z):
        self.to_first(z).wait_recv()
        self.add(self.held(z, self.me.f), self.first[0].at[z])

    def line(self, z):
        me = self.me
        if self.route == "zf":
            self.from_other_half(z)
        for f in self.sides():
            upward, downward = self.along(z, f)

            @pl.when((z > me.z) & (me.z > 0))
            def _():
                upward().wait_recv()
                self.add(self.held(z, f), self.up[0].at[self.slot(z, f)])

            @pl.when((z < me.z) & (me.z < me.top))
            def _():
                downward().wait_recv()
                self.add(self.held(z, f), self.down[0].at[self.slot(z, f)])

            @pl.when(z > me.z)
            def _():
                upward().start()

            @pl.when(z < me.z)
            def _():
                downward().start()

    def final(self):
        me = self.me
        z = me.z
        if self.route == "zf":
            self.from_other_half(z)
        for f in self.sides():
            upward, downward = self.along(z, f)

            @pl.when(z > 0)
            def _():
                upward().wait_recv()
                self.add(self.held(z, f), self.up[0].at[self.slot(z, f)])

            @pl.when(z < me.top)
            def _():
                downward().wait_recv()
                self.add(self.held(z, f), self.down[0].at[self.slot(z, f)])

        if self.route != "zf":
            self.to_first(z).start()
            self.from_other_half(z)
        self.out_ref[pl.ds(self.offset, self.rows), :] = self.held(z, me.f)[...].astype(self.out_ref.dtype)

    def finish(self):
        me = self.me
        for i, z in enumerate(self.zs):
            for f, l in self.pairs():
                self.to_sibling(z, f, l).wait_send()
            for f in (1 - me.f, me.f):
                self.to_last(z, f).wait_send()
            if self.route == "zf" or i == me.top:
                self.to_first(z).wait_send()
            if i < me.top:
                for f in self.sides():
                    self.along(z, f)[0]().wait_send()


def scatter_parts(depth, full, routes, part_ref, out_ref, scratch):
    me = Place(depth)
    rows = full // len(routes)
    each = len(scratch) // len(routes)
    return [
        Scatter(me, full, n * rows, rows, route, part_ref, out_ref, *scratch[each * n : each * (n + 1)]) for n, route in enumerate(routes)
    ]


def scatter_scratch(depth, full, width, dtype, routes):
    dma = pltpu.SemaphoreType.DMA
    scratch = []
    for route in routes:
        line = depth if route == "zf" else depth * 2
        counts = [depth * 4, depth * 4, depth * 2, depth, line, line]
        sems = [depth * 4, depth * 4, depth * 2, depth, line, depth * 4, depth * 2, depth, line, line]
        scratch += [pltpu.VMEM((count, full // len(routes), width), dtype) for count in counts]
        scratch += [dma((count,)) for count in sems]
    return scratch


LANES = 128
NT = (((1,), (1,)), ((), ()))
TN = (((0,), (0,)), ((), ()))


def low_half(shape):
    return lax.broadcasted_iota(jnp.int32, shape, 1) < LANES // 2


def swap_halves(block):
    return pltpu.roll(block, LANES // 2, 1)


def split_blocks(parts, width, *refs):
    scale_ref, extra_ref, out_ref = refs[len(parts) :]
    depth = out_ref.shape[1]
    low = low_half((depth, LANES))

    @pl.loop(0, width // LANES)
    def _(m):
        base = 0
        for count, rows_ref in zip(parts, refs):
            for pair in range((count + 1) // 2):

                def piece(part):
                    lanes = pl.ds(pl.multiple_of(part * width + m * LANES, LANES), LANES)
                    values = rows_ref[:, lanes].astype(jnp.float32)
                    return values * scale_ref[...] if base == 0 else values

                first = piece(2 * pair)
                if 2 * pair + 1 < count:
                    second = piece(2 * pair + 1)
                    even = jnp.where(low, first, swap_halves(second))
                    odd = jnp.where(low, swap_halves(first), second)
                else:
                    rest = extra_ref[...] if base == 0 else jnp.zeros_like(first)
                    even = jnp.where(low, first, rest)
                    odd = jnp.where(low, swap_halves(first), rest)
                lanes = slice((base + pair) * LANES, (base + pair + 1) * LANES)
                out_ref[2 * m, :, lanes] = even.astype(out_ref.dtype)
                out_ref[2 * m + 1, :, lanes] = odd.astype(out_ref.dtype)
            base += (count + 1) // 2

def head_kernel(depth, full, routes, parts_out, width, inputs_ref, w_in_ref, w_out_ref, scale_ref, extra_ref, all_ref, got_ref,
                hat_ref, blocks_ref, w_in, w_out, loads, *scratch):
    copies = [
        pltpu.make_async_copy(source, target, loads.at[n]) for n, (source, target) in enumerate(((w_in_ref, w_in), (w_out_ref, w_out)))
    ]
    for copy in copies:
        copy.start()

    @pl.loop(0, full // 32)
    def _(i):
        rows = pl.ds(pl.multiple_of(i * 32, 32), 32)
        hat_ref[rows, :] = layer_norm(inputs_ref[rows, :].astype(jnp.float32))[0].astype(hat_ref.dtype)

    count = len(gather_scratch(depth, routes))
    parts = gather_parts(depth, full, routes, hat_ref, all_ref, scratch[:count])
    exchange = Exchange(parts[0].me, blocks_ref, got_ref, *scratch[count:])
    parts[0].me.greet_all()
    steps = interleaved(parts)
    for step in steps[: len(parts)]:
        step()
    for copy in copies:
        copy.wait()
    split_blocks(parts_out, width, w_in, w_out, scale_ref, extra_ref, blocks_ref)
    for step in merged(steps[len(parts) :], exchange.steps):
        step()
    for part in parts + [exchange]:
        part.finish()


def head(inputs, w_in, w_out, parts_out, scale, extra, depth, routes, collective_id):
    rows, width = inputs.shape
    own = w_in.shape[0]
    devices = depth * 8
    blocks = (devices, own, sum((count + 1) // 2 for count in parts_out) * LANES)
    here, vmem = pl.BlockSpec(memory_space=pl.ANY), pl.BlockSpec(memory_space=pltpu.VMEM)
    return pl.pallas_call(
        functools.partial(head_kernel, depth, rows, routes, parts_out, width),
        out_shape=(
            jax.ShapeDtypeStruct((devices * rows, width), inputs.dtype),
            jax.ShapeDtypeStruct(blocks, inputs.dtype),
        ),
        in_specs=[vmem, here, here, vmem, vmem],
        out_specs=(here, here),
        scratch_shapes=[
            pltpu.VMEM((rows, width), inputs.dtype),
            pltpu.VMEM(blocks, inputs.dtype),
            pltpu.VMEM(w_in.shape, w_in.dtype),
            pltpu.VMEM(w_out.shape, w_out.dtype),
            pltpu.SemaphoreType.DMA((2,)),
        ]
        + gather_scratch(depth, routes)
        + Exchange.scratch(depth),
        compiler_params=pltpu.CompilerParams(collective_id=collective_id, has_side_effects=True, vmem_limit_bytes=HEAD_VMEM),
    )(inputs, w_in, w_out, scale, extra)


def join_kernel(parts, width, blocks_ref, out_ref, extra_ref):
    depth = out_ref.shape[0]
    low = low_half((depth, LANES))
    extra_ref[...] = jnp.zeros_like(extra_ref)

    @pl.loop(0, width // LANES)
    def _(m):
        for pair in range((parts + 1) // 2):
            lanes = slice(pair * LANES, (pair + 1) * LANES)
            even = blocks_ref[2 * m, :, lanes].astype(jnp.float32)
            odd = blocks_ref[2 * m + 1, :, lanes].astype(jnp.float32)
            first = pl.ds(pl.multiple_of(2 * pair * width + m * LANES, LANES), LANES)
            out_ref[:, first] = jnp.where(low, even, swap_halves(odd))
            if 2 * pair + 1 < parts:
                second = pl.ds(pl.multiple_of((2 * pair + 1) * width + m * LANES, LANES), LANES)
                out_ref[:, second] = jnp.where(low, swap_halves(even), odd)
            else:
                extra_ref[...] += even + odd


def join_blocks(blocks, parts):
    count, depth, _ = blocks.shape
    width = count * HD
    return pl.pallas_call(
        functools.partial(join_kernel, parts, width),
        out_shape=(
            jax.ShapeDtypeStruct((depth, parts * width), jnp.float32),
            jax.ShapeDtypeStruct((depth, LANES), jnp.float32),
        ),
        in_specs=[pl.BlockSpec(memory_space=pltpu.VMEM)],
        out_specs=(pl.BlockSpec(memory_space=pltpu.VMEM), pl.BlockSpec(memory_space=pltpu.VMEM)),
        compiler_params=pltpu.CompilerParams(vmem_limit_bytes=24 << 20),
    )(blocks)


SIDE = 256
HEAD_VMEM = 62 << 20


def turned(block, lane):
    shift = ROT // 2
    return jnp.where(lane % HD < shift, pltpu.roll(block, LANES - shift, 1), pltpu.roll(block, shift, 1))


def gelu_and_slope(t):
    scale = math.sqrt(2.0 / math.pi)
    square = t * t
    bent = jnp.tanh(scale * (t + 0.044715 * (square * t)))
    half = 0.5 * (1.0 + bent)
    return t * half, half + 0.5 * t * (1.0 - bent * bent) * scale * (1.0 + 3.0 * 0.044715 * square)


def allowed_keys(start, first_query, keys):
    query = first_query + lax.broadcasted_iota(jnp.int32, (SIDE, keys), 0)
    key = lax.broadcasted_iota(jnp.int32, (SIDE, keys), 1)
    return (key >= start) & (key <= query)


def document_starts(weights_ref, lanes, first, count):
    pieces = []
    for shard in range(count):
        rows = pl.ds(pl.multiple_of((first + shard) * HD, HD), HD)
        block = weights_ref[rows, lanes].astype(jnp.float32)
        pieces += [block[:, HD + 2 + n : HD + 3 + n] * 256.0 + block[:, HD + 4 + n : HD + 5 + n] for n in range(2)]
    return jnp.concatenate(pieces, 0)


def forward_kernel(depth, shard_rows, joint_width, routes, hat_ref, weights_ref, bias_ref, waves_ref, out_bias_ref, grad_ref,
                   qk_ref, mid_ref, cos_ref, sin_ref, joined_ref, out_ref, grads_ref, keys_ref, values_ref, shift_ref, out_row_ref, *scratch):
    seq = hat_ref.shape[0]
    here = pl.program_id(0)
    low = low_half((SIDE, LANES))
    lane = lax.broadcasted_iota(jnp.int32, (SIDE, LANES), 1)
    scaling = HD ** (-0.5)
    parts = gather_parts(depth, shard_rows, routes, grad_ref, grads_ref, scratch)
    chunks = seq // SIDE
    slots = spread_steps([parts[0].me.greet] + interleaved(parts), len(parts), depth * 2 * chunks, IDLE, [part.finish for part in parts])
    side_lanes = slice(joint_width - LANES, joint_width)

    for q in range(chunks):
        run_slots(slots, here, 2 * q, depth, 2 * chunks)
        if q == 0:

            @pl.when(here == 0)
            def _():
                both = jnp.concatenate([out_bias_ref[...].astype(jnp.float32)] * 2, 1)
                both = jnp.concatenate([both] * (out_row_ref.shape[1] // LANES), 1)
                owner = lax.broadcasted_iota(jnp.int32, both.shape, 1) // HD
                out_row_ref[...] = jnp.where(owner == parts[0].me.z * 8 + parts[0].me.c, both, 0.0)
                pieces = [bias_ref[n : n + 1, :].astype(jnp.float32) for n in range(bias_ref.shape[0])]
                pieces += [jnp.zeros_like(pieces[0])] * (joint_width // HD - len(pieces))
                total = jnp.concatenate(pieces, 1)
                for n in range(weights_ref.shape[0] // SIDE):
                    some = slice(n * SIDE, (n + 1) * SIDE)
                    side = weights_ref[some, side_lanes].astype(jnp.float32)
                    ratio = side[:, HD + 1 : HD + 2] / side[:, HD : HD + 1]
                    total = total + jnp.sum(ratio * weights_ref[some, :joint_width].astype(jnp.float32), 0, keepdims=True)
                shift_ref[...] = total

        rows = slice(q * SIDE, (q + 1) * SIDE)
        joint = jnp.dot(hat_ref[rows, :], weights_ref[:, :joint_width], preferred_element_type=jnp.float32) + shift_ref[...]
        per_chunk = SIDE // shard_rows
        start = document_starts(weights_ref, side_lanes, (here * chunks + q) * per_chunk, per_chunk)
        index = q * SIDE + lax.broadcasted_iota(jnp.int32, (SIDE, 1), 0)
        angles = (index.astype(jnp.float32) - start) * waves_ref[0:1, :]
        cosine, sine = jnp.cos(angles), jnp.sin(angles) * waves_ref[1:2, :]
        cos_ref[rows, :] = cosine
        sin_ref[rows, :] = sine
        qk = joint[:, :LANES]
        qk = qk * cosine + turned(qk, lane) * sine
        keys_ref[rows, :] = swap_halves(qk).astype(jnp.bfloat16)
        query = jnp.where(low, qk * scaling, 0.0).astype(jnp.bfloat16)
        qk_ref[rows, :] = qk.astype(jnp.bfloat16)
        values_ref[rows, :] = jnp.where(low, joint[:, LANES : 2 * LANES], 0.0).astype(jnp.bfloat16)
        count = (q + 1) * SIDE
        scores = lax.dot_general(query, keys_ref[:count, :], NT, preferred_element_type=jnp.float32)
        scores = jnp.where(allowed_keys(start.astype(jnp.int32), q * SIDE, count), scores, negative)
        largest = jnp.max(scores, -1, keepdims=True)
        weights = jnp.exp(scores - largest)
        total = jnp.sum(weights, -1, keepdims=True)
        weights = (weights * (1.0 / total)).astype(jnp.bfloat16)
        attended = jnp.dot(weights, values_ref[:count, :], preferred_element_type=jnp.float32)
        run_slots(slots, here, 2 * q + 1, depth, 2 * chunks)
        lse = largest + jnp.log(total)
        hidden, slope = gelu_and_slope(joint[:, LANES : 2 * LANES])
        mid_ref[rows, :LANES] = jnp.where(low, joint[:, LANES : 2 * LANES], slope)
        joined_ref[rows, :LANES] = jnp.where(low, attended, hidden).astype(jnp.bfloat16)
        hidden, slope = gelu_and_slope(joint[:, 2 * LANES : 3 * LANES])
        mid_ref[rows, LANES : 2 * LANES] = slope
        joined_ref[rows, LANES : 2 * LANES] = hidden.astype(jnp.bfloat16)
        hidden, slope = gelu_and_slope(jnp.where(low, joint[:, 3 * LANES :], 0.0))
        mid_ref[rows, 2 * LANES :] = jnp.where(low, slope, lse)
        joined_ref[rows, 2 * LANES :] = hidden.astype(jnp.bfloat16)
        branch = lax.dot_general(joined_ref[rows, :], weights_ref[:, joint_width:], NT, preferred_element_type=jnp.float32)
        out_ref[rows, :] = (branch + out_row_ref[...]).astype(jnp.bfloat16)

    @pl.when(here == pl.num_programs(0) - 1)
    def _():
        for step in slots[-1]:
            step()


def spread_steps(steps, ahead, count, idle, after):
    slots = [[] for _ in range(count + 1)]
    slots[0] += steps[: 1 + ahead]
    rest = steps[1 + ahead :]
    for n, step in enumerate(rest):
        slots[min(n * (count - idle) // len(rest), count)].append(step)
    slots[-1] += after
    return slots


def run_slots(slots, here, q, blocks, chunks, first=0):
    for block in range(blocks):
        steps = slots[block * chunks + q]
        if steps:

            @pl.when(here == block + first)
            def _():
                for step in steps:
                    step()


def forward(hat_all, weights, joint_width, bias, waves, out_bias, grads, depth, seq, routes, collective_id):
    tokens, width = hat_all.shape
    joined_width = weights.shape[1] - joint_width

    def rows(columns):
        return pl.BlockSpec((seq, columns), lambda b: (b, 0))

    def whole(array):
        return pl.BlockSpec(array.shape, lambda b: (0, 0), pipeline_mode=pl.Buffered(1))

    def out(columns, kind):
        return jax.ShapeDtypeStruct((tokens, columns), kind)

    return pl.pallas_call(
        functools.partial(forward_kernel, depth, grads.shape[0], joint_width, routes),
        grid=(tokens // seq,),
        out_shape=(
            out(LANES, jnp.bfloat16),
            out(joined_width, jnp.float32),
            out(LANES, jnp.float32),
            out(LANES, jnp.float32),
            out(joined_width, jnp.bfloat16),
            out(width, jnp.bfloat16),
            out(width, jnp.bfloat16),
        ),
        in_specs=[rows(width), whole(weights), whole(bias), whole(waves), whole(out_bias), pl.BlockSpec(memory_space=pl.ANY)],
        out_specs=(
            rows(LANES), rows(joined_width), rows(LANES), rows(LANES), rows(joined_width), rows(width),
            pl.BlockSpec(memory_space=pl.ANY),
        ),
        scratch_shapes=[pltpu.VMEM((seq, LANES), jnp.bfloat16)] * 2
        + [pltpu.VMEM((1, joint_width), jnp.float32), pltpu.VMEM((1, width), jnp.float32)]
        + gather_scratch(depth, routes),
        compiler_params=pltpu.CompilerParams(collective_id=collective_id, has_side_effects=True, vmem_limit_bytes=63 << 20),
    )(hat_all, weights, bias, waves, out_bias, grads)


LATEST = 30
IDLE = -4


def backward_kernel(depth, shard_rows, joint_width, routes, grad_ref, hat_ref, weights_ref, qk_ref, mid_ref, cos_ref, sin_ref, branch_ref,
                    d_hat_ref, sums_ref, back_ref, own_ref,
                    keys_ref, values_ref, d_key_ref, d_value_ref, d_query_ref, d_joint_ref, total_ref, *scratch):
    seq = qk_ref.shape[0]
    chunks = seq // SIDE
    here, stage = pl.program_id(0), pl.program_id(1)
    low = low_half((SIDE, LANES))
    lane = lax.broadcasted_iota(jnp.int32, (SIDE, LANES), 1)
    scaling = HD ** (-0.5)
    side_lanes = slice(joint_width - LANES, joint_width)
    parts = scatter_parts(depth, shard_rows, routes, branch_ref, own_ref, scratch)
    main, ahead = interleaved(parts), (1 + depth) * len(parts)
    slots = [[] for _ in range(depth * 2 * chunks)] + [[part.finish for part in parts]]
    slots[0] += [parts[0].me.greet] + main[: len(parts)]
    for n, step in enumerate(main[len(parts) : ahead]):
        slots[1 + n // len(parts)].append(step)
    due = slots[:-1] + [[]]
    for n, step in enumerate(main[ahead:]):
        due[min(1 + depth + n * LATEST // (len(main) - ahead), len(due) - 1)].append(step)
    slots = due[:-1] + [due[-1] + slots[-1]]

    def first_stage(q, rows):
        if q == 0:
            d_key_ref[...] = jnp.zeros_like(d_key_ref)
            d_value_ref[...] = jnp.zeros_like(d_value_ref)

            @pl.when(here == 0)
            def _():
                sums_ref[...] = jnp.zeros_like(sums_ref)
                total_ref[...] = jnp.zeros_like(total_ref)

        d_joined = jnp.dot(grad_ref[...], weights_ref[:, joint_width:], preferred_element_type=jnp.float32)
        per_chunk = SIDE // shard_rows
        start = document_starts(weights_ref, side_lanes, (here * chunks + q) * per_chunk, per_chunk).astype(jnp.int32)
        qk = qk_ref[rows, :].astype(jnp.float32)
        keys_ref[rows, :] = jnp.where(low, swap_halves(qk), 0.0).astype(jnp.bfloat16)
        query = jnp.where(low, qk * scaling, 0.0).astype(jnp.bfloat16)
        values_ref[rows, :] = jnp.where(low, mid_ref[rows, :LANES], 0.0).astype(jnp.bfloat16)
        d_out = jnp.where(low, d_joined[:, :LANES], 0.0).astype(jnp.bfloat16)
        count = (q + 1) * SIDE
        lse = mid_ref[rows, 3 * LANES - 1 : 3 * LANES]
        scores = lax.dot_general(query, keys_ref[:count, :], NT, preferred_element_type=jnp.float32)
        weights = jnp.where(allowed_keys(start, q * SIDE, count), jnp.exp(scores - lse), 0.0)
        d_weights = lax.dot_general(d_out, values_ref[:count, :], NT, preferred_element_type=jnp.float32)
        moved = weights * d_weights
        d_scores = (moved - weights * jnp.sum(moved, -1, keepdims=True)).astype(jnp.bfloat16)
        weights = weights.astype(jnp.bfloat16)
        d_query_ref[rows, :] = jnp.dot(d_scores, keys_ref[:count, :], preferred_element_type=jnp.float32) * scaling
        d_key_ref[:count, :] += lax.dot_general(d_scores, query, TN, preferred_element_type=jnp.float32)
        d_value_ref[:count, :] += lax.dot_general(weights, d_out, TN, preferred_element_type=jnp.float32)
        d_joint_ref[rows, LANES : 2 * LANES] = (d_joined[:, :LANES] * mid_ref[rows, :LANES]).astype(jnp.bfloat16)
        d_joint_ref[rows, 2 * LANES : 3 * LANES] = (
            d_joined[:, LANES : 2 * LANES] * mid_ref[rows, LANES : 2 * LANES]
        ).astype(jnp.bfloat16)
        d_joint_ref[rows, 3 * LANES :] = jnp.where(
            low, d_joined[:, 2 * LANES :] * mid_ref[rows, 2 * LANES :], 0.0
        ).astype(jnp.bfloat16)

    def second_stage(q, rows):
        d_qk = jnp.where(low, d_query_ref[rows, :], swap_halves(d_key_ref[rows, :]))
        d_qk = d_qk * cos_ref[rows, :] - turned(d_qk, lane) * sin_ref[rows, :]
        d_joint_ref[rows, :LANES] = d_qk.astype(jnp.bfloat16)
        d_joint_ref[rows, LANES : 2 * LANES] = jnp.where(
            low, d_value_ref[rows, :], d_joint_ref[rows, LANES : 2 * LANES].astype(jnp.float32)
        ).astype(jnp.bfloat16)
        d_joint = d_joint_ref[rows, :]
        sums_ref[...] += jnp.sum(d_joint.astype(jnp.float32), 0, keepdims=True)
        d_hat = lax.dot_general(d_joint, weights_ref[:, :joint_width], NT, preferred_element_type=jnp.float32)
        d_hat_ref[...] = d_hat.astype(jnp.bfloat16)
        if q % 2 == 1:
            both = slice(rows.start - SIDE, rows.stop)
            total_ref[...] += lax.dot_general(d_joint_ref[both, :], hat_ref[...], TN, preferred_element_type=jnp.float32)

    for at in range(2 * chunks):

        @pl.when(stage == at)
        def _():
            run_slots(slots, here, at, depth, 2 * chunks)
            rows = slice(at % chunks * SIDE, (at % chunks + 1) * SIDE)
            if at < chunks:
                first_stage(at, rows)
            else:
                second_stage(at - chunks, rows)

    @pl.when((here == pl.num_programs(0) - 1) & (stage == 2 * chunks - 1))
    def _():
        side_lane = lax.broadcasted_iota(jnp.int32, (SIDE, LANES), 1)
        for n in range(back_ref.shape[0] // SIDE):
            some = slice(n * SIDE, (n + 1) * SIDE)
            side = weights_ref[some, side_lanes].astype(jnp.float32)
            gain, shift = side[:, HD : HD + 1], side[:, HD + 1 : HD + 2]
            weight = weights_ref[some, :joint_width].astype(jnp.float32)
            total = total_ref[:, some].T
            back = gain * total + shift * sums_ref[...]
            gain_part = jnp.sum(weight * total, 1, keepdims=True) / gain
            shift_part = jnp.sum(weight * sums_ref[...], 1, keepdims=True) / gain
            last = jnp.where(side_lane == HD, gain_part, back[:, side_lanes])
            last = jnp.where(side_lane == HD + 1, shift_part, last)
            back_ref[some, : joint_width - LANES] = back[:, : joint_width - LANES].astype(jnp.bfloat16)
            back_ref[some, side_lanes] = last.astype(jnp.bfloat16)
        for step in slots[-1]:
            step()


def backward(grad_all, hat_all, weights, joint_width, qk, mid, cosine, sine, branch, depth, seq, routes, collective_id):
    tokens, width = grad_all.shape
    joined_width = weights.shape[1] - joint_width
    own = tokens // (depth * 8)
    chunks = seq // SIDE

    def rows(columns):
        return pl.BlockSpec((seq, columns), lambda b, s: (b, 0))

    def whole(shape, **mode):
        return pl.BlockSpec(shape, lambda b, s: (0, 0), **mode)

    def early(columns):
        return pl.BlockSpec((SIDE, columns), lambda b, s: (b * chunks + jnp.minimum(s, chunks - 1), 0))

    def late(columns):
        return pl.BlockSpec((SIDE, columns), lambda b, s: (b * chunks + jnp.maximum(s - chunks, 0), 0))

    return pl.pallas_call(
        functools.partial(backward_kernel, depth, own, joint_width, routes),
        grid=(tokens // seq, 2 * chunks),
        out_shape=(
            jax.ShapeDtypeStruct((tokens, width), jnp.bfloat16),
            jax.ShapeDtypeStruct((1, joint_width), jnp.float32),
            jax.ShapeDtypeStruct((width, joint_width), jnp.bfloat16),
            jax.ShapeDtypeStruct((own, width), jnp.bfloat16),
        ),
        in_specs=[
            early(width),
            pl.BlockSpec((2 * SIDE, width), lambda b, s: ((b * chunks + jnp.maximum(s - chunks, 0)) // 2, 0)),
            whole(weights.shape, pipeline_mode=pl.Buffered(1)),
            rows(LANES), rows(joined_width), rows(LANES), rows(LANES), pl.BlockSpec(memory_space=pl.ANY),
        ],
        out_specs=(late(width), whole((1, joint_width)), whole((width, joint_width)), whole((own, width))),
        scratch_shapes=[pltpu.VMEM((seq, LANES), jnp.bfloat16)] * 2
        + [pltpu.VMEM((seq, LANES), jnp.float32)] * 3
        + [pltpu.VMEM((seq, joint_width), jnp.bfloat16), pltpu.VMEM((joint_width, width), jnp.float32)]
        + scatter_scratch(depth, own, width, branch.dtype, routes),
        compiler_params=pltpu.CompilerParams(collective_id=collective_id, has_side_effects=True, vmem_limit_bytes=63 << 20),
    )(grad_all, hat_all, weights, qk, mid, cosine, sine, branch)


PLANE_SLOT = 7


def tail_kernel(depth, full, routes, joined_ref, grads_ref, part_ref, blocks_ref, inputs_ref, grad_ref,
                out_ref, column_ref, got_in_ref, got_out_ref, total_ref, back_ref, *scratch):
    here = pl.program_id(0)
    count = len(scatter_scratch(depth, full, 1, part_ref.dtype, routes))
    each = len(Exchange.scratch(depth))
    parts = scatter_parts(depth, full, routes, part_ref, out_ref, scratch[:count])
    me = parts[0].me
    early = Exchange(me, blocks_ref, got_in_ref, *scratch[count : count + each])
    late = Exchange(me, back_ref, got_out_ref, *scratch[count + each :])
    chunks = part_ref.shape[0] // grads_ref.shape[0]
    main, ahead = interleaved(parts), (1 + depth) * len(parts)
    slots = [[] for _ in range(chunks)]
    slots[0] += [me.greet_all] + main[: len(parts)] + early.steps
    for n, step in enumerate(main[len(parts) : ahead]):
        slots[1 + n // len(parts)].append(step)
    slots[PLANE_SLOT] += main[ahead : ahead + len(parts)]
    for at in range(chunks):
        run_slots(slots, here, at, 1, chunks, at)

    @pl.when(here == 0)
    def _():
        total_ref[...] = jnp.zeros_like(total_ref)
        column_ref[...] = jnp.zeros_like(column_ref)

    grads = grads_ref[...]
    column_ref[...] += jnp.sum(grads.astype(jnp.float32), 0, keepdims=True)
    total_ref[...] += lax.dot_general(joined_ref[...], grads, TN, preferred_element_type=jnp.float32)

    @pl.when(here == chunks - 1)
    def _():
        depth_rows = back_ref.shape[1]
        for n in range(total_ref.shape[1] // SIDE):
            turned_part = total_ref[:, n * SIDE : (n + 1) * SIDE].T.astype(back_ref.dtype)
            for m in range(SIDE // depth_rows):
                back_ref[n * (SIDE // depth_rows) + m] = turned_part[m * depth_rows : (m + 1) * depth_rows]
        for step in late.steps + main[ahead + len(parts) :]:
            step()

        @pl.loop(0, full // 32)
        def _(i):
            rows = pl.ds(pl.multiple_of(i * 32, 32), 32)
            hat, inv_std = layer_norm(inputs_ref[rows, :].astype(jnp.float32))
            d_hat = out_ref[rows, :]
            d_hat = d_hat - jnp.mean(d_hat, -1, keepdims=True) - hat * jnp.mean(d_hat * hat, -1, keepdims=True)
            out_ref[rows, :] = inv_std * d_hat + grad_ref[rows, :].astype(jnp.float32)

        for part in parts + [early, late]:
            part.finish()


def tail(joined, grads_all, part, blocks, inputs, grads, depth, routes, collective_id):
    tokens, width = part.shape
    joined_width = joined.shape[1]
    devices = depth * 8
    rows = tokens // devices
    chunk = 2 * SIDE
    back = (devices, width // devices, joined_width)
    here = pl.BlockSpec(memory_space=pl.ANY)

    def whole(shape, **mode):
        return pl.BlockSpec(shape, lambda i: (0, 0), **mode)

    def some(columns):
        return pl.BlockSpec((chunk, columns), lambda i: (i, 0))

    once = {"pipeline_mode": pl.Buffered(1)}
    return pl.pallas_call(
        functools.partial(tail_kernel, depth, rows, routes),
        grid=(tokens // chunk,),
        out_shape=(
            jax.ShapeDtypeStruct((rows, width), jnp.float32),
            jax.ShapeDtypeStruct((1, width), jnp.float32),
            jax.ShapeDtypeStruct(blocks.shape, blocks.dtype),
            jax.ShapeDtypeStruct(back, joined.dtype),
        ),
        in_specs=[some(joined_width), some(width), here, here, whole(inputs.shape, **once), whole(grads.shape, **once)],
        out_specs=(whole((rows, width)), whole((1, width)), here, here),
        scratch_shapes=[pltpu.VMEM((joined_width, width), jnp.float32), pltpu.VMEM(back, joined.dtype)]
        + scatter_scratch(depth, rows, width, part.dtype, routes)
        + Exchange.scratch(depth)
        + Exchange.scratch(depth),
        compiler_params=pltpu.CompilerParams(collective_id=collective_id, has_side_effects=True, vmem_limit_bytes=60 << 20),
    )(joined, grads_all, part, blocks, inputs, grads)


def on_device(
    hidden_in, w_in_t, in_bias, ln_gain, ln_shift, w_out_t, out_bias, segment_ids, out_grad
):
    depth = lax.axis_size("dp")
    devices = depth * lax.axis_size("ctx")
    ctx = lax.axis_index("ctx")
    me = lax.axis_index("dp") * lax.axis_size("ctx") + ctx
    tok_rows, model_width = hidden_in.shape[1:]
    seq_len = segment_ids.shape[1]
    own = model_width // devices
    in_parts = in_bias.shape[0]
    out_parts = w_out_t.shape[1] // model_width
    in_width = in_parts * own
    joint_width = (in_parts + 1) // 2 * LANES

    gain, shift = ln_gain.astype(jnp.float32).T, ln_shift.astype(jnp.float32).T
    own_seg = lax.dynamic_slice_in_dim(segment_ids[0], ctx * tok_rows, tok_rows)
    begin = jnp.sum((segment_ids < own_seg[:, None]).astype(jnp.int32), 1)
    begin = jnp.stack([begin // 256, begin % 256]).reshape(-1, own).T.astype(jnp.float32)
    extra = jnp.concatenate(
        [jnp.zeros((own, LANES // 2)), gain, shift, begin, jnp.zeros((own, LANES // 2 - 2 - begin.shape[1]))], 1
    )
    inputs = hidden_in[0]
    hat_all, got = head(inputs, w_in_t.T, w_out_t, (in_parts, out_parts), gain, extra, depth, ("zf", "fz"), 0)

    weights = got.reshape(model_width, -1)
    half = ROT // 2
    lane = np.arange(LANES) % HD
    frequency = np.float32(10000.0) ** (-2.0 * (lane % half).astype(np.float32) / np.float32(ROT))
    waves = np.stack([np.where(lane < ROT, frequency, 0.0), np.where(lane < half, -1.0, 1.0)]).astype(np.float32)
    qk, mid, cosine, sine, joined, branch, g_all = forward(
        hat_all, weights, joint_width, in_bias, waves, out_bias[None], out_grad[0], depth, seq_len, ("zf", "fz"), 1
    )
    d_hat_part, joint_sums, back_in, branch_own = backward(
        g_all, hat_all, weights, joint_width, qk, mid, cosine, sine, branch, depth, seq_len, ("zf",) * 4, 2
    )
    result = (inputs.astype(jnp.float32) + branch_own.astype(jnp.float32)).astype(jnp.bfloat16)
    d_input, column_sums, back_in, back_out = tail(
        joined, g_all, d_hat_part, back_in.reshape(devices, own, -1), inputs, out_grad[0], depth, ("zf",), 3
    )
    grad_w_out, _ = join_blocks(back_out, out_parts)
    grad_w_in, vectors = join_blocks(back_in, in_parts)
    return (
        result[None],
        d_input[None],
        grad_w_in.T,
        joint_sums[:, :in_width].reshape(in_parts, own),
        vectors[:, LANES // 2][None],
        vectors[:, LANES // 2 + 1][None],
        grad_w_out,
        lax.dynamic_slice_in_dim(column_sums[0], me * own, own),
    )


def solution(mesh):
    in_specs = (
        P("dp", "ctx", None),
        P(None, ("dp", "ctx")),
        P(None, ("dp", "ctx")),
        P(None, ("dp", "ctx")),
        P(None, ("dp", "ctx")),
        P(("dp", "ctx"), None),
        P(("dp", "ctx")),
        P("dp", None),
        P("dp", "ctx", None),
    )
    out_specs = (
        P("dp", "ctx", None),
        P("dp", "ctx", None),
        P(None, ("dp", "ctx")),
        P(None, ("dp", "ctx")),
        P(None, ("dp", "ctx")),
        P(None, ("dp", "ctx")),
        P(("dp", "ctx"), None),
        P(("dp", "ctx")),
    )
    tensor_parallel = mesh.shape["ctx"] == 8 and mesh.shape["dp"] * 8 == H
    body = on_device if tensor_parallel else on_device_gathered
    return jax.shard_map(
        body, mesh=mesh, in_specs=in_specs, out_specs=out_specs, check_vma=False
    )
```
